256 devices in a mesh: gx: 4 (over x), gy: 16 (over z_lo, y), gz: 4 (over z_hi, core).
Axes of the slice: x: 4, y: 4, z: 8 (z_hi: 2, z_lo: 4; z = z_hi * 4 + z_lo), core: 2. Of those that a mesh axis runs over, the one named last changes fastest.
Arguments:
- atom_embedding: bfloat16 [4, 16, 4, 64, 512], P('gx', 'gy', 'gz'), may hold values from -6 to 6
- output_adjoint: bfloat16 [4, 16, 4, 64, 512], P('gx', 'gy', 'gz'), may hold values from -6 to 6
- fractional_coords: float32 [4, 16, 4, 3, 512], P('gx', 'gy', 'gz'), may hold values from 0 to 1, as said below
- element_labels: int32 [4, 16, 4, 512], P('gx', 'gy', 'gz'), may hold values from 0 to 3
- adjacent_ghost_entries: int32 [4, 16, 4, 16, 512], P('gx', 'gy', 'gz'), may hold values from 0 to 13823, as said below
- miller_triples: int32 [3, 2048], replicated, may hold values from -8 to 8
- reciprocal_kernel: float32 [2048, 64], replicated, may hold values from 0.02 to 0.2
- channel_mixing_matrix: bfloat16 [64, 64], replicated, may hold values from -0.75 to 0.75
- element_channel_factor: float32 [4, 64], replicated, may hold values from 0.25 to 1.75
- distance_kernel: float32 [16, 64], replicated, may hold values from -1.5 to 1.5
Outputs:
- atom_grad: bfloat16 [4, 16, 4, 64, 512], P('gx', 'gy', 'gz')
- position_grad: float32 [4, 16, 4, 3, 512], P('gx', 'gy', 'gz')
- weight_grad: float32 [64, 64], replicated
- radial_grad: float32 [16, 64], replicated
- filter_grad: float32 [2048, 64], P(('gx', 'gy', 'gz'))
The draws below stay inside these ranges and needn't reach their ends.
Inputs may be any that keep to these rules, and one draw needn't show every extreme that they name: `adjacent_ghost_entries`: the atoms of a brick form 32 blocks of 16 in order; block q < 27 is the cell of offset (q // 9 - 1, (q // 3) % 3 - 1, q % 3 - 1) of the brick, blocks 27 to 31 lie in its central cell. A ghost entry e names atom e % 512 of slot e // 512; an entry in a slot of offset o names an atom of a block whose cell offset equals -o in every dimension where o is not zero, and o is zero in every dimension where the listing atom's cell offset is zero; every slot occurs. `fractional_coords`: an atom of a block whose cell offset is -1 or 1 in a dimension lies within a quarter of the brick length of that face in that dimension. `miller_triples`: integer components; any triple may occur, the zero triple too.
All inputs are finite; a program needn't handle non-finite values.
Results may differ from the reference program's by a relative error of at most 0.0053.
Values may be sent and summed in bfloat16 or wider, within the bound.
No kernel may reach another device: no remote copies, remote signals or barrier semaphores. Data moves between devices by JAX's collectives and lax.ppermute only.
A program may use at most 128 MiB of HBM per device.

```python
import math
import jax
import jax.numpy as jnp
from jax import lax

ATOMS_DEV = 512
CH = 64
RECIP_POINTS = 2048
NBR = 16
NB = 16
KINDS = 4
MAX_RECIP_INDEX = 8
GX = 4
GY = 16
GZ = 4
N_GX = 4
N_GY = 16
N_GZ = 4


rim_width = 0.25


def block_cells():
    block_ids = jnp.arange(32, dtype=jnp.int32)
    first = jnp.where(block_ids < 27, block_ids // 9 - 1, 0)
    second = jnp.where(block_ids < 27, block_ids // 3 % 3 - 1, 0)
    third = jnp.where(block_ids < 27, block_ids % 3 - 1, 0)
    return jnp.stack([first, second, third], axis=1)


def atom_cells():
    atom_ids = jnp.arange(ATOMS_DEV, dtype=jnp.int32)
    return block_cells()[atom_ids // (ATOMS_DEV // 32)]


def draw_fractional_coords(key, part):
    cells = jnp.transpose(atom_cells(), (1, 0))
    uniform_part = jax.random.uniform(key, (GX, GY, GZ, 3, ATOMS_DEV), jnp.float32)
    low_side = rim_width * uniform_part
    high_side = 1.0 - rim_width + rim_width * uniform_part
    middle = rim_width + (1.0 - 2.0 * rim_width) * uniform_part
    return jnp.where(cells == -1, low_side, jnp.where(cells == 1, high_side, middle)).astype(jnp.float32)


def draw_adjacent_ghost_entries(key, part):
    key_cross = jax.random.fold_in(key, 11)
    key_centre = jax.random.fold_in(key, 12)
    key_atom = jax.random.fold_in(key, 13)
    array_dimensions = (GX, GY, GZ, NBR, ATOMS_DEV)
    cell_atoms = ATOMS_DEV // 32
    own_cell = jnp.transpose(atom_cells(), (1, 0))
    crossing = jax.random.randint(key_cross, (GX, GY, GZ, NBR, 3, ATOMS_DEV), 0, 2).astype(jnp.int32)
    offsets = own_cell * crossing
    target = jnp.where(offsets != 0, -own_cell, own_cell)
    slot_id = 9 * (offsets[:, :, :, :, 0] + 1) + 3 * (offsets[:, :, :, :, 1] + 1) + (offsets[:, :, :, :, 2] + 1)
    drawn_block = 9 * (target[:, :, :, :, 0] + 1) + 3 * (target[:, :, :, :, 1] + 1) + (target[:, :, :, :, 2] + 1)
    centre_pick = jax.random.randint(key_centre, array_dimensions, 0, 6).astype(jnp.int32)
    centre_block = jnp.where(centre_pick == 0, 13, 26 + centre_pick)
    target_block = jnp.where(drawn_block == 13, centre_block, drawn_block)
    atom_pick = jax.random.randint(key_atom, array_dimensions, 0, cell_atoms).astype(jnp.int32)
    return (slot_id * ATOMS_DEV + target_block * cell_atoms + atom_pick).astype(jnp.int32)


def touch_ends(drawn, rng, least, largest):
    index_at = [jax.random.randint(jax.random.fold_in(rng, axis), (), 0, length) for axis, length in enumerate(drawn.shape)]
    widest = drawn.shape.index(max(drawn.shape))
    neighbour = index_at[:widest] + [(index_at[widest] + 1) % drawn.shape[widest]] + index_at[widest + 1:]
    return drawn.at[tuple(index_at)].set(least).at[tuple(neighbour)].set(largest)


def level_of(own_key, shape, cuts, least, high):
    level = 1.0
    for axis_at, blocks in cuts:
        steps = jax.random.uniform(jax.random.fold_in(jax.random.fold_in(own_key, 6), axis_at), (blocks,), jnp.float32, least / len(cuts), high / len(cuts))
        level = level * jnp.repeat(jnp.exp(steps), shape[axis_at] // blocks).reshape((-1,) + (1,) * (len(shape) - 1 - axis_at))
    return level


def centred(key, shape, scale, bound, pieces=(), kind=jnp.bfloat16):
    result = jax.random.normal(key, shape, jnp.float32) * scale
    if len(pieces) > 0:
        result = level_of(key, shape, pieces, -0.22, 0.18) * result
    return jnp.clip(result, min=-bound, max=bound).astype(kind)


def setup_inputs(seed: int = 0) -> dict:
    arg_keys = jax.random.split(jax.random.key(seed), 11)
    return {
        "atom_embedding": centred(arg_keys[0], (GX, GY, GZ, CH, ATOMS_DEV), 1.0, 6.0, ((0, 4), (1, 16), (2, 4))),
        "output_adjoint": centred(arg_keys[1], (GX, GY, GZ, CH, ATOMS_DEV), 1.0, 6.0, ((0, 4), (1, 16), (2, 4))),
        "fractional_coords": draw_fractional_coords(jax.random.fold_in(arg_keys[10], 71), 0),
        "element_labels": touch_ends(jax.random.randint(arg_keys[3], (GX, GY, GZ, ATOMS_DEV), 0, KINDS), jax.random.fold_in(arg_keys[3], 1), 0, KINDS - 1).astype(jnp.int32),
        "adjacent_ghost_entries": draw_adjacent_ghost_entries(jax.random.fold_in(arg_keys[10], 71), 0),
        "miller_triples": touch_ends(jax.random.randint(arg_keys[5], (3, RECIP_POINTS), 0 - MAX_RECIP_INDEX, MAX_RECIP_INDEX + 1), jax.random.fold_in(arg_keys[5], 1), 0 - MAX_RECIP_INDEX, MAX_RECIP_INDEX).astype(jnp.int32),
        "reciprocal_kernel": jnp.clip(jnp.exp(jax.random.uniform(arg_keys[6], (RECIP_POINTS, CH), jnp.float32, math.log(0.02), math.log(0.2))), 0.02, 0.2),
        "channel_mixing_matrix": centred(arg_keys[7], (CH, CH), CH ** -0.5, 0.75),
        "element_channel_factor": jnp.clip(1.0 + 0.15 * jax.random.normal(arg_keys[8], (KINDS, CH), jnp.float32), 0.25, 1.75),
        "distance_kernel": centred(arg_keys[9], (NB, CH), NB ** -0.5, 1.5, (), jnp.float32),
    }


circle_angle = 2.0 * math.pi
reach_sq = 0.75

def phases(local_pos, anchor, reciprocal_points_rescaled):
    absolute = local_pos + anchor[:, None]
    angles = absolute[0][:, None] * reciprocal_points_rescaled[0][None, :]
    angles = angles + absolute[1][:, None] * reciprocal_points_rescaled[1][None, :]
    angles = angles + absolute[2][:, None] * reciprocal_points_rescaled[2][None, :]
    return (jnp.cos(angles).astype(jnp.bfloat16), jnp.sin(angles).astype(jnp.bfloat16))

def structure_terms(cos_part, sin_part, stacked):
    contract = (((0,), (1,)), ((), ()))
    with_cos = lax.dot_general(cos_part, stacked, contract, preferred_element_type=jnp.float32)
    with_sin = lax.dot_general(sin_part, stacked, contract, preferred_element_type=jnp.float32)
    return jnp.concatenate([with_cos, with_sin], axis=1)

def coefficients(totals, filt_rows, norm_atoms, norm_k):
    channels = filt_rows.shape[1]
    cos_struct = totals[:, 0:channels] * norm_atoms
    cos_back = totals[:, channels:2 * channels] * norm_k
    sin_struct = totals[:, 2 * channels:3 * channels] * norm_atoms
    sin_back = totals[:, 3 * channels:4 * channels] * norm_k
    coeffs = jnp.concatenate([norm_atoms * filt_rows * cos_back, norm_k * filt_rows * cos_struct, norm_atoms * filt_rows * sin_back, norm_k * filt_rows * sin_struct], axis=1)
    return (coeffs.astype(jnp.bfloat16), cos_struct * cos_back + sin_struct * sin_back)

def ewald_pieces(running, piece_rows, start_at, cos_all, sin_all, stacked, reciprocal_points_rescaled):
    count_rows = piece_rows.shape[0]
    channels = stacked.shape[0] // 2
    cos_part = lax.dynamic_slice_in_dim(cos_all, start_at, count_rows, 1)
    sin_part = lax.dynamic_slice_in_dim(sin_all, start_at, count_rows, 1)
    kv_part = lax.dynamic_slice_in_dim(reciprocal_points_rescaled, start_at, count_rows, 1)
    contract = (((0,), (1,)), ((), ()))
    atom_part = lax.dot_general(piece_rows[:, 0:channels], cos_part, contract, preferred_element_type=jnp.float32)
    atom_part = atom_part + lax.dot_general(piece_rows[:, 2 * channels:3 * channels], sin_part, contract, preferred_element_type=jnp.float32)
    along_u = lax.dot_general(stacked, piece_rows[:, 0:2 * channels], contract, preferred_element_type=jnp.float32)
    along_v = lax.dot_general(stacked, piece_rows[:, 2 * channels:4 * channels], contract, preferred_element_type=jnp.float32)
    angle_grad = along_v * cos_part.astype(jnp.float32) - along_u * sin_part.astype(jnp.float32)
    pos_part = lax.dot_general(kv_part, angle_grad, (((1,), (1,)), ((), ())), precision=lax.Precision.HIGHEST)
    return (running[0] + atom_part, running[1] + pos_part)

def species_gains(table, kinds):
    onehot = (kinds[None, :] == jnp.arange(table.shape[0], dtype=jnp.int32)[:, None]).astype(jnp.float32)
    return lax.dot_general(table, onehot, (((0,), (0,)), ((), ())), precision=lax.Precision.HIGHEST)

def offset_table():
    steps_one = jnp.arange(3, dtype=jnp.float32) - 1.0
    along_x = jnp.broadcast_to(steps_one[:, None, None], (3, 3, 3))
    along_y = jnp.broadcast_to(steps_one[None, :, None], (3, 3, 3))
    along_z = jnp.broadcast_to(steps_one[None, None, :], (3, 3, 3))
    return jnp.stack([along_x, along_y, along_z], axis=-1)

def short_range(ghost_values, ghost_places, neighbour_ids, radial_weights):
    channels = ghost_values.shape[1]
    flat_z = jnp.transpose(ghost_values, (1, 0, 2)).reshape(channels, -1)
    flat_pos = jnp.transpose(ghost_places, (1, 0, 2)).reshape(3, -1)
    near_z = flat_z[:, neighbour_ids]
    near_pos = flat_pos[:, neighbour_ids]
    relative = near_pos - ghost_places[13][:, None, :]
    dist_sq = lax.optimization_barrier(jnp.sum(relative * relative, axis=0))
    basis_count = radial_weights.shape[0]
    spacing = reach_sq / (basis_count - 1)
    centres = jnp.arange(basis_count, dtype=jnp.float32) * spacing
    radial_basis = jnp.exp(-jnp.square((dist_sq[None, :, :] - centres[:, None, None]) / (2.0 * spacing)))
    filters = jnp.einsum('bc,bja->cja', radial_weights, radial_basis, precision=lax.Precision.HIGHEST)
    agg = lax.optimization_barrier(jnp.sum(filters * near_z, axis=1)) * neighbour_ids.shape[0] ** (-0.5)
    return jax.nn.silu(agg)

def local_backward(ghost_z, ghost_pos, neighbour_ids, distance_kernel, upstream):

    def mapped(ghost_values, ghost_places, radial_weights):
        return short_range(ghost_values, ghost_places, neighbour_ids, radial_weights)
    _, pullback = jax.vjp(mapped, ghost_z.astype(jnp.float32), ghost_pos, distance_kernel)
    return pullback(upstream.astype(jnp.float32))

def fold_wrap(padded, along_axis):
    inner_size = padded.shape[along_axis] - 2
    interior = lax.slice_in_dim(padded, 1, inner_size + 1, axis=along_axis)
    low_plane = lax.slice_in_dim(padded, 0, 1, axis=along_axis)
    high_plane = lax.slice_in_dim(padded, inner_size + 1, inner_size + 2, axis=along_axis)
    middle_shape = list(low_plane.shape)
    middle_shape[along_axis] = inner_size - 2
    middle = jnp.zeros(middle_shape, padded.dtype)
    return interior + jnp.concatenate([high_plane, middle, low_plane], axis=along_axis)

def reference(atom_embedding, output_adjoint, fractional_coords, element_labels, adjacent_ghost_entries, miller_triples, reciprocal_kernel, channel_mixing_matrix, element_channel_factor, distance_kernel):
    brick_count = N_GX * N_GY * N_GZ
    atom_count = ATOMS_DEV
    norm_atoms = (atom_count * brick_count) ** (-0.5)
    norm_k = RECIP_POINTS ** (-0.5)
    accumulated_entries = jnp.array([N_GX, N_GY, N_GZ], jnp.float32)
    reciprocal_points_rescaled = miller_triples.astype(jnp.float32) * (circle_angle / accumulated_entries)[:, None]
    flat_h = atom_embedding.reshape(brick_count, CH, atom_count)
    flat_dy = output_adjoint.reshape(brick_count, CH, atom_count)
    flat_pos = fractional_coords.reshape(brick_count, 3, atom_count)
    flat_kind = element_labels.reshape(brick_count, atom_count)
    flat_nbr = adjacent_ghost_entries.reshape(brick_count, NBR, atom_count)
    indices = jnp.arange(brick_count, dtype=jnp.int32)

    def locate(brick_id):
        brick_id = brick_id.astype(jnp.int32)
        return ((brick_id // (N_GY * N_GZ)).astype(jnp.int32), (brick_id // N_GZ % N_GY).astype(jnp.int32), (brick_id % N_GZ).astype(jnp.int32))

    def anchor_of(brick_id):
        brick_x, brick_y, brick_z = locate(brick_id)
        return jnp.stack([brick_x, brick_y, brick_z]).astype(jnp.float32)

    def add_terms(totals, brick_id):
        cos_all, sin_all = phases(flat_pos[brick_id], anchor_of(brick_id), reciprocal_points_rescaled)
        stacked = jnp.concatenate([flat_h[brick_id], flat_dy[brick_id]], axis=0)
        return (totals + structure_terms(cos_all, sin_all, stacked), None)
    totals, _ = lax.scan(add_terms, jnp.zeros((RECIP_POINTS, 4 * CH), jnp.float32), indices)
    coeffs, filter_grad = coefficients(totals, reciprocal_kernel, norm_atoms, norm_k)

    def make_z(brick_id):
        gain_rows = species_gains(element_channel_factor, flat_kind[brick_id])
        projected = lax.dot_general(channel_mixing_matrix, flat_h[brick_id], (((0,), (0,)), ((), ())), preferred_element_type=jnp.float32)
        return ((projected * gain_rows).astype(jnp.bfloat16), gain_rows)
    zfeat, gains_all = lax.map(make_z, indices)
    pad_spec = ((1, 1), (1, 1), (1, 1), (0, 0), (0, 0))
    z_pad = jnp.pad(zfeat.reshape(N_GX, N_GY, N_GZ, CH, atom_count), pad_spec, mode='wrap')
    p_pad = jnp.pad(fractional_coords, pad_spec, mode='wrap')
    offsets = offset_table()[..., None]

    def brick_step(running, brick_id):
        grad_zpad, grad_ppad, grad_rad = running
        brick_x, brick_y, brick_z = locate(brick_id)
        zero_index = jnp.zeros((), jnp.int32)
        corner = (brick_x, brick_y, brick_z, zero_index, zero_index)
        ghost_z = lax.dynamic_slice(z_pad, corner, (3, 3, 3, CH, atom_count)).reshape(27, CH, atom_count)
        ghost_p = (lax.dynamic_slice(p_pad, corner, (3, 3, 3, 3, atom_count)) + offsets).reshape(27, 3, atom_count)
        grad_z, grad_p, grad_r = local_backward(ghost_z, ghost_p, flat_nbr[brick_id], distance_kernel, flat_dy[brick_id])
        region_z = lax.dynamic_slice(grad_zpad, corner, (3, 3, 3, CH, atom_count)) + grad_z.reshape(3, 3, 3, CH, atom_count)
        grad_zpad = lax.dynamic_update_slice(grad_zpad, region_z, corner)
        region_p = lax.dynamic_slice(grad_ppad, corner, (3, 3, 3, 3, atom_count)) + grad_p.reshape(3, 3, 3, 3, atom_count)
        grad_ppad = lax.dynamic_update_slice(grad_ppad, region_p, corner)
        cos_all, sin_all = phases(flat_pos[brick_id], anchor_of(brick_id), reciprocal_points_rescaled)
        stacked = jnp.concatenate([flat_h[brick_id], flat_dy[brick_id]], axis=0)
        zeros_pair = (jnp.zeros((CH, atom_count), jnp.float32), jnp.zeros((3, atom_count), jnp.float32))
        ewald_h, ewald_pos = ewald_pieces(zeros_pair, coeffs, zero_index, cos_all, sin_all, stacked, reciprocal_points_rescaled)
        return ((grad_zpad, grad_ppad, grad_rad + grad_r), (ewald_h, ewald_pos))
    start_state = (jnp.zeros((N_GX + 2, N_GY + 2, N_GZ + 2, CH, atom_count), jnp.float32), jnp.zeros((N_GX + 2, N_GY + 2, N_GZ + 2, 3, atom_count), jnp.float32), jnp.zeros((NB, CH), jnp.float32))
    (grad_zpad, grad_ppad, radial_grad), (ewald_h, ewald_pos) = lax.scan(brick_step, start_state, indices)
    zgrad = fold_wrap(fold_wrap(fold_wrap(grad_zpad, 0), 1), 2).reshape(brick_count, CH, atom_count)
    pos_short = fold_wrap(fold_wrap(fold_wrap(grad_ppad, 0), 1), 2).reshape(brick_count, 3, atom_count)
    zscaled = (zgrad * gains_all).astype(jnp.bfloat16)

    def finish(brick_id):
        atom_short = jnp.dot(channel_mixing_matrix, zscaled[brick_id], preferred_element_type=jnp.float32)
        atom_total = (flat_dy[brick_id].astype(jnp.float32) + ewald_h[brick_id] + atom_short).astype(jnp.bfloat16)
        weight_part = lax.dot_general(flat_h[brick_id], zscaled[brick_id], (((1,), (1,)), ((), ())), preferred_element_type=jnp.float32)
        return (atom_total, weight_part)
    atom_grad, weight_parts = lax.map(finish, indices)
    weight_grad = lax.optimization_barrier(jnp.sum(weight_parts, axis=0))
    position_grad = (ewald_pos + pos_short).reshape(fractional_coords.shape)
    return (atom_grad.reshape(atom_embedding.shape), position_grad, weight_grad, radial_grad, filter_grad)
```

```python
import functools
import math

import jax
import jax.numpy as jnp
from jax import lax
from jax.experimental import pallas as pl
from jax.experimental.pallas import tpu as pltpu
from jax.sharding import Mesh
from jax.sharding import PartitionSpec as P

GY = ("gy_0", "gy_1")
GZ = ("gz_0", "gz_1")
GX_GY_GZ = ("gx", "gy_0", "gy_1", "gz_0", "gz_1")

circle_angle = 2.0 * math.pi
CHUNK = 256
SIN_TERMS = (6.28316404, -41.33714227, 81.34076528, -70.99339569)
COS_TERMS = (0.99999995, -19.73917143, 64.93459054, -85.24032775, 56.2423573)
WHOLE = pl.BlockSpec(memory_space=pltpu.VMEM)

reach_sq = 0.75
GROUPS = 4
ROWS = 72
BLOCKS = 132
HIGH = BLOCKS // GROUPS * 16


def split_two(x):
    high = x.astype(jnp.bfloat16)
    return high, (x - high.astype(jnp.float32)).astype(jnp.bfloat16)


def row_pick(first, second, third, shape):
    row = lax.broadcasted_iota(jnp.int32, shape, 0) % 4
    spread = lambda v: jnp.broadcast_to(v, shape)
    return jnp.where(
        row == 0,
        spread(first),
        jnp.where(row == 1, spread(second), jnp.where(row == 2, spread(third), 0.0)),
    )


def short_kernel(
    table_ref,
    ids_ref,
    pos_ref,
    dy_ref,
    radial_ref,
    zgrad_ref,
    own_ref,
    rgrad_ref,
    lhs_ref,
    high_ref,
    low_ref,
    near_ref,
    rel_ref,
    basis_ref,
    filt_ref,
    acc_ref,
):
    channels, atoms = dy_ref.shape
    listed = ids_ref.shape[0]
    count = radial_ref.shape[0]
    f32, bf16 = jnp.float32, jnp.bfloat16
    spacing = reach_sq / (count - 1)
    width = 2.0 * spacing
    share = listed ** (-0.5)
    for g in range(GROUPS):
        part = table_ref[g * HIGH : (g + 1) * HIGH, :].astype(f32)
        lhs_ref[g * ROWS : (g + 1) * ROWS, :] = jnp.transpose(part)[0:ROWS, :].astype(bf16)
    ids = ids_ref[...]
    slot = lax.shift_right_logical(ids, 9)
    atom = jnp.bitwise_and(ids, 511)
    block = lax.shift_right_logical(atom, 4)
    ox = slot // 9
    oy = (slot // 3) % 3
    oz = slot % 3
    qx = block // 9
    qy = (block // 3) % 3
    qz = block % 3
    grid = ((3 * ox + qx - 2) * 5 + 3 * oy + qy - 2) * 5 + 3 * oz + qz - 2
    grid = jnp.where(block >= 27, block + (125 - 27), grid)
    low = grid // (BLOCKS // GROUPS)
    high = (grid - low * (BLOCKS // GROUPS)) * 16 + jnp.bitwise_and(atom, 15)
    high_ref[...] = high
    low_ref[...] = low
    offs = [(o - 1).astype(f32) for o in (ox, oy, oz)]
    own = pos_ref[...]
    own8 = row_pick(own[0:1], own[1:2], own[2:3], (8, atoms))
    w_hi, w_lo = split_two(radial_ref[...])
    w_stack = jnp.concatenate([w_hi, w_hi, w_lo], axis=0)
    centre = lax.broadcasted_iota(jnp.int32, (count, 1), 0).astype(f32) * spacing
    iota = lax.broadcasted_iota(jnp.int32, (HIGH, atoms), 0)

    def hot(j):
        return (high_ref[pl.ds(j, 1), :] == iota).astype(f32).astype(bf16)

    agg = jnp.zeros((channels, atoms), f32)
    for j in range(listed):
        found = jnp.dot(lhs_ref[...], hot(j), preferred_element_type=f32)
        low_j = low_ref[j : j + 1, :]
        near = found[0:ROWS]
        for g in range(1, GROUPS):
            near = jnp.where(low_j == g, found[g * ROWS : (g + 1) * ROWS], near)
        near_z = near[0:channels]
        near_ref[j] = near_z.astype(bf16)
        halves = near[channels : channels + 8]
        off8 = row_pick(offs[0][j : j + 1], offs[1][j : j + 1], offs[2][j : j + 1], (8, atoms))
        rel = halves + pltpu.roll(halves, 4, 0) + off8 - own8
        rel_ref[j] = rel
        dist = 0.5 * jnp.sum(rel * rel, axis=0, keepdims=True)
        scaled = (dist - centre) / width
        basis = jnp.exp(-(scaled * scaled))
        basis_ref[j] = basis
        b_hi, b_lo = split_two(basis)
        filt = lax.dot_general(
            w_stack,
            jnp.concatenate([b_hi, b_lo, b_hi], axis=0),
            (((0,), (0,)), ((), ())),
            preferred_element_type=f32,
        )
        filt_ref[j] = filt
        agg = agg + filt * near_z
    agg = agg * share
    gate = 1.0 / (1.0 + jnp.exp(-agg))
    g_all = dy_ref[...].astype(f32) * (gate * (1.0 + agg * (1.0 - gate))) * share
    acc_ref[...] = jnp.zeros_like(acc_ref)
    own_grad = jnp.zeros((8, atoms), f32)
    radial = jnp.zeros((2 * count, 2 * channels), f32)
    w_wide = jnp.concatenate([w_hi, w_hi, w_lo], axis=1)
    for j in range(listed):
        near_z = near_ref[j].astype(f32)
        dz = filt_ref[j] * g_all
        df = near_z * g_all
        f_hi, f_lo = split_two(df)
        basis = basis_ref[j]
        b_hi, b_lo = split_two(basis)
        radial = radial + lax.dot_general(
            jnp.concatenate([b_hi, b_lo], axis=0),
            jnp.concatenate([f_hi, f_lo], axis=0),
            (((1,), (1,)), ((), ())),
            preferred_element_type=f32,
        )
        dbasis = jnp.dot(
            w_wide, jnp.concatenate([f_hi, f_lo, f_hi], axis=0), preferred_element_type=f32
        )
        rel = rel_ref[j]
        dist = 0.5 * jnp.sum(rel * rel, axis=0, keepdims=True)
        slope = dbasis * basis * (dist - centre)
        ddist = jnp.sum(slope, axis=0, keepdims=True) * (-2.0 / (width * width))
        gpos = rel * (2.0 * ddist)
        own_grad = own_grad - gpos
        p_hi = gpos.astype(bf16).astype(f32)
        row8 = lax.broadcasted_iota(jnp.int32, (8, atoms), 0)
        tail = jnp.where(row8 < 4, p_hi, gpos - p_hi)
        full = jnp.concatenate([dz, tail], axis=0)
        low_j = low_ref[j : j + 1, :]
        spread = jnp.concatenate(
            [jnp.where(low_j == g, full, 0.0) for g in range(GROUPS)], axis=0
        ).astype(bf16)
        acc_ref[...] += lax.dot_general(
            spread, hot(j), (((1,), (1,)), ((), ())), preferred_element_type=f32
        )
    own_ref[...] = own_grad
    rgrad_ref[...] = (
        radial[0:count, 0:channels]
        + radial[count:, 0:channels]
        + radial[0:count, channels:]
        + radial[count:, channels:]
    )
    for g in range(GROUPS):
        part = jnp.transpose(acc_ref[g * ROWS : (g + 1) * ROWS, :])
        zgrad_ref[g * HIGH : (g + 1) * HIGH, :] = jnp.concatenate(
            [part, jnp.zeros((HIGH, 128 - ROWS), f32)], axis=1
        )


def short_range(table, ids, pos, dy, radial, interpret=False):
    channels, atoms = dy.shape
    listed = ids.shape[0]
    count = radial.shape[0]
    vmem = lambda s, d: pltpu.VMEM(s, d)
    spec = pl.BlockSpec(memory_space=pltpu.VMEM)
    return pl.pallas_call(
        short_kernel,
        out_shape=(
            jax.ShapeDtypeStruct((GROUPS * HIGH, 128), jnp.float32),
            jax.ShapeDtypeStruct((8, atoms), jnp.float32),
            jax.ShapeDtypeStruct((count, channels), jnp.float32),
        ),
        in_specs=[spec] * 5,
        out_specs=(spec,) * 3,
        scratch_shapes=[
            vmem((GROUPS * ROWS, HIGH), jnp.bfloat16),
            vmem((listed, atoms), jnp.int32),
            vmem((listed, atoms), jnp.int32),
            vmem((listed, channels, atoms), jnp.bfloat16),
            vmem((listed, 8, atoms), jnp.float32),
            vmem((listed, count, atoms), jnp.float32),
            vmem((listed, channels, atoms), jnp.float32),
            vmem((GROUPS * ROWS, HIGH), jnp.float32),
        ],
        interpret=interpret,
        name="short_range",
    )(table, ids, pos, dy, radial)


def from_behind(x, axis, by):
    devices = lax.axis_size(axis)
    return lax.ppermute(x, axis, [(i, (i + by) % devices) for i in range(devices)])


def project_kernel(h_ref, mix_ref, gain_ref, kind_ref, pos_ref, table_ref, gains_ref):
    f32, bf16 = jnp.float32, jnp.bfloat16
    channels, atoms = h_ref.shape
    kinds = gain_ref.shape[0]
    columns = jnp.transpose(gain_ref[...])
    label = kind_ref[...]
    gains = jnp.zeros((channels, atoms), f32)
    for kind in range(kinds):
        gains = jnp.where(label == kind, columns[:, kind : kind + 1], gains)
    gains_ref[...] = gains
    projected = lax.dot_general(
        mix_ref[...], h_ref[...], (((0,), (0,)), ((), ())), preferred_element_type=f32
    )
    z = (projected * gains).astype(bf16).astype(f32)
    pos = pos_ref[...]
    p_hi, p_lo = split_two(pos)
    none = jnp.zeros((1, atoms), f32)
    rows = jnp.concatenate(
        [z, p_hi.astype(f32), none, p_lo.astype(f32), none, jnp.zeros((128 - ROWS, atoms), f32)],
        axis=0,
    )
    table_ref[...] = jnp.transpose(rows).astype(bf16)


def project(h, mix, table, kinds, pos):
    channels, atoms = h.shape
    return pl.pallas_call(
        project_kernel,
        out_shape=(
            jax.ShapeDtypeStruct((atoms, 128), jnp.bfloat16),
            jax.ShapeDtypeStruct((channels, atoms), jnp.float32),
        ),
        in_specs=[WHOLE] * 5,
        out_specs=(WHOLE,) * 2,
        name="project",
    )(h, mix, table, kinds, pos)


def phase_kernel(turns_ref, miller_ref, stacked_ref, cos_ref, sin_ref, part_ref, flip_ref, t_ref):
    f32, bf16 = jnp.float32, jnp.bfloat16
    width = stacked_ref.shape[0]

    @pl.when(pl.program_id(0) == 0)
    def _():
        flip_ref[...] = jnp.transpose(stacked_ref[...])

    whole = turns_ref[...]
    t_hi, t_rest = whole.astype(bf16), whole - whole.astype(bf16).astype(f32)
    t_mid = t_rest.astype(bf16)
    t_lo = (t_rest - t_mid.astype(f32)).astype(bf16)
    rhs = jnp.concatenate([t_hi, t_mid, t_lo], axis=0)
    m = miller_ref[...].astype(f32).astype(bf16)
    lhs = jnp.concatenate([m, m, m], axis=0)
    t_ref[...] = lax.dot_general(lhs, rhs, (((0,), (0,)), ((), ())), preferred_element_type=f32)
    rows, lanes = 16, 256
    for top in range(0, t_ref.shape[0], rows):
        for left in range(0, t_ref.shape[1], lanes):
            at = (slice(top, top + rows), slice(left, left + lanes))
            t = t_ref[at]
            r = t - jnp.round(t)
            u = jnp.abs(r) - 0.25
            q = u * u
            s = SIN_TERMS[3]
            for term in SIN_TERMS[2::-1]:
                s = s * q + term
            c = COS_TERMS[4]
            for term in COS_TERMS[3::-1]:
                c = c * q + term
            cos_ref[at] = -(s * u).astype(bf16)
            sin_ref[at] = jnp.where(r < 0.0, -c, c).astype(bf16)
    part_ref[:, 0:width] = jnp.dot(
        cos_ref[...], flip_ref[...], preferred_element_type=f32
    ).astype(part_ref.dtype)
    part_ref[:, width:] = jnp.dot(
        sin_ref[...], flip_ref[...], preferred_element_type=f32
    ).astype(part_ref.dtype)


def phase_sums(turns, miller, stacked):
    points = miller.shape[1]
    width, atoms = stacked.shape
    step = min(CHUNK, points)
    return pl.pallas_call(
        phase_kernel,
        grid=(points // step,),
        out_shape=(
            jax.ShapeDtypeStruct((points, atoms), jnp.bfloat16),
            jax.ShapeDtypeStruct((points, atoms), jnp.bfloat16),
            jax.ShapeDtypeStruct((points, 2 * width), jnp.bfloat16),
        ),
        in_specs=[
            pl.BlockSpec(turns.shape, lambda i: (0, 0)),
            pl.BlockSpec((miller.shape[0], step), lambda i: (0, i)),
            pl.BlockSpec(stacked.shape, lambda i: (0, 0)),
        ],
        out_specs=(
            pl.BlockSpec((step, atoms), lambda i: (i, 0)),
            pl.BlockSpec((step, atoms), lambda i: (i, 0)),
            pl.BlockSpec((step, 2 * width), lambda i: (i, 0)),
        ),
        scratch_shapes=[
            pltpu.VMEM((atoms, width), jnp.bfloat16),
            pltpu.VMEM((step, atoms), jnp.float32),
        ],
        name="phase_sums",
    )(turns, miller, stacked)


def ewald_kernel(coeff_ref, cos_ref, sin_ref, miller_ref, stacked_ref, h_ref, pos_ref):
    f32, bf16 = jnp.float32, jnp.bfloat16
    width = stacked_ref.shape[0]
    channels = width // 2

    @pl.when(pl.program_id(0) == 0)
    def _():
        h_ref[...] = jnp.zeros_like(h_ref)
        pos_ref[...] = jnp.zeros_like(pos_ref)

    coeffs = coeff_ref[...]
    cos_part, sin_part = cos_ref[...], sin_ref[...]
    over_rows = (((0,), (0,)), ((), ()))
    h_ref[...] += lax.dot_general(
        coeffs[:, 0:channels], cos_part, over_rows, preferred_element_type=f32
    ) + lax.dot_general(
        coeffs[:, width : width + channels], sin_part, over_rows, preferred_element_type=f32
    )
    along_u = jnp.dot(coeffs[:, 0:width], stacked_ref[...], preferred_element_type=f32)
    along_v = jnp.dot(coeffs[:, width:], stacked_ref[...], preferred_element_type=f32)
    angle = along_v * cos_part.astype(f32) - along_u * sin_part.astype(f32)
    a_hi, a_lo = split_two(angle)
    m = miller_ref[...].astype(f32).astype(bf16)
    pos_ref[...] += jnp.dot(m, a_hi, preferred_element_type=f32) + jnp.dot(
        m, a_lo, preferred_element_type=f32
    )


def ewald(coeffs, cos_all, sin_all, miller, stacked):
    points, atoms = cos_all.shape
    width = stacked.shape[0]
    step = min(CHUNK, points)
    return pl.pallas_call(
        ewald_kernel,
        grid=(points // step,),
        out_shape=(
            jax.ShapeDtypeStruct((width // 2, atoms), jnp.float32),
            jax.ShapeDtypeStruct((miller.shape[0], atoms), jnp.float32),
        ),
        in_specs=[
            pl.BlockSpec((step, coeffs.shape[1]), lambda i: (i, 0)),
            pl.BlockSpec((step, atoms), lambda i: (i, 0)),
            pl.BlockSpec((step, atoms), lambda i: (i, 0)),
            pl.BlockSpec((miller.shape[0], step), lambda i: (0, i)),
            pl.BlockSpec(stacked.shape, lambda i: (0, 0)),
        ],
        out_specs=(
            pl.BlockSpec((width // 2, atoms), lambda i: (0, 0)),
            pl.BlockSpec((miller.shape[0], atoms), lambda i: (0, 0)),
        ),
        name="ewald",
    )(coeffs, cos_all, sin_all, miller, stacked)


def finish_kernel(rows_ref, gains_ref, mix_ref, h_ref, own_ref, short_ref, weight_ref, pos_ref):
    f32, bf16 = jnp.float32, jnp.bfloat16
    channels = h_ref.shape[0]
    flat = jnp.transpose(rows_ref[...])
    zscaled = (flat[0:channels] * gains_ref[...]).astype(bf16)
    short_ref[...] = jnp.dot(mix_ref[...], zscaled, preferred_element_type=f32)
    weight_ref[...] = lax.dot_general(
        h_ref[...], zscaled, (((1,), (1,)), ((), ())), preferred_element_type=f32
    )
    halves = flat[channels : channels + 8]
    pos_ref[...] = halves + pltpu.roll(halves, 4, 0) + own_ref[...]


def finish(rows, gains, mix, h, own):
    channels, atoms = h.shape
    return pl.pallas_call(
        finish_kernel,
        out_shape=(
            jax.ShapeDtypeStruct((channels, atoms), jnp.float32),
            jax.ShapeDtypeStruct((channels, channels), jnp.float32),
            jax.ShapeDtypeStruct((8, atoms), jnp.float32),
        ),
        in_specs=[WHOLE] * 5,
        out_specs=(WHOLE,) * 3,
        name="finish",
    )(rows, gains, mix, h, own)


def coefficients(totals, filt_rows, norm_atoms, norm_k):
    channels = filt_rows.shape[1]
    cos_struct = totals[:, 0:channels] * norm_atoms
    cos_back = totals[:, channels : 2 * channels] * norm_k
    sin_struct = totals[:, 2 * channels : 3 * channels] * norm_atoms
    sin_back = totals[:, 3 * channels : 4 * channels] * norm_k
    coeffs = jnp.concatenate(
        [
            norm_atoms * filt_rows * cos_back,
            norm_k * filt_rows * cos_struct,
            norm_atoms * filt_rows * sin_back,
            norm_k * filt_rows * sin_struct,
        ],
        axis=1,
    )
    return (coeffs.astype(jnp.bfloat16), cos_struct * cos_back + sin_struct * sin_back)


def widened(x, sides):
    for axis, dim in sides:
        length = x.shape[dim]
        before = from_behind(lax.slice_in_dim(x, length - 1, length, axis=dim), axis, 1)
        after = from_behind(lax.slice_in_dim(x, 0, 1, axis=dim), axis, -1)
        x = jnp.concatenate([before, x, after], axis=dim)
    return x


def folded(x, sides):
    for axis, dim in sides:
        length = x.shape[dim]
        first = lax.slice_in_dim(x, 0, 1, axis=dim).astype(jnp.bfloat16)
        last = lax.slice_in_dim(x, length - 1, length, axis=dim).astype(jnp.bfloat16)
        to_last = from_behind(first, axis, -1).astype(jnp.float32)
        to_first = from_behind(last, axis, 1).astype(jnp.float32)
        inner = lax.slice_in_dim(x, 1, length - 1, axis=dim)
        low = lax.slice_in_dim(inner, 0, 1, axis=dim) + to_first
        middle = lax.slice_in_dim(inner, 1, length - 3, axis=dim)
        high = lax.slice_in_dim(inner, length - 3, length - 2, axis=dim) + to_last
        x = jnp.concatenate([low, middle, high], axis=dim)
    return x


def shards(
    atom_embedding,
    output_adjoint,
    fractional_coords,
    element_labels,
    adjacent_ghost_entries,
    miller_triples,
    reciprocal_kernel,
    channel_mixing_matrix,
    element_channel_factor,
    distance_kernel,
):
    h = atom_embedding[0, 0, 0]
    dy = output_adjoint[0, 0, 0]
    pos = fractional_coords[0, 0, 0]
    channels, atoms = h.shape
    points = miller_triples.shape[1]
    devices = lax.axis_size(GX_GY_GZ)
    norm_atoms = (atoms * devices) ** (-0.5)
    norm_k = points ** (-0.5)
    lengths = jnp.array([lax.axis_size("gx"), lax.axis_size(GY), lax.axis_size(GZ)], jnp.float32)
    anchor = jnp.stack([lax.axis_index("gx"), lax.axis_index(GY), lax.axis_index(GZ)]).astype(
        jnp.float32
    )
    share_rows = points // devices
    share_start = lax.axis_index(GX_GY_GZ) * share_rows

    own_table, gains = project(
        h, channel_mixing_matrix, element_channel_factor, element_labels[0, 0], pos
    )
    sides = ((GZ, 2), (GY, 1), ("gx", 0))
    cells = own_table[0:432].reshape(3, 3, 3, 16, 128)
    wide = widened(cells, sides)

    turns = (pos + anchor[:, None]) / lengths[:, None]
    stacked = jnp.concatenate([h, dy], axis=0)
    cos_all, sin_all, part = phase_sums(turns, miller_triples, stacked)
    pieces = lax.all_to_all(part.reshape(devices, share_rows, 4 * channels), GX_GY_GZ, 0, 0)
    totals = jnp.sum(pieces.astype(jnp.float32), axis=0)
    filt_rows = lax.dynamic_slice_in_dim(reciprocal_kernel, share_start, share_rows, 0)
    own_coeffs, filter_share = coefficients(totals, filt_rows, norm_atoms, norm_k)
    spread = jnp.broadcast_to(own_coeffs[None], (devices, share_rows, 4 * channels))
    coeffs = lax.all_to_all(spread, GX_GY_GZ, 0, 0).reshape(points, 4 * channels)

    table = jnp.concatenate(
        [
            wide.reshape(2000, 128),
            own_table[432:512],
            jnp.zeros((GROUPS * HIGH - 2080, 128), jnp.bfloat16),
        ],
        axis=0,
    )
    ghost_grad, own_grad, grad_radial = short_range(
        table, adjacent_ghost_entries[0, 0, 0], pos, dy, distance_kernel
    )
    grid = ghost_grad[0:2000].reshape(5, 5, 5, 16, 128)
    inner = folded(grid, sides[::-1])
    rows = jnp.concatenate([inner.reshape(432, 128), ghost_grad[2000:2080]], axis=0)
    atom_short, weight_local, pos_short = finish(rows, gains, channel_mixing_matrix, h, own_grad)
    summed = lax.psum(jnp.concatenate([weight_local, grad_radial], axis=0), GX_GY_GZ)
    weight_grad, radial_grad = summed[0:channels], summed[channels:]

    ewald_h, ewald_pos = ewald(coeffs, cos_all, sin_all, miller_triples, stacked)
    atom_grad = (dy.astype(jnp.float32) + ewald_h + atom_short).astype(jnp.bfloat16)
    position_grad = ewald_pos * (circle_angle / lengths)[:, None] + pos_short[0:3]
    return (
        atom_grad[None, None, None],
        position_grad[None, None, None],
        weight_grad,
        radial_grad,
        filter_share,
    )


def solution(mesh):
    finer = Mesh(
        mesh.devices.reshape(mesh.shape["gx"], 4, 4, 2, 2), ("gx", "gy_0", "gy_1", "gz_0", "gz_1")
    )
    in_specs = (
        P("gx", GY, GZ, None, None),
        P("gx", GY, GZ, None, None),
        P("gx", GY, GZ, None, None),
        P("gx", GY, GZ, None),
        P("gx", GY, GZ, None, None),
        P(),
        P(),
        P(),
        P(),
        P(),
    )
    out_specs = (
        P("gx", GY, GZ, None, None),
        P("gx", GY, GZ, None, None),
        P(),
        P(),
        P(GX_GY_GZ, None),
    )
    return jax.shard_map(
        shards, mesh=finer, in_specs=in_specs, out_specs=out_specs, check_vma=False
    )
```

```python
import functools
import math

import jax
import jax.numpy as jnp
from jax import lax
from jax.experimental import pallas as pl
from jax.experimental.pallas import tpu as pltpu
from jax.sharding import Mesh
from jax.sharding import PartitionSpec as P

GY = ("gy_0", "gy_1")
GZ = ("gz_0", "gz_1")
CHIPS = ("gx", "gy_0", "gy_1", "gz_0")
PAIR = "gz_1"
GX_GY_GZ = ("gx", "gy_0", "gy_1", "gz_0", "gz_1")

circle_angle = 2.0 * math.pi
CHUNK = 256
SIN_TERMS = (6.28316404, -41.33714227, 81.34076528, -70.99339569)
COS_TERMS = (0.99999995, -19.73917143, 64.93459054, -85.24032775, 56.2423573)
WHOLE = pl.BlockSpec(memory_space=pltpu.VMEM)

reach_sq = 0.75
GROUPS = 4
ROWS = 72
BLOCKS = 132
HIGH = BLOCKS // GROUPS * 16


def split_two(x):
    high = x.astype(jnp.bfloat16)
    return high, (x - high.astype(jnp.float32)).astype(jnp.bfloat16)


def row_pick(first, second, third, shape):
    row = lax.broadcasted_iota(jnp.int32, shape, 0) % 4
    spread = lambda v: jnp.broadcast_to(v, shape)
    return jnp.where(
        row == 0,
        spread(first),
        jnp.where(row == 1, spread(second), jnp.where(row == 2, spread(third), 0.0)),
    )


def gains_of(gain_rows, labels, shape):
    columns = jnp.transpose(gain_rows)
    gains = jnp.zeros(shape, jnp.float32)
    for kind in range(gain_rows.shape[0]):
        gains = jnp.where(labels == kind, columns[:, kind : kind + 1], gains)
    return gains


def short_kernel(
    table_ref,
    ids_ref,
    pos_ref,
    dy_ref,
    radial_ref,
    mix_ref,
    gain_ref,
    zgrad_ref,
    own_ref,
    sums_ref,
    lhs_ref,
    feat_ref,
    gains_ref,
    high_ref,
    low_ref,
    near_ref,
    rel_ref,
    basis_ref,
    filt_ref,
    acc_ref,
):
    channels, atoms = dy_ref.shape
    listed = ids_ref.shape[0]
    count = radial_ref.shape[0]
    f32, bf16 = jnp.float32, jnp.bfloat16
    spacing = reach_sq / (count - 1)
    width = 2.0 * spacing
    share = listed ** (-0.5)
    for g in range(GROUPS):
        part = jnp.transpose(table_ref[g * HIGH : (g + 1) * HIGH, :].astype(f32))
        feat = part[0:channels].astype(bf16)
        gains = gains_of(gain_ref[...], part[ROWS : ROWS + 1], (channels, HIGH))
        feat_ref[g] = feat
        gains_ref[g] = gains
        z = lax.dot_general(
            mix_ref[...], feat, (((0,), (0,)), ((), ())), preferred_element_type=f32
        )
        lhs_ref[g * ROWS : (g + 1) * ROWS, :] = jnp.concatenate(
            [z * gains, part[channels:ROWS]], axis=0
        ).astype(bf16)
    ids = ids_ref[...]
    slot = lax.shift_right_logical(ids, 9)
    atom = jnp.bitwise_and(ids, 511)
    block = lax.shift_right_logical(atom, 4)
    ox = slot // 9
    oy = (slot // 3) % 3
    oz = slot % 3
    qx = block // 9
    qy = (block // 3) % 3
    qz = block % 3
    grid = ((3 * ox + qx - 2) * 5 + 3 * oy + qy - 2) * 5 + 3 * oz + qz - 2
    grid = jnp.where(block >= 27, block + (125 - 27), grid)
    low = grid // (BLOCKS // GROUPS)
    high = (grid - low * (BLOCKS // GROUPS)) * 16 + jnp.bitwise_and(atom, 15)
    high_ref[...] = high
    low_ref[...] = low
    offs = [(o - 1).astype(f32) for o in (ox, oy, oz)]
    own = pos_ref[...]
    own8 = row_pick(own[0:1], own[1:2], own[2:3], (8, atoms))
    w_hi, w_lo = split_two(radial_ref[...])
    w_stack = jnp.concatenate([w_hi, w_hi, w_lo], axis=0)
    centre = lax.broadcasted_iota(jnp.int32, (count, 1), 0).astype(f32) * spacing
    iota = lax.broadcasted_iota(jnp.int32, (HIGH, atoms), 0)

    def hot(j):
        return (high_ref[pl.ds(j, 1), :] == iota).astype(f32).astype(bf16)

    agg = jnp.zeros((channels, atoms), f32)
    for j in range(listed):
        found = jnp.dot(lhs_ref[...], hot(j), preferred_element_type=f32)
        low_j = low_ref[j : j + 1, :]
        near = found[0:ROWS]
        for g in range(1, GROUPS):
            near = jnp.where(low_j == g, found[g * ROWS : (g + 1) * ROWS], near)
        near_z = near[0:channels]
        near_ref[j] = near_z.astype(bf16)
        halves = near[channels : channels + 8]
        off8 = row_pick(offs[0][j : j + 1], offs[1][j : j + 1], offs[2][j : j + 1], (8, atoms))
        rel = halves + pltpu.roll(halves, 4, 0) + off8 - own8
        rel_ref[j] = rel
        dist = 0.5 * jnp.sum(rel * rel, axis=0, keepdims=True)
        scaled = (dist - centre) / width
        basis = jnp.exp(-(scaled * scaled))
        basis_ref[j] = basis
        b_hi, b_lo = split_two(basis)
        filt = lax.dot_general(
            w_stack,
            jnp.concatenate([b_hi, b_lo, b_hi], axis=0),
            (((0,), (0,)), ((), ())),
            preferred_element_type=f32,
        )
        filt_ref[j] = filt
        agg = agg + filt * near_z
    agg = agg * share
    gate = 1.0 / (1.0 + jnp.exp(-agg))
    g_all = dy_ref[...].astype(f32) * (gate * (1.0 + agg * (1.0 - gate))) * share
    acc_ref[...] = jnp.zeros_like(acc_ref)
    own_grad = jnp.zeros((8, atoms), f32)
    radial = jnp.zeros((2 * count, 2 * channels), f32)
    w_wide = jnp.concatenate([w_hi, w_hi, w_lo], axis=1)
    for j in range(listed):
        near_z = near_ref[j].astype(f32)
        dz = filt_ref[j] * g_all
        df = near_z * g_all
        f_hi, f_lo = split_two(df)
        basis = basis_ref[j]
        b_hi, b_lo = split_two(basis)
        radial = radial + lax.dot_general(
            jnp.concatenate([b_hi, b_lo], axis=0),
            jnp.concatenate([f_hi, f_lo], axis=0),
            (((1,), (1,)), ((), ())),
            preferred_element_type=f32,
        )
        dbasis = jnp.dot(
            w_wide, jnp.concatenate([f_hi, f_lo, f_hi], axis=0), preferred_element_type=f32
        )
        rel = rel_ref[j]
        dist = 0.5 * jnp.sum(rel * rel, axis=0, keepdims=True)
        slope = dbasis * basis * (dist - centre)
        ddist = jnp.sum(slope, axis=0, keepdims=True) * (-2.0 / (width * width))
        gpos = rel * (2.0 * ddist)
        own_grad = own_grad - gpos
        p_hi = gpos.astype(bf16).astype(f32)
        row8 = lax.broadcasted_iota(jnp.int32, (8, atoms), 0)
        tail = jnp.where(row8 < 4, p_hi, gpos - p_hi)
        full = jnp.concatenate([dz, tail], axis=0)
        low_j = low_ref[j : j + 1, :]
        spread = jnp.concatenate(
            [jnp.where(low_j == g, full, 0.0) for g in range(GROUPS)], axis=0
        ).astype(bf16)
        acc_ref[...] += lax.dot_general(
            spread, hot(j), (((1,), (1,)), ((), ())), preferred_element_type=f32
        )
    own_ref[...] = own_grad
    sums_ref[...] = jnp.zeros_like(sums_ref)
    sums_ref[channels : channels + count, 0:channels] = (
        radial[0:count, 0:channels]
        + radial[count:, 0:channels]
        + radial[0:count, channels:]
        + radial[count:, channels:]
    )
    weight = jnp.zeros((channels, channels), f32)
    for g in range(GROUPS):
        z_hi, z_lo = split_two(acc_ref[g * ROWS : g * ROWS + channels, :] * gains_ref[g])
        for piece in (z_hi, z_lo):
            weight = weight + lax.dot_general(
                feat_ref[g], piece, (((1,), (1,)), ((), ())), preferred_element_type=f32
            )
        part = jnp.transpose(acc_ref[g * ROWS : (g + 1) * ROWS, :])
        zgrad_ref[g * HIGH : (g + 1) * HIGH, :] = jnp.concatenate(
            [part, jnp.zeros((HIGH, 128 - ROWS), f32)], axis=1
        )
    sums_ref[0:channels, 0:channels] = weight


def short_range(table, ids, pos, dy, radial, mix, gain, interpret=False):
    channels, atoms = dy.shape
    listed = ids.shape[0]
    count = radial.shape[0]
    vmem = lambda s, d: pltpu.VMEM(s, d)
    spec = pl.BlockSpec(memory_space=pltpu.VMEM)
    return pl.pallas_call(
        short_kernel,
        out_shape=(
            jax.ShapeDtypeStruct((GROUPS * HIGH, 128), jnp.float32),
            jax.ShapeDtypeStruct((8, atoms), jnp.float32),
            jax.ShapeDtypeStruct((128, 128), jnp.float32),
        ),
        in_specs=[spec] * 7,
        out_specs=(spec,) * 3,
        scratch_shapes=[
            vmem((GROUPS * ROWS, HIGH), jnp.bfloat16),
            vmem((GROUPS, channels, HIGH), jnp.bfloat16),
            vmem((GROUPS, channels, HIGH), jnp.float32),
            vmem((listed, atoms), jnp.int32),
            vmem((listed, atoms), jnp.int32),
            vmem((listed, channels, atoms), jnp.bfloat16),
            vmem((listed, 8, atoms), jnp.float32),
            vmem((listed, count, atoms), jnp.float32),
            vmem((listed, channels, atoms), jnp.float32),
            vmem((GROUPS * ROWS, HIGH), jnp.float32),
        ],
        interpret=interpret,
        name="short_range",
    )(table, ids, pos, dy, radial, mix, gain)


def from_behind(x, axis, by):
    devices = lax.axis_size(axis)
    return lax.ppermute(x, axis, [(i, (i + by) % devices) for i in range(devices)])


def pack_kernel(h_ref, kind_ref, pos_ref, table_ref):
    f32 = jnp.float32
    channels, atoms = h_ref.shape
    p_hi, p_lo = split_two(pos_ref[...])
    none = jnp.zeros((1, atoms), f32)
    rows = jnp.concatenate(
        [
            h_ref[...].astype(f32),
            p_hi.astype(f32),
            none,
            p_lo.astype(f32),
            none,
            kind_ref[...].astype(f32),
            jnp.zeros((127 - ROWS, atoms), f32),
        ],
        axis=0,
    )
    table_ref[...] = jnp.transpose(rows).astype(jnp.bfloat16)


def pack(h, kinds, pos):
    return pl.pallas_call(
        pack_kernel,
        out_shape=jax.ShapeDtypeStruct((h.shape[1], 128), jnp.bfloat16),
        in_specs=[WHOLE] * 3,
        out_specs=WHOLE,
        name="pack",
    )(h, kinds, pos)


def phase_kernel(
    where_ref, pos_ref, miller_ref, h_ref, dy_ref, cos_ref, sin_ref, part_ref, flip_ref, t_ref
):
    f32, bf16 = jnp.float32, jnp.bfloat16
    width = 2 * h_ref.shape[0]

    @pl.when(pl.program_id(0) == 0)
    def _():
        flip_ref[...] = jnp.transpose(jnp.concatenate([h_ref[...], dy_ref[...]], axis=0))

    pos = pos_ref[...]
    turns = jnp.concatenate(
        [(pos[d : d + 1] + where_ref[0, d]) / where_ref[1, d] for d in range(3)], axis=0
    )
    t_hi, t_rest = split_two(turns)[0], turns - split_two(turns)[0].astype(f32)
    t_mid, t_lo = split_two(t_rest)
    rhs = jnp.concatenate([t_hi, t_mid, t_lo], axis=0)
    m = miller_ref[...].astype(f32).astype(bf16)
    lhs = jnp.concatenate([m, m, m], axis=0)
    t_ref[...] = lax.dot_general(lhs, rhs, (((0,), (0,)), ((), ())), preferred_element_type=f32)
    rows, lanes = 16, 256
    for top in range(0, t_ref.shape[0], rows):
        for left in range(0, t_ref.shape[1], lanes):
            at = (slice(top, top + rows), slice(left, left + lanes))
            t = t_ref[at]
            r = t - jnp.round(t)
            u = jnp.abs(r) - 0.25
            q = u * u
            s = SIN_TERMS[3]
            for term in SIN_TERMS[2::-1]:
                s = s * q + term
            c = COS_TERMS[4]
            for term in COS_TERMS[3::-1]:
                c = c * q + term
            cos_ref[at] = -(s * u).astype(bf16)
            sin_ref[at] = jnp.where(r < 0.0, -c, c).astype(bf16)
    part_ref[:, 0:width] = jnp.dot(
        cos_ref[...], flip_ref[...], preferred_element_type=f32
    ).astype(part_ref.dtype)
    part_ref[:, width:] = jnp.dot(
        sin_ref[...], flip_ref[...], preferred_element_type=f32
    ).astype(part_ref.dtype)


def phase_sums(place, pos, miller, h, dy):
    points = miller.shape[1]
    channels, atoms = h.shape
    width = 2 * channels
    step = min(CHUNK, points)
    still = lambda i: (0, 0)
    return pl.pallas_call(
        phase_kernel,
        grid=(points // step,),
        out_shape=(
            jax.ShapeDtypeStruct((points, atoms), jnp.bfloat16),
            jax.ShapeDtypeStruct((points, atoms), jnp.bfloat16),
            jax.ShapeDtypeStruct((points, 2 * width), jnp.float32),
        ),
        in_specs=[
            pl.BlockSpec(memory_space=pltpu.SMEM),
            pl.BlockSpec(pos.shape, still),
            pl.BlockSpec((miller.shape[0], step), lambda i: (0, i)),
            pl.BlockSpec(h.shape, still),
            pl.BlockSpec(dy.shape, still),
        ],
        out_specs=(
            pl.BlockSpec((step, atoms), lambda i: (i, 0)),
            pl.BlockSpec((step, atoms), lambda i: (i, 0)),
            pl.BlockSpec((step, 2 * width), lambda i: (i, 0)),
        ),
        scratch_shapes=[
            pltpu.VMEM((atoms, width), jnp.bfloat16),
            pltpu.VMEM((step, atoms), jnp.float32),
        ],
        cost_estimate=pl.CostEstimate(
            flops=6 * points * atoms * width, transcendentals=0, bytes_accessed=4 * points * atoms
        ),
        name="phase_sums",
    )(place, pos, miller, h, dy)


def ewald_kernel(last, where_ref, coeff_ref, cos_ref, sin_ref, miller_ref, h_ref, dy_ref, *rest):
    f32, bf16 = jnp.float32, jnp.bfloat16
    channels = h_ref.shape[0]
    width = 2 * channels
    step = pl.program_id(0)
    if last:
        from_sums, from_turn, short_ref, near_ref, atom_ref, pos_ref, both_ref, sums_ref, turn_ref = rest
    else:
        sums_ref, turn_ref, both_ref = rest

    @pl.when(step == 0)
    def _():
        both_ref[...] = jnp.concatenate([h_ref[...], dy_ref[...]], axis=0)
        sums_ref[...] = from_sums[...] if last else jnp.zeros_like(sums_ref)
        turn_ref[...] = from_turn[...] if last else jnp.zeros_like(turn_ref)

    coeffs = coeff_ref[...]
    cos_part, sin_part = cos_ref[...], sin_ref[...]
    over_rows = (((0,), (0,)), ((), ()))
    sums_ref[...] += lax.dot_general(
        coeffs[:, 0:channels], cos_part, over_rows, preferred_element_type=f32
    ) + lax.dot_general(
        coeffs[:, width : width + channels], sin_part, over_rows, preferred_element_type=f32
    )
    along_u = jnp.dot(coeffs[:, 0:width], both_ref[...], preferred_element_type=f32)
    along_v = jnp.dot(coeffs[:, width : 2 * width], both_ref[...], preferred_element_type=f32)
    angle = along_v * cos_part.astype(f32) - along_u * sin_part.astype(f32)
    a_hi, a_lo = split_two(angle)
    m = miller_ref[...].astype(f32).astype(bf16)
    turn_ref[...] += jnp.dot(m, a_hi, preferred_element_type=f32) + jnp.dot(
        m, a_lo, preferred_element_type=f32
    )
    if last:

        @pl.when(step == pl.num_programs(0) - 1)
        def _():
            atom_ref[...] = (dy_ref[...].astype(f32) + sums_ref[...] + short_ref[...]).astype(bf16)
            for d in range(3):
                pos_ref[d : d + 1, :] = (
                    turn_ref[d : d + 1, :] * (circle_angle / where_ref[1, d])
                    + near_ref[d : d + 1, :]
                )


def ewald(place, coeffs, cos_all, sin_all, miller, h, dy, more=()):
    points, atoms = cos_all.shape
    channels = h.shape[0]
    dims = miller.shape[0]
    step = min(CHUNK, points)
    last = len(more) > 0
    still = lambda i: (0, 0)
    sums = jax.ShapeDtypeStruct((channels, atoms), jnp.float32)
    turn = jax.ShapeDtypeStruct((dims, atoms), jnp.float32)
    scratch = [pltpu.VMEM((2 * channels, atoms), jnp.bfloat16)]
    if last:
        scratch += [pltpu.VMEM(sums.shape, jnp.float32), pltpu.VMEM(turn.shape, jnp.float32)]
        sums = jax.ShapeDtypeStruct(sums.shape, jnp.bfloat16)
    return pl.pallas_call(
        functools.partial(ewald_kernel, last),
        grid=(points // step,),
        out_shape=(sums, turn),
        in_specs=[
            pl.BlockSpec(memory_space=pltpu.SMEM),
            pl.BlockSpec((step, coeffs.shape[1]), lambda i: (i, 0)),
            pl.BlockSpec((step, atoms), lambda i: (i, 0)),
            pl.BlockSpec((step, atoms), lambda i: (i, 0)),
            pl.BlockSpec((dims, step), lambda i: (0, i)),
            pl.BlockSpec(h.shape, still),
            pl.BlockSpec(dy.shape, still),
        ]
        + [pl.BlockSpec(x.shape, still) for x in more],
        out_specs=(pl.BlockSpec(sums.shape, still), pl.BlockSpec(turn.shape, still)),
        scratch_shapes=scratch,
        cost_estimate=pl.CostEstimate(
            flops=8 * points * atoms * channels, transcendentals=0, bytes_accessed=4 * points * atoms
        ),
        name="ewald",
    )(place, coeffs, cos_all, sin_all, miller, h, dy, *more)


def finish_kernel(rows_ref, kind_ref, gain_ref, mix_ref, own_ref, short_ref, pos_ref):
    f32, bf16 = jnp.float32, jnp.bfloat16
    channels, atoms = short_ref.shape
    flat = jnp.transpose(rows_ref[...])
    gains = gains_of(gain_ref[...], kind_ref[...], (channels, atoms))
    zscaled = (flat[0:channels] * gains).astype(bf16)
    short_ref[...] = jnp.dot(mix_ref[...], zscaled, preferred_element_type=f32)
    halves = flat[channels : channels + 8]
    pos_ref[...] = halves + pltpu.roll(halves, 4, 0) + own_ref[...]


def finish(rows, kinds, gain, mix, own):
    channels, atoms = mix.shape[0], rows.shape[0]
    return pl.pallas_call(
        finish_kernel,
        out_shape=(
            jax.ShapeDtypeStruct((channels, atoms), jnp.float32),
            jax.ShapeDtypeStruct((8, atoms), jnp.float32),
        ),
        in_specs=[WHOLE] * 5,
        out_specs=(WHOLE,) * 2,
        name="finish",
    )(rows, kinds, gain, mix, own)


def coefficients(totals, filt_rows, norm_atoms, norm_k):
    channels = filt_rows.shape[1]
    cos_struct = totals[:, 0:channels] * norm_atoms
    cos_back = totals[:, channels : 2 * channels] * norm_k
    sin_struct = totals[:, 2 * channels : 3 * channels] * norm_atoms
    sin_back = totals[:, 3 * channels : 4 * channels] * norm_k
    coeffs = jnp.concatenate(
        [
            norm_atoms * filt_rows * cos_back,
            norm_k * filt_rows * cos_struct,
            norm_atoms * filt_rows * sin_back,
            norm_k * filt_rows * sin_struct,
        ],
        axis=1,
    )
    return (coeffs.astype(jnp.bfloat16), cos_struct * cos_back + sin_struct * sin_back)


def widened(x, sides):
    for axis, dim in sides:
        length = x.shape[dim]
        before = from_behind(lax.slice_in_dim(x, length - 1, length, axis=dim), axis, 1)
        after = from_behind(lax.slice_in_dim(x, 0, 1, axis=dim), axis, -1)
        x = jnp.concatenate([before, x, after], axis=dim)
    return x


def folded(x, sides):
    for axis, dim in sides:
        length = x.shape[dim]
        first = lax.slice_in_dim(x, 0, 1, axis=dim).astype(jnp.bfloat16)
        last = lax.slice_in_dim(x, length - 1, length, axis=dim).astype(jnp.bfloat16)
        to_last = from_behind(first, axis, -1).astype(jnp.float32)
        to_first = from_behind(last, axis, 1).astype(jnp.float32)
        inner = lax.slice_in_dim(x, 1, length - 1, axis=dim)
        low = lax.slice_in_dim(inner, 0, 1, axis=dim) + to_first
        middle = lax.slice_in_dim(inner, 1, length - 3, axis=dim)
        high = lax.slice_in_dim(inner, length - 3, length - 2, axis=dim) + to_last
        x = jnp.concatenate([low, middle, high], axis=dim)
    return x


def shards(
    atom_embedding,
    output_adjoint,
    fractional_coords,
    element_labels,
    adjacent_ghost_entries,
    miller_triples,
    reciprocal_kernel,
    channel_mixing_matrix,
    element_channel_factor,
    distance_kernel,
):
    h = atom_embedding[0, 0, 0]
    dy = output_adjoint[0, 0, 0]
    pos = fractional_coords[0, 0, 0]
    kinds = element_labels[0, 0]
    channels, atoms = h.shape
    points = miller_triples.shape[1]
    devices = lax.axis_size(GX_GY_GZ)
    norm_atoms = (atoms * devices) ** (-0.5)
    norm_k = points ** (-0.5)
    lengths = jnp.array([lax.axis_size("gx"), lax.axis_size(GY), lax.axis_size(GZ)], jnp.float32)
    anchor = jnp.stack([lax.axis_index("gx"), lax.axis_index(GY), lax.axis_index(GZ)]).astype(
        jnp.float32
    )
    place = jnp.stack([anchor, lengths])
    share_rows = points // devices
    share_start = lax.axis_index(GX_GY_GZ) * share_rows
    core = lax.axis_index(PAIR)
    groups = lax.axis_size(CHIPS)
    half = points // 2

    own_table = pack(h, kinds, pos)
    sides = ((GZ, 2), (GY, 1), ("gx", 0))
    cells = own_table[0:432].reshape(3, 3, 3, 16, 128)
    wide = widened(cells, sides)
    table = jnp.concatenate(
        [
            wide.reshape(2000, 128),
            own_table[432:512],
            jnp.zeros((GROUPS * HIGH - 2080, 128), jnp.bfloat16),
        ],
        axis=0,
    )

    split = miller_triples.reshape(3, groups, 2, share_rows)
    even, odd = split[:, :, 0].reshape(3, half), split[:, :, 1].reshape(3, half)
    miller_mine = jnp.where(core == 0, even, odd)
    miller_next = jnp.where(core == 0, odd, even)
    cos_next, sin_next, part_next = phase_sums(place, pos, miller_next, h, dy)
    received = from_behind(part_next, PAIR, 1)
    cos_mine, sin_mine, part_mine = phase_sums(place, pos, miller_mine, h, dy)
    paired = (part_mine + received).astype(jnp.bfloat16)
    paired, table = lax.optimization_barrier((paired, table))
    pieces = lax.all_to_all(paired.reshape(groups, share_rows, 4 * channels), CHIPS, 0, 0)

    ghost_grad, own_grad, sums = short_range(
        table,
        adjacent_ghost_entries[0, 0, 0],
        pos,
        dy,
        distance_kernel,
        channel_mixing_matrix,
        element_channel_factor,
    )
    sums = sums + from_behind(sums, PAIR, 1)
    tiles = sums.astype(jnp.bfloat16).reshape(1, 16, 1, 8, 128)
    tiles = jnp.broadcast_to(tiles, (groups // 32, 16, 2, 8, 128)).reshape(groups, 8, 128)

    totals = jnp.sum(pieces.astype(jnp.float32), axis=0)
    filt_rows = lax.dynamic_slice_in_dim(reciprocal_kernel, share_start, share_rows, 0)
    own_coeffs, filter_share = coefficients(totals, filt_rows, norm_atoms, norm_k)
    spread = jnp.broadcast_to(own_coeffs[None], (groups, share_rows, 4 * channels))
    got = lax.all_to_all(jnp.concatenate([spread, tiles], axis=2), CHIPS, 0, 0)
    tile_sum = jnp.sum(got[:, :, 4 * channels :].astype(jnp.float32), axis=0)
    coeffs_mine = got.reshape(half, 4 * channels + 128)
    coeffs_next = from_behind(coeffs_mine, PAIR, 1)

    grid = ghost_grad[0:2000].reshape(5, 5, 5, 16, 128)
    inner = folded(grid, sides[::-1])
    rows = jnp.concatenate([inner.reshape(432, 128), ghost_grad[2000:2080]], axis=0)
    atom_short, pos_short = finish(
        rows, kinds, element_channel_factor, channel_mixing_matrix, own_grad
    )
    every = lax.all_to_all(jnp.broadcast_to(tile_sum[None], (16, 8, 128)), GY, 0, 0)
    every = every.reshape(128, 128)
    weight_grad = every[0:channels, 0:channels]
    radial_grad = every[channels : channels + distance_kernel.shape[0], 0:channels]

    first = ewald(place, coeffs_mine, cos_mine, sin_mine, miller_mine, h, dy)
    atom_grad, position_grad = ewald(
        place, coeffs_next, cos_next, sin_next, miller_next, h, dy, (*first, atom_short, pos_short)
    )
    return (
        atom_grad[None, None, None],
        position_grad[None, None, None],
        weight_grad,
        radial_grad,
        filter_share,
    )


def solution(mesh):
    finer = Mesh(
        mesh.devices.reshape(mesh.shape["gx"], 4, 4, 2, 2), ("gx", "gy_0", "gy_1", "gz_0", "gz_1")
    )
    in_specs = (
        P("gx", GY, GZ, None, None),
        P("gx", GY, GZ, None, None),
        P("gx", GY, GZ, None, None),
        P("gx", GY, GZ, None),
        P("gx", GY, GZ, None, None),
        P(),
        P(),
        P(),
        P(),
        P(),
    )
    out_specs = (
        P("gx", GY, GZ, None, None),
        P("gx", GY, GZ, None, None),
        P(),
        P(),
        P(GX_GY_GZ, None),
    )
    return jax.shard_map(
        shards, mesh=finer, in_specs=in_specs, out_specs=out_specs, check_vma=False
    )
```

```python
import functools
import math

import jax
import jax.numpy as jnp
from jax import lax
from jax.experimental import pallas as pl
from jax.experimental.pallas import tpu as pltpu
from jax.sharding import Mesh
from jax.sharding import PartitionSpec as P

GY = ("gy_0", "gy_1")
GZ = ("gz_0", "gz_1")
CHIPS = ("gx", "gy_0", "gy_1", "gz_0")
PAIR = "gz_1"
GX_GY_GZ = ("gx", "gy_0", "gy_1", "gz_0", "gz_1")

circle_angle = 2.0 * math.pi
CHUNK = 256
SHARE = 8
SIN_TERMS = (6.28316404, -41.33714227, 81.34076528, -70.99339569)
COS_TERMS = (0.99999995, -19.73917143, 64.93459054, -85.24032775, 56.2423573)
WHOLE = pl.BlockSpec(memory_space=pltpu.VMEM)

reach_sq = 0.75
GROUPS = 9
ROWS = 72
BLOCKS = 135
HIGH = BLOCKS // GROUPS * 16


def split_two(x):
    high = x.astype(jnp.bfloat16)
    return high, (x - high.astype(jnp.float32)).astype(jnp.bfloat16)


def row_pick(first, second, third, shape):
    row = lax.broadcasted_iota(jnp.int32, shape, 0) % 4
    spread = lambda v: jnp.broadcast_to(v, shape)
    return jnp.where(
        row == 0,
        spread(first),
        jnp.where(row == 1, spread(second), jnp.where(row == 2, spread(third), 0.0)),
    )


def gains_of(gain_rows, labels, shape):
    columns = jnp.transpose(gain_rows)
    gains = jnp.zeros(shape, jnp.float32)
    for kind in range(gain_rows.shape[0]):
        gains = jnp.where(labels == kind, columns[:, kind : kind + 1], gains)
    return gains


def short_kernel(
    table_ref,
    ids_ref,
    pos_ref,
    dy_ref,
    radial_ref,
    mix_ref,
    gain_ref,
    zgrad_ref,
    thin_ref,
    own_ref,
    sums_ref,
    lhs_ref,
    feat_ref,
    gains_ref,
    high_ref,
    low_ref,
    near_ref,
    rel_ref,
    basis_ref,
    filt_ref,
    acc_ref,
):
    channels, atoms = dy_ref.shape
    listed = ids_ref.shape[0]
    count = radial_ref.shape[0]
    f32, bf16 = jnp.float32, jnp.bfloat16
    spacing = reach_sq / (count - 1)
    width = 2.0 * spacing
    share = listed ** (-0.5)
    for g in range(GROUPS):
        part = jnp.transpose(table_ref[g * HIGH : (g + 1) * HIGH, :].astype(f32))
        feat = part[0:channels].astype(bf16)
        gains = gains_of(gain_ref[...], part[ROWS : ROWS + 1], (channels, HIGH))
        feat_ref[g] = feat
        gains_ref[g] = gains
        z = lax.dot_general(
            mix_ref[...], feat, (((0,), (0,)), ((), ())), preferred_element_type=f32
        )
        lhs_ref[g * ROWS : (g + 1) * ROWS, :] = jnp.concatenate(
            [z * gains, part[channels:ROWS]], axis=0
        ).astype(bf16)
    ids = ids_ref[...]
    slot = lax.shift_right_logical(ids, 9)
    atom = jnp.bitwise_and(ids, 511)
    block = lax.shift_right_logical(atom, 4)
    ox = slot // 9
    oy = (slot // 3) % 3
    oz = slot % 3
    qx = block // 9
    qy = (block // 3) % 3
    qz = block % 3
    grid = ((3 * ox + qx - 2) * 5 + 3 * oy + qy - 2) * 5 + 3 * oz + qz - 2
    grid = jnp.where(block >= 27, block + (125 - 27), grid)
    low = grid // (BLOCKS // GROUPS)
    high = (grid - low * (BLOCKS // GROUPS)) * 16 + jnp.bitwise_and(atom, 15)
    high_ref[...] = high
    low_ref[...] = low
    offs = [(o - 1).astype(f32) for o in (ox, oy, oz)]
    own8 = row_pick(pos_ref[0], pos_ref[1], pos_ref[2], (8, atoms))
    w_hi, w_lo = split_two(radial_ref[...])
    w_stack = jnp.concatenate([w_hi, w_hi, w_lo], axis=0)
    centre = lax.broadcasted_iota(jnp.int32, (count, 1), 0).astype(f32) * spacing
    iota = lax.broadcasted_iota(jnp.int32, (HIGH, atoms), 0)

    def hot(j):
        return (high_ref[pl.ds(j, 1), :] == iota).astype(f32).astype(bf16)

    agg = jnp.zeros((channels, atoms), f32)
    for j in range(listed):
        found = jnp.dot(lhs_ref[...], hot(j), preferred_element_type=f32)
        low_j = low_ref[j : j + 1, :]
        near = found[0:ROWS]
        for g in range(1, GROUPS):
            near = jnp.where(low_j == g, found[g * ROWS : (g + 1) * ROWS], near)
        near_z = near[0:channels]
        near_ref[j] = near_z.astype(bf16)
        halves = near[channels : channels + 8]
        off8 = row_pick(offs[0][j : j + 1], offs[1][j : j + 1], offs[2][j : j + 1], (8, atoms))
        rel = halves + pltpu.roll(halves, 4, 0) + off8 - own8
        rel_ref[j] = rel
        dist = 0.5 * jnp.sum(rel * rel, axis=0, keepdims=True)
        scaled = (dist - centre) / width
        basis = jnp.exp(-(scaled * scaled))
        basis_ref[j] = basis
        b_hi, b_lo = split_two(basis)
        filt = lax.dot_general(
            w_stack,
            jnp.concatenate([b_hi, b_lo, b_hi], axis=0),
            (((0,), (0,)), ((), ())),
            preferred_element_type=f32,
        )
        filt_ref[j] = filt
        agg = agg + filt * near_z
    agg = agg * share
    gate = 1.0 / (1.0 + jnp.exp(-agg))
    g_all = dy_ref[...].astype(f32) * (gate * (1.0 + agg * (1.0 - gate))) * share
    acc_ref[...] = jnp.zeros_like(acc_ref)
    own_grad = jnp.zeros((8, atoms), f32)
    radial = jnp.zeros((2 * count, 2 * channels), f32)
    w_wide = jnp.concatenate([w_hi, w_hi, w_lo], axis=1)
    for j in range(listed):
        near_z = near_ref[j].astype(f32)
        dz = filt_ref[j] * g_all
        df = near_z * g_all
        f_hi, f_lo = split_two(df)
        basis = basis_ref[j]
        b_hi, b_lo = split_two(basis)
        radial = radial + lax.dot_general(
            jnp.concatenate([b_hi, b_lo], axis=0),
            jnp.concatenate([f_hi, f_lo], axis=0),
            (((1,), (1,)), ((), ())),
            preferred_element_type=f32,
        )
        dbasis = jnp.dot(
            w_wide, jnp.concatenate([f_hi, f_lo, f_hi], axis=0), preferred_element_type=f32
        )
        rel = rel_ref[j]
        dist = 0.5 * jnp.sum(rel * rel, axis=0, keepdims=True)
        slope = dbasis * basis * (dist - centre)
        ddist = jnp.sum(slope, axis=0, keepdims=True) * (-2.0 / (width * width))
        gpos = rel * (2.0 * ddist)
        own_grad = own_grad - gpos
        p_hi = gpos.astype(bf16).astype(f32)
        row8 = lax.broadcasted_iota(jnp.int32, (8, atoms), 0)
        tail = jnp.where(row8 < 4, p_hi, gpos - p_hi)
        full = jnp.concatenate([dz, tail], axis=0)
        low_j = low_ref[j : j + 1, :]
        spread = jnp.concatenate(
            [jnp.where(low_j == g, full, 0.0) for g in range(GROUPS)], axis=0
        ).astype(bf16)
        acc_ref[...] += lax.dot_general(
            spread, hot(j), (((1,), (1,)), ((), ())), preferred_element_type=f32
        )
    own_ref[...] = own_grad
    sums_ref[...] = jnp.zeros_like(sums_ref)
    sums_ref[channels : channels + count, 0:channels] = (
        radial[0:count, 0:channels]
        + radial[count:, 0:channels]
        + radial[0:count, channels:]
        + radial[count:, channels:]
    )
    weight = jnp.zeros((channels, channels), f32)
    for g in range(GROUPS):
        z_hi, z_lo = split_two(acc_ref[g * ROWS : g * ROWS + channels, :] * gains_ref[g])
        for piece in (z_hi, z_lo):
            weight = weight + lax.dot_general(
                feat_ref[g], piece, (((1,), (1,)), ((), ())), preferred_element_type=f32
            )
        part = jnp.transpose(acc_ref[g * ROWS : (g + 1) * ROWS, :])
        part = jnp.concatenate([part, jnp.zeros((HIGH, 128 - ROWS), f32)], axis=1)
        zgrad_ref[g * HIGH : (g + 1) * HIGH, :] = part
        thin_ref[g * HIGH : (g + 1) * HIGH, :] = part.astype(bf16)
    sums_ref[0:channels, 0:channels] = weight


def short_range(table, ids, pos, dy, radial, mix, gain, interpret=False):
    channels, atoms = dy.shape
    listed = ids.shape[0]
    count = radial.shape[0]
    vmem = lambda s, d: pltpu.VMEM(s, d)
    spec = pl.BlockSpec(memory_space=pltpu.VMEM)
    return pl.pallas_call(
        short_kernel,
        out_shape=(
            jax.ShapeDtypeStruct((GROUPS * HIGH, 128), jnp.float32),
            jax.ShapeDtypeStruct((GROUPS * HIGH, 128), jnp.bfloat16),
            jax.ShapeDtypeStruct((8, atoms), jnp.float32),
            jax.ShapeDtypeStruct((128, 128), jnp.float32),
        ),
        in_specs=[spec] * 7,
        out_specs=(spec,) * 4,
        scratch_shapes=[
            vmem((GROUPS * ROWS, HIGH), jnp.bfloat16),
            vmem((GROUPS, channels, HIGH), jnp.bfloat16),
            vmem((GROUPS, channels, HIGH), jnp.float32),
            vmem((listed, atoms), jnp.int32),
            vmem((listed, atoms), jnp.int32),
            vmem((listed, channels, atoms), jnp.bfloat16),
            vmem((listed, 8, atoms), jnp.float32),
            vmem((listed, count, atoms), jnp.float32),
            vmem((listed, channels, atoms), jnp.float32),
            vmem((GROUPS * ROWS, HIGH), jnp.float32),
        ],
        interpret=interpret,
        name="short_range",
    )(table, ids, pos, dy, radial, mix, gain)


def from_behind(x, axis, by):
    devices = lax.axis_size(axis)
    return lax.ppermute(x, axis, [(i, (i + by) % devices) for i in range(devices)])


def chosen(parity):
    column = lax.broadcasted_iota(jnp.int32, (2 * CHUNK, CHUNK), 1)
    row = lax.broadcasted_iota(jnp.int32, (2 * CHUNK, CHUNK), 0)
    picked = (column // SHARE) * (2 * SHARE) + column % SHARE + parity * SHARE
    return (row == picked).astype(jnp.float32).astype(jnp.bfloat16)


def pack_kernel(h_ref, kind_ref, pos_ref, miller_ref, table_ref, mine_ref, next_ref):
    f32, bf16 = jnp.float32, jnp.bfloat16
    channels, atoms = h_ref.shape
    none = jnp.zeros((1, atoms), f32)
    halves = [split_two(pos_ref[d]) for d in range(3)]
    rows = jnp.concatenate(
        [h_ref[...].astype(f32)]
        + [half[0].astype(f32) for half in halves]
        + [none]
        + [half[1].astype(f32) for half in halves]
        + [none, kind_ref[...].astype(f32), jnp.zeros((127 - ROWS, atoms), f32)],
        axis=0,
    )
    table_ref[...] = jnp.transpose(rows).astype(bf16)
    m = miller_ref[...].astype(f32)
    tall = jnp.concatenate([m, m, m, jnp.zeros((7, m.shape[1]), f32)], axis=0).astype(bf16)
    runs = m.shape[1] // (2 * CHUNK)
    stack = jnp.concatenate(
        [tall[:, j * 2 * CHUNK : (j + 1) * 2 * CHUNK] for j in range(runs)], axis=0
    )
    core = lax.axis_index(PAIR)
    for parity, out_ref in ((core, mine_ref), (1 - core, next_ref)):
        got = jnp.dot(stack, chosen(parity), preferred_element_type=f32).astype(bf16)
        for j in range(runs):
            out_ref[:, j * CHUNK : (j + 1) * CHUNK] = got[j * 16 : (j + 1) * 16]


def pack(h, kinds, pos, miller):
    half = jax.ShapeDtypeStruct((16, miller.shape[1] // 2), jnp.bfloat16)
    return pl.pallas_call(
        pack_kernel,
        out_shape=(jax.ShapeDtypeStruct((h.shape[1], 128), jnp.bfloat16), half, half),
        in_specs=[WHOLE] * 4,
        out_specs=(WHOLE,) * 3,
        name="pack",
    )(h, kinds, pos, miller)


def phase_kernel(
    pos_ref,
    miller_ref,
    h_ref,
    dy_ref,
    cos_out,
    sin_out,
    part_out,
    cos_ref,
    sin_ref,
    part_ref,
    flip_ref,
    rhs_ref,
    t_ref,
    sems,
):
    f32, bf16 = jnp.float32, jnp.bfloat16
    width = 2 * h_ref.shape[0]
    flip_ref[...] = jnp.transpose(jnp.concatenate([h_ref[...], dy_ref[...]], axis=0))
    axes = ("gx", GY, GZ)
    turns = jnp.concatenate(
        [
            (pos_ref[d] + lax.axis_index(axes[d]).astype(f32)) / float(lax.axis_size(axes[d]))
            for d in range(3)
        ],
        axis=0,
    )
    t_hi = turns.astype(bf16)
    t_mid, t_lo = split_two(turns - t_hi.astype(f32))
    rhs_ref[...] = jnp.concatenate(
        [t_hi, t_mid, t_lo, jnp.zeros((7, turns.shape[1]), bf16)], axis=0
    )
    steps = miller_ref.shape[1] // CHUNK
    rows, lanes = 16, 256

    def copies(i):
        at = pl.ds(pl.multiple_of(i * CHUNK, CHUNK), CHUNK)
        return [
            pltpu.make_async_copy(src.at[at], dst.at[at], sems.at[n, i])
            for n, (src, dst) in enumerate(
                ((cos_ref, cos_out), (sin_ref, sin_out), (part_ref, part_out))
            )
        ]

    def one(i, carry):
        base = pl.multiple_of(i * CHUNK, CHUNK)
        t_ref[...] = lax.dot_general(
            miller_ref[:, pl.ds(base, CHUNK)],
            rhs_ref[...],
            (((0,), (0,)), ((), ())),
            preferred_element_type=f32,
        )
        for top in range(0, CHUNK, rows):
            for left in range(0, t_ref.shape[1], lanes):
                t = t_ref[top : top + rows, left : left + lanes]
                r = t - jnp.round(t)
                u = jnp.abs(r) - 0.25
                q = u * u
                s = SIN_TERMS[3]
                for term in SIN_TERMS[2::-1]:
                    s = s * q + term
                c = COS_TERMS[4]
                for term in COS_TERMS[3::-1]:
                    c = c * q + term
                at = (pl.ds(base + top, rows), pl.ds(left, lanes))
                cos_ref[at] = -(s * u).astype(bf16)
                sin_ref[at] = jnp.where(r < 0.0, -c, c).astype(bf16)
        here = pl.ds(base, CHUNK)
        part_ref[here, 0:width] = jnp.dot(
            cos_ref[here, :], flip_ref[...], preferred_element_type=f32
        )
        part_ref[here, width:] = jnp.dot(
            sin_ref[here, :], flip_ref[...], preferred_element_type=f32
        )
        for copy in copies(i):
            copy.start()
        return carry

    lax.fori_loop(0, steps, one, 0)
    for i in range(steps):
        for copy in copies(i):
            copy.wait()


def phase_sums(pos, miller, h, dy):
    points = miller.shape[1]
    channels, atoms = h.shape
    width = 2 * channels
    wave = jax.ShapeDtypeStruct((points, atoms), jnp.bfloat16)
    sums = jax.ShapeDtypeStruct((points, 2 * width), jnp.float32)
    return pl.pallas_call(
        phase_kernel,
        out_shape=(wave, wave, sums),
        in_specs=[WHOLE] * 4,
        out_specs=(pl.BlockSpec(memory_space=pl.ANY),) * 3,
        scratch_shapes=[
            pltpu.VMEM(wave.shape, wave.dtype),
            pltpu.VMEM(wave.shape, wave.dtype),
            pltpu.VMEM(sums.shape, sums.dtype),
            pltpu.VMEM((atoms, width), jnp.bfloat16),
            pltpu.VMEM((16, atoms), jnp.bfloat16),
            pltpu.VMEM((CHUNK, atoms), jnp.float32),
            pltpu.SemaphoreType.DMA((3, points // CHUNK)),
        ],
        cost_estimate=pl.CostEstimate(
            flops=6 * points * atoms * width, transcendentals=0, bytes_accessed=4 * points * atoms
        ),
        name="phase_sums",
    )(pos, miller, h, dy)


def ewald_kernel(last, coeff_in, cos_in, sin_in, miller_ref, h_ref, dy_ref, *rest):
    f32, bf16 = jnp.float32, jnp.bfloat16
    channels = h_ref.shape[0]
    width = 2 * channels
    coeff_ref, cos_ref, sin_ref, both_ref, sems = rest[-5:]
    steps = miller_ref.shape[1] // CHUNK

    def copies(i):
        at = pl.ds(pl.multiple_of(i * CHUNK, CHUNK), CHUNK)
        wide = pl.ds(0, 2 * width)
        return [
            pltpu.make_async_copy(coeff_in.at[at, wide], coeff_ref.at[at], sems.at[0, i]),
            pltpu.make_async_copy(cos_in.at[at], cos_ref.at[at], sems.at[1, i]),
            pltpu.make_async_copy(sin_in.at[at], sin_ref.at[at], sems.at[2, i]),
        ]

    for i in range(steps):
        for copy in copies(i):
            copy.start()
    both_ref[...] = jnp.concatenate([h_ref[...], dy_ref[...]], axis=0)
    if last:
        sums_ref, turn_ref = rest[-7:-5]
        sums_ref[...] = rest[0][...]
        turn_ref[...] = rest[1][...]
    else:
        sums_ref, turn_ref = rest[0:2]
        sums_ref[...] = jnp.zeros_like(sums_ref)
        turn_ref[...] = jnp.zeros_like(turn_ref)
    over_rows = (((0,), (0,)), ((), ()))

    def one(i, carry):
        for copy in copies(i):
            copy.wait()
        at = pl.ds(pl.multiple_of(i * CHUNK, CHUNK), CHUNK)
        coeffs = coeff_ref[at, :]
        cos_part, sin_part = cos_ref[at, :], sin_ref[at, :]
        sums_ref[...] += lax.dot_general(
            coeffs[:, 0:channels], cos_part, over_rows, preferred_element_type=f32
        ) + lax.dot_general(
            coeffs[:, width : width + channels], sin_part, over_rows, preferred_element_type=f32
        )
        along_u = jnp.dot(coeffs[:, 0:width], both_ref[...], preferred_element_type=f32)
        along_v = jnp.dot(coeffs[:, width : 2 * width], both_ref[...], preferred_element_type=f32)
        angle = along_v * cos_part.astype(f32) - along_u * sin_part.astype(f32)
        a_hi, a_lo = split_two(angle)
        m = miller_ref[:, at]
        turn_ref[...] += jnp.dot(m, a_hi, preferred_element_type=f32) + jnp.dot(
            m, a_lo, preferred_element_type=f32
        )
        return carry

    lax.fori_loop(0, steps, one, 0)
    if last:
        short_ref, near_ref, all_ref, atom_ref, pos_ref, weight_ref, radial_ref = rest[2:9]
        atom_ref[...] = (dy_ref[...].astype(f32) + sums_ref[...] + short_ref[...]).astype(bf16)
        axes = ("gx", GY, GZ)
        for d in range(3):
            pos_ref[d] = (
                turn_ref[d : d + 1, :] * (circle_angle / lax.axis_size(axes[d]))
                + near_ref[d : d + 1, :]
            )
        weight_ref[...] = all_ref[0:channels, 0:channels]
        radial_ref[...] = all_ref[channels : channels + radial_ref.shape[0], 0:channels]


def ewald(coeffs, cos_all, sin_all, miller, h, dy, more=(), basis=0):
    points, atoms = cos_all.shape
    channels = h.shape[0]
    last = len(more) > 0
    sums = jax.ShapeDtypeStruct((channels, atoms), jnp.float32)
    turn = jax.ShapeDtypeStruct((16, atoms), jnp.float32)
    scratch = [
        pltpu.VMEM((points, 4 * channels), jnp.bfloat16),
        pltpu.VMEM(cos_all.shape, jnp.bfloat16),
        pltpu.VMEM(cos_all.shape, jnp.bfloat16),
        pltpu.VMEM((2 * channels, atoms), jnp.bfloat16),
        pltpu.SemaphoreType.DMA((3, points // CHUNK)),
    ]
    outs = (sums, turn)
    if last:
        scratch = [pltpu.VMEM(sums.shape, sums.dtype), pltpu.VMEM(turn.shape, turn.dtype)] + scratch
        outs = (
            jax.ShapeDtypeStruct(sums.shape, jnp.bfloat16),
            jax.ShapeDtypeStruct((3, 1, atoms), jnp.float32),
            jax.ShapeDtypeStruct((channels, channels), jnp.float32),
            jax.ShapeDtypeStruct((basis, channels), jnp.float32),
        )
    return pl.pallas_call(
        functools.partial(ewald_kernel, last),
        out_shape=outs,
        in_specs=[pl.BlockSpec(memory_space=pl.ANY)] * 3 + [WHOLE] * (3 + len(more)),
        out_specs=(WHOLE,) * len(outs),
        scratch_shapes=scratch,
        cost_estimate=pl.CostEstimate(
            flops=8 * points * atoms * channels,
            transcendentals=0,
            bytes_accessed=4 * points * atoms,
        ),
        name="ewald",
    )(coeffs, cos_all, sin_all, miller, h, dy, *more)


def finish_kernel(rows_ref, kind_ref, gain_ref, mix_ref, own_ref, short_ref, pos_ref):
    f32, bf16 = jnp.float32, jnp.bfloat16
    channels, atoms = short_ref.shape
    flat = jnp.transpose(rows_ref[...])
    gains = gains_of(gain_ref[...], kind_ref[...], (channels, atoms))
    zscaled = (flat[0:channels] * gains).astype(bf16)
    short_ref[...] = jnp.dot(mix_ref[...], zscaled, preferred_element_type=f32)
    halves = flat[channels : channels + 8]
    pos_ref[...] = halves + pltpu.roll(halves, 4, 0) + own_ref[...]


def finish(rows, kinds, gain, mix, own):
    channels, atoms = mix.shape[0], rows.shape[0]
    return pl.pallas_call(
        finish_kernel,
        out_shape=(
            jax.ShapeDtypeStruct((channels, atoms), jnp.float32),
            jax.ShapeDtypeStruct((8, atoms), jnp.float32),
        ),
        in_specs=[WHOLE] * 5,
        out_specs=(WHOLE,) * 2,
        name="finish",
    )(rows, kinds, gain, mix, own)


def coefficients(totals, filt_rows, norm_atoms, norm_k):
    channels = filt_rows.shape[1]
    cos_struct = totals[:, 0:channels] * norm_atoms
    cos_back = totals[:, channels : 2 * channels] * norm_k
    sin_struct = totals[:, 2 * channels : 3 * channels] * norm_atoms
    sin_back = totals[:, 3 * channels : 4 * channels] * norm_k
    coeffs = jnp.concatenate(
        [
            norm_atoms * filt_rows * cos_back,
            norm_k * filt_rows * cos_struct,
            norm_atoms * filt_rows * sin_back,
            norm_k * filt_rows * sin_struct,
        ],
        axis=1,
    )
    return (coeffs.astype(jnp.bfloat16), cos_struct * cos_back + sin_struct * sin_back)


def sent_out(x, axis, dim):
    length = x.shape[dim]
    before = from_behind(lax.slice_in_dim(x, length - 1, length, axis=dim), axis, 1)
    after = from_behind(lax.slice_in_dim(x, 0, 1, axis=dim), axis, -1)
    return before, after


def sent_back(x, axis, dim):
    length = x.shape[dim]
    first = lax.slice_in_dim(x, 0, 1, axis=dim).astype(jnp.bfloat16)
    last = lax.slice_in_dim(x, length - 1, length, axis=dim).astype(jnp.bfloat16)
    return from_behind(first, axis, -1), from_behind(last, axis, 1)


def folded(x, pieces, dim):
    to_last, to_first = [piece.astype(jnp.float32) for piece in pieces]
    low = lax.slice_in_dim(x, 1, 2, axis=dim) + to_first
    middle = lax.slice_in_dim(x, 2, 3, axis=dim)
    high = lax.slice_in_dim(x, 3, 4, axis=dim) + to_last
    return jnp.concatenate([low, middle, high], axis=dim)


def shards(
    atom_embedding,
    output_adjoint,
    fractional_coords,
    element_labels,
    adjacent_ghost_entries,
    miller_triples,
    reciprocal_kernel,
    channel_mixing_matrix,
    element_channel_factor,
    distance_kernel,
):
    h = atom_embedding[0, 0, 0]
    dy = output_adjoint[0, 0, 0]
    pos = fractional_coords[0, 0, 0][:, None, :]
    kinds = element_labels[0, 0]
    channels, atoms = h.shape
    points = miller_triples.shape[1]
    devices = lax.axis_size(GX_GY_GZ)
    norm_atoms = (atoms * devices) ** (-0.5)
    norm_k = points ** (-0.5)
    share_rows = points // devices
    share_start = lax.axis_index(GX_GY_GZ) * share_rows
    groups = lax.axis_size(CHIPS)
    half = points // 2

    own_table, miller_mine, miller_next = pack(h, kinds, pos, miller_triples)
    cells = own_table[0:432].reshape(3, 3, 3, 16, 128)
    below, above = sent_out(cells, GZ, 2)
    cos_next, sin_next, part_next = phase_sums(pos, miller_next, h, dy)
    received = from_behind(part_next, PAIR, 1)
    below, above, part_next = lax.optimization_barrier((below, above, part_next))
    cells = jnp.concatenate([below, cells, above], axis=2)
    below, above = sent_out(cells, GY, 1)
    cos_mine, sin_mine, part_mine = phase_sums(pos, miller_mine, h, dy)
    below, above, part_mine = lax.optimization_barrier((below, above, part_mine))
    cells = jnp.concatenate([below, cells, above], axis=1)
    below, above = sent_out(cells, "gx", 0)
    paired = (part_mine + received).astype(jnp.bfloat16)
    paired, below, above = lax.optimization_barrier((paired, below, above))
    pieces = lax.all_to_all(paired.reshape(groups, share_rows, 4 * channels), CHIPS, 0, 0)

    table = jnp.concatenate(
        [
            below.reshape(400, 128),
            cells.reshape(1200, 128),
            above.reshape(400, 128),
            own_table[432:512],
            jnp.zeros((GROUPS * HIGH - 2080, 128), jnp.bfloat16),
        ],
        axis=0,
    )
    ghost_grad, ghost_thin, own_grad, sums = short_range(
        table,
        adjacent_ghost_entries[0, 0, 0],
        pos,
        dy,
        distance_kernel,
        channel_mixing_matrix,
        element_channel_factor,
    )
    sums = sums + from_behind(sums, PAIR, 1)
    tiles = sums.astype(jnp.bfloat16).reshape(1, 16, 1, 8, 128)
    tiles = jnp.broadcast_to(tiles, (groups // 32, 16, 2, 8, 128)).reshape(groups, 8, 128)

    totals = jnp.sum(pieces.astype(jnp.float32), axis=0)
    filt_rows = lax.dynamic_slice_in_dim(reciprocal_kernel, share_start, share_rows, 0)
    own_coeffs, filter_share = coefficients(totals, filt_rows, norm_atoms, norm_k)
    spread = jnp.broadcast_to(own_coeffs[None], (groups, share_rows, 4 * channels))
    got = lax.all_to_all(jnp.concatenate([spread, tiles], axis=2), CHIPS, 0, 0)

    to_side = sent_back(ghost_thin[0:2000].reshape(5, 5, 5, 16, 128), "gx", 0)
    grid = folded(ghost_grad[0:2000].reshape(5, 5, 5, 16, 128), to_side, 0)
    grid = folded(grid, sent_back(grid, GY, 1), 1)

    tile_sum = jnp.sum(got[:, :, 4 * channels :].astype(jnp.float32), axis=0)
    coeffs_mine = got.reshape(half, 4 * channels + 128)
    coeffs_next = from_behind(coeffs_mine, PAIR, 1)
    every = lax.all_to_all(jnp.broadcast_to(tile_sum[None], (16, 8, 128)), GY, 0, 0)
    every = every.reshape(128, 128)
    to_side = sent_back(grid, GZ, 2)
    first = ewald(coeffs_mine, cos_mine, sin_mine, miller_mine, h, dy)
    to_side, first = lax.optimization_barrier((to_side, first))
    grid = folded(grid, to_side, 2)
    rows = jnp.concatenate([grid.reshape(432, 128), ghost_grad[2000:2080]], axis=0)
    atom_short, pos_short = finish(
        rows, kinds, element_channel_factor, channel_mixing_matrix, own_grad
    )
    atom_grad, position_grad, weight_grad, radial_grad = ewald(
        coeffs_next,
        cos_next,
        sin_next,
        miller_next,
        h,
        dy,
        (*first, atom_short, pos_short, every),
        distance_kernel.shape[0],
    )
    position_grad = position_grad[:, 0, :]
    return (
        atom_grad[None, None, None],
        position_grad[None, None, None],
        weight_grad,
        radial_grad,
        filter_share,
    )


def solution(mesh):
    finer = Mesh(
        mesh.devices.reshape(mesh.shape["gx"], 4, 4, 2, 2), ("gx", "gy_0", "gy_1", "gz_0", "gz_1")
    )
    in_specs = (
        P("gx", GY, GZ, None, None),
        P("gx", GY, GZ, None, None),
        P("gx", GY, GZ, None, None),
        P("gx", GY, GZ, None),
        P("gx", GY, GZ, None, None),
        P(),
        P(),
        P(),
        P(),
        P(),
    )
    out_specs = (
        P("gx", GY, GZ, None, None),
        P("gx", GY, GZ, None, None),
        P(),
        P(),
        P(GX_GY_GZ, None),
    )
    return jax.shard_map(
        shards, mesh=finer, in_specs=in_specs, out_specs=out_specs, check_vma=False
    )
```

```python
import functools
import math

import jax
import jax.numpy as jnp
from jax import lax
from jax.experimental import pallas as pl
from jax.experimental.pallas import tpu as pltpu
from jax.sharding import Mesh
from jax.sharding import PartitionSpec as P


GY = ("gy_0", "gy_1")
GZ = ("gz_0", "gz_1")
CHIPS = ("gx", "gy_0", "gy_1", "gz_0")
PLANE = ("gy_0", "gy_1", "gz_0")
PAIR = "gz_1"
GX_GY_GZ = ("gx", "gy_0", "gy_1", "gz_0", "gz_1")

circle_angle = 2.0 * math.pi
CHUNK = 256
SHARE = 8
SIN_TERMS = (6.28316404, -41.33714227, 81.34076528, -70.99339569)
COS_TERMS = (0.99999995, -19.73917143, 64.93459054, -85.24032775, 56.2423573)
WHOLE = pl.BlockSpec(memory_space=pltpu.VMEM)

reach_sq = 0.75
GROUPS = 9
ROWS = 72
BLOCKS = 135
HIGH = BLOCKS // GROUPS * 16


def split_two(x):
    high = x.astype(jnp.bfloat16)
    return high, (x - high.astype(jnp.float32)).astype(jnp.bfloat16)


def row_pick(first, second, third, shape):
    row = lax.broadcasted_iota(jnp.int32, shape, 0) % 4
    spread = lambda v: jnp.broadcast_to(v, shape)
    return jnp.where(
        row == 0,
        spread(first),
        jnp.where(row == 1, spread(second), jnp.where(row == 2, spread(third), 0.0)),
    )


def gains_of(gain_rows, labels, shape):
    columns = jnp.transpose(gain_rows)
    gains = jnp.zeros(shape, jnp.float32)
    for kind in range(gain_rows.shape[0]):
        gains = jnp.where(labels == kind, columns[:, kind : kind + 1], gains)
    return gains


def short_kernel(
    table_ref,
    ids_ref,
    pos_ref,
    dy_ref,
    radial_ref,
    mix_ref,
    gain_ref,
    zgrad_ref,
    thin_ref,
    own_ref,
    sums_ref,
    lhs_ref,
    feat_ref,
    gains_ref,
    high_ref,
    low_ref,
    near_ref,
    rel_ref,
    basis_ref,
    filt_ref,
    acc_ref,
):
    channels, atoms = dy_ref.shape
    listed = ids_ref.shape[0]
    count = radial_ref.shape[0]
    f32, bf16 = jnp.float32, jnp.bfloat16
    spacing = reach_sq / (count - 1)
    width = 2.0 * spacing
    share = listed ** (-0.5)
    for g in range(GROUPS):
        part = jnp.transpose(table_ref[g * HIGH : (g + 1) * HIGH, :].astype(f32))
        feat = part[0:channels].astype(bf16)
        gains = gains_of(gain_ref[...], part[ROWS : ROWS + 1], (channels, HIGH))
        feat_ref[g] = feat
        gains_ref[g] = gains
        z = lax.dot_general(
            mix_ref[...], feat, (((0,), (0,)), ((), ())), preferred_element_type=f32
        )
        lhs_ref[g * ROWS : (g + 1) * ROWS, :] = jnp.concatenate(
            [z * gains, part[channels:ROWS]], axis=0
        ).astype(bf16)
    ids = ids_ref[...]
    slot = lax.shift_right_logical(ids, 9)
    atom = jnp.bitwise_and(ids, 511)
    block = lax.shift_right_logical(atom, 4)
    ox = slot // 9
    oy = (slot // 3) % 3
    oz = slot % 3
    qx = block // 9
    qy = (block // 3) % 3
    qz = block % 3
    grid = ((3 * ox + qx - 2) * 5 + 3 * oy + qy - 2) * 5 + 3 * oz + qz - 2
    grid = jnp.where(block >= 27, block + (125 - 27), grid)
    low = grid // (BLOCKS // GROUPS)
    high = (grid - low * (BLOCKS // GROUPS)) * 16 + jnp.bitwise_and(atom, 15)
    high_ref[...] = high
    low_ref[...] = low
    offs = [(o - 1).astype(f32) for o in (ox, oy, oz)]
    own8 = row_pick(pos_ref[0], pos_ref[1], pos_ref[2], (8, atoms))
    w_hi, w_lo = split_two(radial_ref[...])
    w_stack = jnp.concatenate([w_hi, w_hi, w_lo], axis=0)
    centre = lax.broadcasted_iota(jnp.int32, (count, 1), 0).astype(f32) * spacing
    iota = lax.broadcasted_iota(jnp.int32, (HIGH, atoms), 0)

    def hot(j):
        return (high_ref[pl.ds(j, 1), :] == iota).astype(f32).astype(bf16)

    agg = jnp.zeros((channels, atoms), f32)
    for j in range(listed):
        found = jnp.dot(lhs_ref[...], hot(j), preferred_element_type=f32)
        low_j = low_ref[j : j + 1, :]
        near = found[0:ROWS]
        for g in range(1, GROUPS):
            near = jnp.where(low_j == g, found[g * ROWS : (g + 1) * ROWS], near)
        near_z = near[0:channels]
        near_ref[j] = near_z.astype(bf16)
        halves = near[channels : channels + 8]
        off8 = row_pick(offs[0][j : j + 1], offs[1][j : j + 1], offs[2][j : j + 1], (8, atoms))
        rel = halves + pltpu.roll(halves, 4, 0) + off8 - own8
        rel_ref[j] = rel
        dist = 0.5 * jnp.sum(rel * rel, axis=0, keepdims=True)
        scaled = (dist - centre) / width
        basis = jnp.exp(-(scaled * scaled))
        basis_ref[j] = basis
        b_hi, b_lo = split_two(basis)
        filt = lax.dot_general(
            w_stack,
            jnp.concatenate([b_hi, b_lo, b_hi], axis=0),
            (((0,), (0,)), ((), ())),
            preferred_element_type=f32,
        )
        filt_ref[j] = filt
        agg = agg + filt * near_z
    agg = agg * share
    gate = 1.0 / (1.0 + jnp.exp(-agg))
    g_all = dy_ref[...].astype(f32) * (gate * (1.0 + agg * (1.0 - gate))) * share
    acc_ref[...] = jnp.zeros_like(acc_ref)
    own_grad = jnp.zeros((8, atoms), f32)
    radial = jnp.zeros((2 * count, 2 * channels), f32)
    w_wide = jnp.concatenate([w_hi, w_hi, w_lo], axis=1)
    for j in range(listed):
        near_z = near_ref[j].astype(f32)
        dz = filt_ref[j] * g_all
        df = near_z * g_all
        f_hi, f_lo = split_two(df)
        basis = basis_ref[j]
        b_hi, b_lo = split_two(basis)
        radial = radial + lax.dot_general(
            jnp.concatenate([b_hi, b_lo], axis=0),
            jnp.concatenate([f_hi, f_lo], axis=0),
            (((1,), (1,)), ((), ())),
            preferred_element_type=f32,
        )
        dbasis = jnp.dot(
            w_wide, jnp.concatenate([f_hi, f_lo, f_hi], axis=0), preferred_element_type=f32
        )
        rel = rel_ref[j]
        dist = 0.5 * jnp.sum(rel * rel, axis=0, keepdims=True)
        slope = dbasis * basis * (dist - centre)
        ddist = jnp.sum(slope, axis=0, keepdims=True) * (-2.0 / (width * width))
        gpos = rel * (2.0 * ddist)
        own_grad = own_grad - gpos
        p_hi = gpos.astype(bf16).astype(f32)
        row8 = lax.broadcasted_iota(jnp.int32, (8, atoms), 0)
        tail = jnp.where(row8 < 4, p_hi, gpos - p_hi)
        full = jnp.concatenate([dz, tail], axis=0)
        low_j = low_ref[j : j + 1, :]
        spread = jnp.concatenate(
            [jnp.where(low_j == g, full, 0.0) for g in range(GROUPS)], axis=0
        ).astype(bf16)
        acc_ref[...] += lax.dot_general(
            spread, hot(j), (((1,), (1,)), ((), ())), preferred_element_type=f32
        )
    own_ref[...] = own_grad
    sums_ref[...] = jnp.zeros_like(sums_ref)
    sums_ref[channels : channels + count, 0:channels] = (
        radial[0:count, 0:channels]
        + radial[count:, 0:channels]
        + radial[0:count, channels:]
        + radial[count:, channels:]
    )
    weight = jnp.zeros((channels, channels), f32)
    for g in range(GROUPS):
        z_hi, z_lo = split_two(acc_ref[g * ROWS : g * ROWS + channels, :] * gains_ref[g])
        for piece in (z_hi, z_lo):
            weight = weight + lax.dot_general(
                feat_ref[g], piece, (((1,), (1,)), ((), ())), preferred_element_type=f32
            )
        part = jnp.transpose(acc_ref[g * ROWS : (g + 1) * ROWS, :])
        part = jnp.concatenate([part, jnp.zeros((HIGH, 128 - ROWS), f32)], axis=1)
        zgrad_ref[g * HIGH : (g + 1) * HIGH, :] = part
        thin_ref[g * HIGH : (g + 1) * HIGH, :] = part.astype(bf16)
    sums_ref[0:channels, 0:channels] = weight


def short_range(table, ids, pos, dy, radial, mix, gain, interpret=False):
    channels, atoms = dy.shape
    listed = ids.shape[0]
    count = radial.shape[0]
    vmem = lambda s, d: pltpu.VMEM(s, d)
    spec = pl.BlockSpec(memory_space=pltpu.VMEM)
    return pl.pallas_call(
        short_kernel,
        out_shape=(
            jax.ShapeDtypeStruct((GROUPS * HIGH, 128), jnp.float32),
            jax.ShapeDtypeStruct((GROUPS * HIGH, 128), jnp.bfloat16),
            jax.ShapeDtypeStruct((8, atoms), jnp.float32),
            jax.ShapeDtypeStruct((128, 128), jnp.float32),
        ),
        in_specs=[spec] * 7,
        out_specs=(spec,) * 4,
        scratch_shapes=[
            vmem((GROUPS * ROWS, HIGH), jnp.bfloat16),
            vmem((GROUPS, channels, HIGH), jnp.bfloat16),
            vmem((GROUPS, channels, HIGH), jnp.float32),
            vmem((listed, atoms), jnp.int32),
            vmem((listed, atoms), jnp.int32),
            vmem((listed, channels, atoms), jnp.bfloat16),
            vmem((listed, 8, atoms), jnp.float32),
            vmem((listed, count, atoms), jnp.float32),
            vmem((listed, channels, atoms), jnp.float32),
            vmem((GROUPS * ROWS, HIGH), jnp.float32),
        ],
        interpret=interpret,
        name="short_range",
    )(table, ids, pos, dy, radial, mix, gain)


def from_behind(x, axis, by):
    devices = lax.axis_size(axis)
    return lax.ppermute(x, axis, [(i, (i + by) % devices) for i in range(devices)])


def chosen(parity):
    column = lax.broadcasted_iota(jnp.int32, (2 * CHUNK, CHUNK), 1)
    row = lax.broadcasted_iota(jnp.int32, (2 * CHUNK, CHUNK), 0)
    picked = (column // SHARE) * (2 * SHARE) + column % SHARE + parity * SHARE
    return (row == picked).astype(jnp.float32).astype(jnp.bfloat16)


def pack_kernel(h_ref, kind_ref, pos_ref, miller_ref, table_ref, mine_ref, next_ref):
    f32, bf16 = jnp.float32, jnp.bfloat16
    _, atoms = h_ref.shape
    none = jnp.zeros((1, atoms), f32)
    halves = [split_two(pos_ref[d]) for d in range(3)]
    rows = jnp.concatenate(
        [h_ref[...].astype(f32)]
        + [half[0].astype(f32) for half in halves]
        + [none]
        + [half[1].astype(f32) for half in halves]
        + [none, kind_ref[...].astype(f32), jnp.zeros((127 - ROWS, atoms), f32)],
        axis=0,
    )
    table_ref[...] = jnp.transpose(rows).astype(bf16)
    m = miller_ref[...].astype(f32)
    tall = jnp.concatenate([m, m, m, jnp.zeros((7, m.shape[1]), f32)], axis=0).astype(bf16)
    runs = m.shape[1] // (2 * CHUNK)
    stack = jnp.concatenate(
        [tall[:, j * 2 * CHUNK : (j + 1) * 2 * CHUNK] for j in range(runs)], axis=0
    )
    core = lax.axis_index(PAIR)
    for parity, out_ref in ((core, mine_ref), (1 - core, next_ref)):
        got = jnp.dot(stack, chosen(parity), preferred_element_type=f32).astype(bf16)
        for j in range(runs):
            out_ref[:, j * CHUNK : (j + 1) * CHUNK] = got[j * 16 : (j + 1) * 16]


def pack(h, kinds, pos, miller):
    half = jax.ShapeDtypeStruct((16, miller.shape[1] // 2), jnp.bfloat16)
    return pl.pallas_call(
        pack_kernel,
        out_shape=(jax.ShapeDtypeStruct((h.shape[1], 128), jnp.bfloat16), half, half),
        in_specs=[WHOLE] * 4,
        out_specs=(WHOLE,) * 3,
        name="pack",
    )(h, kinds, pos, miller)


def phase_kernel(
    pos_ref,
    miller_ref,
    h_ref,
    dy_ref,
    cos_out,
    sin_out,
    part_ref,
    cos_ref,
    sin_ref,
    flip_ref,
    rhs_ref,
    t_ref,
    sems,
):
    f32, bf16 = jnp.float32, jnp.bfloat16
    width = 2 * h_ref.shape[0]
    flip_ref[...] = jnp.transpose(jnp.concatenate([h_ref[...], dy_ref[...]], axis=0))
    axes = ("gx", GY, GZ)
    turns = jnp.concatenate(
        [
            (pos_ref[d] + lax.axis_index(axes[d]).astype(f32)) / float(lax.axis_size(axes[d]))
            for d in range(3)
        ],
        axis=0,
    )
    t_hi = turns.astype(bf16)
    t_mid, t_lo = split_two(turns - t_hi.astype(f32))
    rhs_ref[...] = jnp.concatenate(
        [t_hi, t_mid, t_lo, jnp.zeros((7, turns.shape[1]), bf16)], axis=0
    )
    steps = miller_ref.shape[1] // CHUNK
    rows, lanes = 16, 256

    def copies(i):
        at = pl.ds(pl.multiple_of(i * CHUNK, CHUNK), CHUNK)
        return [
            pltpu.make_async_copy(src.at[at], dst.at[at], sems.at[n, i])
            for n, (src, dst) in enumerate(
                ((cos_ref, cos_out), (sin_ref, sin_out))
            )
        ]

    def one(i, carry):
        base = pl.multiple_of(i * CHUNK, CHUNK)
        t_ref[...] = lax.dot_general(
            miller_ref[:, pl.ds(base, CHUNK)],
            rhs_ref[...],
            (((0,), (0,)), ((), ())),
            preferred_element_type=f32,
        )
        for top in range(0, CHUNK, rows):
            for left in range(0, t_ref.shape[1], lanes):
                t = t_ref[top : top + rows, left : left + lanes]
                r = t - jnp.round(t)
                u = jnp.abs(r) - 0.25
                q = u * u
                s = SIN_TERMS[3]
                for term in SIN_TERMS[2::-1]:
                    s = s * q + term
                c = COS_TERMS[4]
                for term in COS_TERMS[3::-1]:
                    c = c * q + term
                at = (pl.ds(base + top, rows), pl.ds(left, lanes))
                cos_ref[at] = -(s * u).astype(bf16)
                sin_ref[at] = jnp.where(r < 0.0, -c, c).astype(bf16)
        here = pl.ds(base, CHUNK)
        part_ref[here, 0:width] = jnp.dot(
            cos_ref[here, :], flip_ref[...], preferred_element_type=f32
        )
        part_ref[here, width:] = jnp.dot(
            sin_ref[here, :], flip_ref[...], preferred_element_type=f32
        )
        for copy in copies(i):
            copy.start()
        return carry

    lax.fori_loop(0, steps, one, 0)
    for i in range(steps):
        for copy in copies(i):
            copy.wait()


def phase_sums(pos, miller, h, dy):
    points = miller.shape[1]
    channels, atoms = h.shape
    width = 2 * channels
    wave = jax.ShapeDtypeStruct((points, atoms), jnp.bfloat16)
    sums = jax.ShapeDtypeStruct((points, 2 * width), jnp.float32)
    return pl.pallas_call(
        phase_kernel,
        out_shape=(wave, wave, sums),
        in_specs=[WHOLE] * 4,
        out_specs=(pl.BlockSpec(memory_space=pl.ANY),) * 2 + (WHOLE,),
        scratch_shapes=[
            pltpu.VMEM(wave.shape, wave.dtype),
            pltpu.VMEM(wave.shape, wave.dtype),
            pltpu.VMEM((atoms, width), jnp.bfloat16),
            pltpu.VMEM((16, atoms), jnp.bfloat16),
            pltpu.VMEM((CHUNK, atoms), jnp.float32),
            pltpu.SemaphoreType.DMA((2, points // CHUNK)),
        ],
        cost_estimate=pl.CostEstimate(
            flops=6 * points * atoms * width, transcendentals=0, bytes_accessed=4 * points * atoms
        ),
        name="phase_sums",
    )(pos, miller, h, dy)


def ewald_kernel(last, coeff_in, cos_in, sin_in, miller_ref, h_ref, dy_ref, *rest):
    f32, bf16 = jnp.float32, jnp.bfloat16
    channels = h_ref.shape[0]
    width = 2 * channels
    coeff_ref, cos_ref, sin_ref, both_ref, sems = rest[-5:]
    steps = miller_ref.shape[1] // CHUNK

    def copies(i):
        at = pl.ds(pl.multiple_of(i * CHUNK, CHUNK), CHUNK)
        return [
            pltpu.make_async_copy(coeff_in.at[i, pl.ds(0, CHUNK)], coeff_ref.at[at], sems.at[0, i]),
            pltpu.make_async_copy(cos_in.at[at], cos_ref.at[at], sems.at[1, i]),
            pltpu.make_async_copy(sin_in.at[at], sin_ref.at[at], sems.at[2, i]),
        ]

    for i in range(steps):
        for copy in copies(i):
            copy.start()
    both_ref[...] = jnp.concatenate([h_ref[...], dy_ref[...]], axis=0)
    if last:
        sums_ref, turn_ref = rest[-7:-5]
        first_ref, angle_ref, grid_ref, upper_ref, lower_ref = rest[0:5]
        core_ref, own_ref, all_ref, kind_ref, gain_ref, mix_ref = rest[5:11]
        inner = [
            grid_ref[:, :, 1] + lower_ref[:, :, 0].astype(f32),
            grid_ref[:, :, 2],
            grid_ref[:, :, 3] + upper_ref[:, :, 0].astype(f32),
        ]
        cells = jnp.stack(inner, axis=2).reshape(432, 128)
        flat = jnp.transpose(jnp.concatenate([cells, core_ref[...]], axis=0))
        gains = gains_of(gain_ref[...], kind_ref[...], (channels, flat.shape[1]))
        zscaled = (flat[0:channels] * gains).astype(bf16)
        halves = flat[channels : channels + 8]
        near = halves + pltpu.roll(halves, 4, 0) + own_ref[...]
        sums_ref[...] = first_ref[...] + jnp.dot(
            mix_ref[...], zscaled, preferred_element_type=f32
        )
        turn_ref[...] = angle_ref[...]
    else:
        sums_ref, turn_ref = rest[0:2]
        sums_ref[...] = jnp.zeros_like(sums_ref)
        turn_ref[...] = jnp.zeros_like(turn_ref)
    over_rows = (((0,), (0,)), ((), ()))

    def one(i, carry):
        for copy in copies(i):
            copy.wait()
        at = pl.ds(pl.multiple_of(i * CHUNK, CHUNK), CHUNK)
        coeffs = coeff_ref[at, :]
        cos_part, sin_part = cos_ref[at, :], sin_ref[at, :]
        sums_ref[...] += lax.dot_general(
            coeffs[:, 0:channels], cos_part, over_rows, preferred_element_type=f32
        ) + lax.dot_general(
            coeffs[:, width : width + channels], sin_part, over_rows, preferred_element_type=f32
        )
        along_u = jnp.dot(coeffs[:, 0:width], both_ref[...], preferred_element_type=f32)
        along_v = jnp.dot(coeffs[:, width : 2 * width], both_ref[...], preferred_element_type=f32)
        angle = along_v * cos_part.astype(f32) - along_u * sin_part.astype(f32)
        a_hi, a_lo = split_two(angle)
        m = miller_ref[:, at]
        turn_ref[...] += jnp.dot(m, a_hi, preferred_element_type=f32) + jnp.dot(
            m, a_lo, preferred_element_type=f32
        )
        return carry

    lax.fori_loop(0, steps, one, 0)
    if last:
        atom_ref, pos_ref, weight_ref, radial_ref = rest[11:15]
        atom_ref[...] = (dy_ref[...].astype(f32) + sums_ref[...]).astype(bf16)
        axes = ("gx", GY, GZ)
        for d in range(3):
            pos_ref[d] = (
                turn_ref[d : d + 1, :] * (circle_angle / lax.axis_size(axes[d]))
                + near[d : d + 1, :]
            )
        weight_ref[...] = all_ref[0:channels, 0:channels]
        radial_ref[...] = all_ref[channels : channels + radial_ref.shape[0], 0:channels]


def ewald(coeffs, cos_all, sin_all, miller, h, dy, more=(), basis=0):
    points, atoms = cos_all.shape
    channels = h.shape[0]
    last = len(more) > 0
    sums = jax.ShapeDtypeStruct((channels, atoms), jnp.float32)
    turn = jax.ShapeDtypeStruct((16, atoms), jnp.float32)
    scratch = [
        pltpu.VMEM((points, 4 * channels), jnp.bfloat16),
        pltpu.VMEM(cos_all.shape, jnp.bfloat16),
        pltpu.VMEM(cos_all.shape, jnp.bfloat16),
        pltpu.VMEM((2 * channels, atoms), jnp.bfloat16),
        pltpu.SemaphoreType.DMA((3, points // CHUNK)),
    ]
    outs = (sums, turn)
    if last:
        scratch = [pltpu.VMEM(sums.shape, sums.dtype), pltpu.VMEM(turn.shape, turn.dtype)] + scratch
        outs = (
            jax.ShapeDtypeStruct(sums.shape, jnp.bfloat16),
            jax.ShapeDtypeStruct((3, 1, atoms), jnp.float32),
            jax.ShapeDtypeStruct((channels, channels), jnp.float32),
            jax.ShapeDtypeStruct((basis, channels), jnp.float32),
        )
    return pl.pallas_call(
        functools.partial(ewald_kernel, last),
        out_shape=outs,
        in_specs=[pl.BlockSpec(memory_space=pl.ANY)] * 3 + [WHOLE] * (3 + len(more)),
        out_specs=(WHOLE,) * len(outs),
        scratch_shapes=scratch,
        cost_estimate=pl.CostEstimate(
            flops=8 * points * atoms * channels,
            transcendentals=0,
            bytes_accessed=4 * points * atoms,
        ),
        name="ewald",
    )(coeffs, cos_all, sin_all, miller, h, dy, *more)


def coefficients(totals, filt_rows, norm_atoms, norm_k):
    channels = filt_rows.shape[1]
    cos_struct = totals[:, 0:channels] * norm_atoms
    cos_back = totals[:, channels : 2 * channels] * norm_k
    sin_struct = totals[:, 2 * channels : 3 * channels] * norm_atoms
    sin_back = totals[:, 3 * channels : 4 * channels] * norm_k
    coeffs = jnp.concatenate(
        [
            norm_atoms * filt_rows * cos_back,
            norm_k * filt_rows * cos_struct,
            norm_atoms * filt_rows * sin_back,
            norm_k * filt_rows * sin_struct,
        ],
        axis=1,
    )
    return (coeffs.astype(jnp.bfloat16), cos_struct * cos_back + sin_struct * sin_back)


def sent_out(x, axis, dim):
    length = x.shape[dim]
    before = from_behind(lax.slice_in_dim(x, length - 1, length, axis=dim), axis, 1)
    after = from_behind(lax.slice_in_dim(x, 0, 1, axis=dim), axis, -1)
    return before, after


def sent_back(x, axis, dim):
    length = x.shape[dim]
    first = lax.slice_in_dim(x, 0, 1, axis=dim).astype(jnp.bfloat16)
    last = lax.slice_in_dim(x, length - 1, length, axis=dim).astype(jnp.bfloat16)
    return from_behind(first, axis, -1), from_behind(last, axis, 1)


def folded(x, pieces, dim):
    to_last, to_first = [piece.astype(jnp.float32) for piece in pieces]
    low = lax.slice_in_dim(x, 1, 2, axis=dim) + to_first
    middle = lax.slice_in_dim(x, 2, 3, axis=dim)
    high = lax.slice_in_dim(x, 3, 4, axis=dim) + to_last
    return jnp.concatenate([low, middle, high], axis=dim)


def whole(
    atom_embedding,
    output_adjoint,
    fractional_coords,
    element_labels,
    adjacent_ghost_entries,
    miller_triples,
    reciprocal_kernel,
    channel_mixing_matrix,
    element_channel_factor,
    distance_kernel,
):
    h = atom_embedding[0, 0, 0]
    dy = output_adjoint[0, 0, 0]
    pos = fractional_coords[0, 0, 0][:, None, :]
    kinds = element_labels[0, 0]
    channels, atoms = h.shape
    points = miller_triples.shape[1]
    devices = lax.axis_size(GX_GY_GZ)
    norm_atoms = (atoms * devices) ** (-0.5)
    norm_k = points ** (-0.5)
    share_rows = points // devices
    share_start = lax.axis_index(GX_GY_GZ) * share_rows
    groups = lax.axis_size(CHIPS)

    own_table, miller_mine, miller_next = pack(h, kinds, pos, miller_triples)
    cells = own_table[0:432].reshape(3, 3, 3, 16, 128)
    below, above = sent_out(cells, GZ, 2)
    cos_next, sin_next, part_next = phase_sums(pos, miller_next, h, dy)
    received = from_behind(part_next, PAIR, 1)
    cells = jnp.concatenate([below, cells, above], axis=2)
    below, above = sent_out(cells, GY, 1)
    cos_mine, sin_mine, part_mine = phase_sums(pos, miller_mine, h, dy)
    cells = jnp.concatenate([below, cells, above], axis=1)
    below, above = sent_out(cells, "gx", 0)
    paired = (part_mine + received).astype(jnp.bfloat16)
    pieces = lax.all_to_all(paired.reshape(groups, share_rows, 4 * channels), CHIPS, 0, 0)

    table = jnp.concatenate(
        [
            below.reshape(400, 128),
            cells.reshape(1200, 128),
            above.reshape(400, 128),
            own_table[432:512],
            jnp.zeros((GROUPS * HIGH - 2080, 128), jnp.bfloat16),
        ],
        axis=0,
    )
    ghost_grad, ghost_thin, own_grad, sums = short_range(
        table,
        adjacent_ghost_entries[0, 0, 0],
        pos,
        dy,
        distance_kernel,
        channel_mixing_matrix,
        element_channel_factor,
    )
    sums = sums + from_behind(sums, PAIR, 1)
    tiles = sums.astype(jnp.bfloat16).reshape(16, 1, 8, 128)
    tiles = jnp.broadcast_to(tiles, (16, 2, 8, 128)).reshape(32, 8, 128)

    totals = jnp.sum(pieces.astype(jnp.float32), axis=0)
    filt_rows = lax.dynamic_slice_in_dim(reciprocal_kernel, share_start, share_rows, 0)
    own_coeffs, filter_share = coefficients(totals, filt_rows, norm_atoms, norm_k)
    spread = jnp.broadcast_to(own_coeffs[None], (32, share_rows, 4 * channels))
    got = lax.all_to_all(jnp.concatenate([spread, tiles], axis=2), PLANE, 0, 0)

    grid = ghost_grad[0:2000].reshape(5, 5, 5, 16, 128)
    to_side = sent_back(ghost_thin[0:2000].reshape(5, 5, 5, 16, 128), "gx", 0)
    grid = folded(grid, to_side, 0)
    to_side = sent_back(grid, GY, 1)

    tile_part = jnp.sum(got[:, :, 4 * channels :].astype(jnp.float32), axis=0)
    lines = lax.axis_size("gx")
    strip = jnp.concatenate(
        [
            got[:, :, 0 : 4 * channels].reshape(32 * share_rows, 4 * channels),
            jnp.concatenate(
                [tile_part.astype(jnp.bfloat16), jnp.zeros((8, 128), jnp.bfloat16)], axis=1
            ),
        ],
        axis=0,
    )
    got = lax.all_to_all(jnp.broadcast_to(strip[None], (lines,) + strip.shape), "gx", 0, 0)
    grid = folded(grid, to_side, 1)
    to_side = sent_back(grid, GZ, 2)
    tile_sum = jnp.sum(got[:, 32 * share_rows :, 0:128].astype(jnp.float32), axis=0)
    got_next = from_behind(got, PAIR, 1)
    every = lax.all_to_all(jnp.broadcast_to(tile_sum[None], (16, 8, 128)), GY, 0, 0)
    every = every.reshape(128, 128)
    first = ewald(got, cos_mine, sin_mine, miller_mine, h, dy)
    atom_grad, position_grad, weight_grad, radial_grad = ewald(
        got_next,
        cos_next,
        sin_next,
        miller_next,
        h,
        dy,
        (
            *first,
            grid,
            *to_side,
            ghost_grad[2000:2080],
            own_grad,
            every,
            kinds,
            element_channel_factor,
            channel_mixing_matrix,
        ),
        distance_kernel.shape[0],
    )
    position_grad = position_grad[:, 0, :]
    return (
        atom_grad[None, None, None],
        position_grad[None, None, None],
        weight_grad,
        radial_grad,
        filter_share,
    )


def solution(mesh):
    finer = Mesh(
        mesh.devices.reshape(mesh.shape["gx"], 4, 4, 2, 2), ("gx", "gy_0", "gy_1", "gz_0", "gz_1")
    )
    in_specs = (
        P("gx", GY, GZ, None, None),
        P("gx", GY, GZ, None, None),
        P("gx", GY, GZ, None, None),
        P("gx", GY, GZ, None),
        P("gx", GY, GZ, None, None),
        P(),
        P(),
        P(),
        P(),
        P(),
    )
    out_specs = (
        P("gx", GY, GZ, None, None),
        P("gx", GY, GZ, None, None),
        P(),
        P(),
        P(GX_GY_GZ, None),
    )
    return jax.shard_map(whole, mesh=finer, in_specs=in_specs, out_specs=out_specs, check_vma=False)
```

```python
import functools
import math

import jax
import jax.numpy as jnp
from jax import lax
from jax.experimental import pallas as pl
from jax.experimental.pallas import tpu as pltpu
from jax.sharding import Mesh
from jax.sharding import PartitionSpec as P


GY = ("gy_0", "gy_1")
GZ = ("gz_0", "gz_1")

SHEET = ("gx", "gy_1")
TOWER = ("gy_0", "gz_0")
PAIR = "gz_1"
GX_GY_GZ = ("gx", "gy_0", "gy_1", "gz_0", "gz_1")

circle_angle = 2.0 * math.pi
CHUNK = 256
SHARE = 8
SIN_TERMS = (6.28316404, -41.33714227, 81.34076528, -70.99339569)
COS_TERMS = (0.99999995, -19.73917143, 64.93459054, -85.24032775, 56.2423573)
WHOLE = pl.BlockSpec(memory_space=pltpu.VMEM)

reach_sq = 0.75
GROUPS = 9
ROWS = 72
BLOCKS = 135
HIGH = BLOCKS // GROUPS * 16


def split_two(x):
    high = x.astype(jnp.bfloat16)
    return high, (x - high.astype(jnp.float32)).astype(jnp.bfloat16)


def row_pick(first, second, third, shape):
    row = lax.broadcasted_iota(jnp.int32, shape, 0) % 4
    spread = lambda v: jnp.broadcast_to(v, shape)
    return jnp.where(
        row == 0,
        spread(first),
        jnp.where(row == 1, spread(second), jnp.where(row == 2, spread(third), 0.0)),
    )


def gains_of(gain_rows, labels, shape):
    columns = jnp.transpose(gain_rows)
    gains = jnp.zeros(shape, jnp.float32)
    for kind in range(gain_rows.shape[0]):
        gains = jnp.where(labels == kind, columns[:, kind : kind + 1], gains)
    return gains


def short_kernel(
    below_ref,
    cells_ref,
    above_ref,
    core_ref,
    ids_ref,
    pos_ref,
    dy_ref,
    radial_ref,
    mix_ref,
    gain_ref,
    low_out,
    mid_out,
    high_out,
    core_out,
    own_ref,
    sums_ref,
    lhs_ref,
    feat_ref,
    gains_ref,
    high_ref,
    low_ref,
    near_ref,
    rel_ref,
    basis_ref,
    filt_ref,
    acc_ref,
    table_ref,
    zgrad_ref,
):
    channels, atoms = dy_ref.shape
    side, inner, rest = below_ref.shape[0], cells_ref.shape[0], core_ref.shape[0]
    bounds = (0, side, side + inner, 2 * side + inner, 2 * side + inner + rest)
    for n, ref in enumerate((below_ref, cells_ref, above_ref, core_ref)):
        table_ref[bounds[n] : bounds[n + 1], :] = ref[...]
    table_ref[bounds[4] :, :] = jnp.zeros((GROUPS * HIGH - bounds[4], 128), jnp.bfloat16)
    listed = ids_ref.shape[0]
    count = radial_ref.shape[0]
    f32, bf16 = jnp.float32, jnp.bfloat16
    spacing = reach_sq / (count - 1)
    width = 2.0 * spacing
    share = listed ** (-0.5)
    for g in range(GROUPS):
        part = jnp.transpose(table_ref[g * HIGH : (g + 1) * HIGH, :].astype(f32))
        feat = part[0:channels].astype(bf16)
        gains = gains_of(gain_ref[...], part[ROWS : ROWS + 1], (channels, HIGH))
        feat_ref[g] = feat
        gains_ref[g] = gains
        z = lax.dot_general(
            mix_ref[...], feat, (((0,), (0,)), ((), ())), preferred_element_type=f32
        )
        lhs_ref[g * ROWS : (g + 1) * ROWS, :] = jnp.concatenate(
            [z * gains, part[channels:ROWS]], axis=0
        ).astype(bf16)
    ids = ids_ref[...]
    slot = lax.shift_right_logical(ids, 9)
    atom = jnp.bitwise_and(ids, 511)
    block = lax.shift_right_logical(atom, 4)
    ox = slot // 9
    oy = (slot // 3) % 3
    oz = slot % 3
    qx = block // 9
    qy = (block // 3) % 3
    qz = block % 3
    grid = ((3 * ox + qx - 2) * 5 + 3 * oy + qy - 2) * 5 + 3 * oz + qz - 2
    grid = jnp.where(block >= 27, block + (125 - 27), grid)
    low = grid // (BLOCKS // GROUPS)
    high = (grid - low * (BLOCKS // GROUPS)) * 16 + jnp.bitwise_and(atom, 15)
    high_ref[...] = high
    low_ref[...] = low
    offs = [(o - 1).astype(f32) for o in (ox, oy, oz)]
    own8 = row_pick(pos_ref[0], pos_ref[1], pos_ref[2], (8, atoms))
    w_hi, w_lo = split_two(radial_ref[...])
    w_stack = jnp.concatenate([w_hi, w_hi, w_lo], axis=0)
    centre = lax.broadcasted_iota(jnp.int32, (count, 1), 0).astype(f32) * spacing
    iota = lax.broadcasted_iota(jnp.int32, (HIGH, atoms), 0)

    def hot(j):
        return (high_ref[pl.ds(j, 1), :] == iota).astype(f32).astype(bf16)

    agg = jnp.zeros((channels, atoms), f32)
    for j in range(listed):
        found = jnp.dot(lhs_ref[...], hot(j), preferred_element_type=f32)
        low_j = low_ref[j : j + 1, :]
        near = found[0:ROWS]
        for g in range(1, GROUPS):
            near = jnp.where(low_j == g, found[g * ROWS : (g + 1) * ROWS], near)
        near_z = near[0:channels]
        near_ref[j] = near_z.astype(bf16)
        halves = near[channels : channels + 8]
        off8 = row_pick(offs[0][j : j + 1], offs[1][j : j + 1], offs[2][j : j + 1], (8, atoms))
        rel = halves + pltpu.roll(halves, 4, 0) + off8 - own8
        rel_ref[j] = rel
        dist = 0.5 * jnp.sum(rel * rel, axis=0, keepdims=True)
        scaled = (dist - centre) / width
        basis = jnp.exp(-(scaled * scaled))
        basis_ref[j] = basis
        b_hi, b_lo = split_two(basis)
        filt = lax.dot_general(
            w_stack,
            jnp.concatenate([b_hi, b_lo, b_hi], axis=0),
            (((0,), (0,)), ((), ())),
            preferred_element_type=f32,
        )
        filt_ref[j] = filt
        agg = agg + filt * near_z
    agg = agg * share
    gate = 1.0 / (1.0 + jnp.exp(-agg))
    g_all = dy_ref[...].astype(f32) * (gate * (1.0 + agg * (1.0 - gate))) * share
    acc_ref[...] = jnp.zeros_like(acc_ref)
    own_grad = jnp.zeros((8, atoms), f32)
    radial = jnp.zeros((2 * count, 2 * channels), f32)
    w_wide = jnp.concatenate([w_hi, w_hi, w_lo], axis=1)
    for j in range(listed):
        near_z = near_ref[j].astype(f32)
        dz = filt_ref[j] * g_all
        df = near_z * g_all
        f_hi, f_lo = split_two(df)
        basis = basis_ref[j]
        b_hi, b_lo = split_two(basis)
        radial = radial + lax.dot_general(
            jnp.concatenate([b_hi, b_lo], axis=0),
            jnp.concatenate([f_hi, f_lo], axis=0),
            (((1,), (1,)), ((), ())),
            preferred_element_type=f32,
        )
        dbasis = jnp.dot(
            w_wide, jnp.concatenate([f_hi, f_lo, f_hi], axis=0), preferred_element_type=f32
        )
        rel = rel_ref[j]
        dist = 0.5 * jnp.sum(rel * rel, axis=0, keepdims=True)
        slope = dbasis * basis * (dist - centre)
        ddist = jnp.sum(slope, axis=0, keepdims=True) * (-2.0 / (width * width))
        gpos = rel * (2.0 * ddist)
        own_grad = own_grad - gpos
        p_hi = gpos.astype(bf16).astype(f32)
        row8 = lax.broadcasted_iota(jnp.int32, (8, atoms), 0)
        tail = jnp.where(row8 < 4, p_hi, gpos - p_hi)
        full = jnp.concatenate([dz, tail], axis=0)
        low_j = low_ref[j : j + 1, :]
        spread = jnp.concatenate(
            [jnp.where(low_j == g, full, 0.0) for g in range(GROUPS)], axis=0
        ).astype(bf16)
        acc_ref[...] += lax.dot_general(
            spread, hot(j), (((1,), (1,)), ((), ())), preferred_element_type=f32
        )
    own_ref[...] = own_grad
    sums_ref[...] = jnp.zeros_like(sums_ref)
    radial = (
        radial[0:count, 0:channels]
        + radial[count:, 0:channels]
        + radial[0:count, channels:]
        + radial[count:, channels:]
    )
    weight = jnp.zeros((channels, channels), f32)
    for g in range(GROUPS):
        z_hi, z_lo = split_two(acc_ref[g * ROWS : g * ROWS + channels, :] * gains_ref[g])
        for piece in (z_hi, z_lo):
            weight = weight + lax.dot_general(
                feat_ref[g], piece, (((1,), (1,)), ((), ())), preferred_element_type=f32
            )
        part = jnp.transpose(acc_ref[g * ROWS : (g + 1) * ROWS, :])
        part = jnp.concatenate([part, jnp.zeros((HIGH, 128 - ROWS), f32)], axis=1)
        zgrad_ref[g * HIGH : (g + 1) * HIGH, :] = part
    for n, (ref, kind) in enumerate(
        ((low_out, bf16), (mid_out, f32), (high_out, bf16), (core_out, f32))
    ):
        ref[...] = zgrad_ref[bounds[n] : bounds[n + 1], :].astype(kind)
    tall = jnp.concatenate([weight, radial], axis=0)
    cut = (channels + count) // 2
    sums_ref[0:cut, :] = jnp.concatenate([tall[0:cut], tall[cut:]], axis=1)


def short_range(pieces, ids, pos, dy, radial, mix, gain, interpret=False):
    channels, atoms = dy.shape
    listed = ids.shape[0]
    count = radial.shape[0]
    vmem = lambda s, d: pltpu.VMEM(s, d)
    spec = pl.BlockSpec(memory_space=pltpu.VMEM)
    return pl.pallas_call(
        short_kernel,
        out_shape=(
            jax.ShapeDtypeStruct(pieces[0].shape, jnp.bfloat16),
            jax.ShapeDtypeStruct(pieces[1].shape, jnp.float32),
            jax.ShapeDtypeStruct(pieces[2].shape, jnp.bfloat16),
            jax.ShapeDtypeStruct(pieces[3].shape, jnp.float32),
            jax.ShapeDtypeStruct((8, atoms), jnp.float32),
            jax.ShapeDtypeStruct((64, 128), jnp.float32),
        ),
        in_specs=[spec] * 10,
        out_specs=(spec,) * 6,
        scratch_shapes=[
            vmem((GROUPS * ROWS, HIGH), jnp.bfloat16),
            vmem((GROUPS, channels, HIGH), jnp.bfloat16),
            vmem((GROUPS, channels, HIGH), jnp.float32),
            vmem((listed, atoms), jnp.int32),
            vmem((listed, atoms), jnp.int32),
            vmem((listed, channels, atoms), jnp.bfloat16),
            vmem((listed, 8, atoms), jnp.float32),
            vmem((listed, count, atoms), jnp.float32),
            vmem((listed, channels, atoms), jnp.float32),
            vmem((GROUPS * ROWS, HIGH), jnp.float32),
            vmem((GROUPS * HIGH, 128), jnp.bfloat16),
            vmem((GROUPS * HIGH, 128), jnp.float32),
        ],
        interpret=interpret,
        name="short_range",
    )(*pieces, ids, pos, dy, radial, mix, gain)


def from_behind(x, axis, by):
    devices = lax.axis_size(axis)
    return lax.ppermute(x, axis, [(i, (i + by) % devices) for i in range(devices)])


def chosen(parity):
    column = lax.broadcasted_iota(jnp.int32, (2 * CHUNK, CHUNK), 1)
    row = lax.broadcasted_iota(jnp.int32, (2 * CHUNK, CHUNK), 0)
    n = column // SHARE
    outer, inner, least = [lax.axis_size(axis) for axis in ("gy_0", "gy_1", "gz_0")]
    group = ((n // least) % outer * inner + n // (least * outer)) * least + n % least
    picked = group * (2 * SHARE) + column % SHARE + parity * SHARE
    return (row == picked).astype(jnp.float32).astype(jnp.bfloat16)


def pack_kernel(h_ref, kind_ref, pos_ref, miller_ref, cells_ref, core_ref, mine_ref, next_ref):
    f32, bf16 = jnp.float32, jnp.bfloat16
    _, atoms = h_ref.shape
    none = jnp.zeros((1, atoms), f32)
    halves = [split_two(pos_ref[d]) for d in range(3)]
    rows = jnp.concatenate(
        [h_ref[...].astype(f32)]
        + [half[0].astype(f32) for half in halves]
        + [none]
        + [half[1].astype(f32) for half in halves]
        + [none, kind_ref[...].astype(f32), jnp.zeros((127 - ROWS, atoms), f32)],
        axis=0,
    )
    flat = jnp.transpose(rows).astype(bf16)
    cells_ref[...] = flat[0 : cells_ref.shape[0]]
    core_ref[...] = flat[cells_ref.shape[0] :]
    m = miller_ref[...].astype(f32)
    tall = jnp.concatenate([m, m, m, jnp.zeros((7, m.shape[1]), f32)], axis=0).astype(bf16)
    runs = m.shape[1] // (2 * CHUNK)
    stack = jnp.concatenate(
        [tall[:, j * 2 * CHUNK : (j + 1) * 2 * CHUNK] for j in range(runs)], axis=0
    )
    core = lax.axis_index(PAIR)
    for parity, out_ref in ((core, mine_ref), (1 - core, next_ref)):
        got = jnp.dot(stack, chosen(parity), preferred_element_type=f32).astype(bf16)
        for j in range(runs):
            out_ref[:, j * CHUNK : (j + 1) * CHUNK] = got[j * 16 : (j + 1) * 16]


def pack(h, kinds, pos, miller):
    half = jax.ShapeDtypeStruct((16, miller.shape[1] // 2), jnp.bfloat16)
    return pl.pallas_call(
        pack_kernel,
        out_shape=(
            jax.ShapeDtypeStruct((432, 128), jnp.bfloat16),
            jax.ShapeDtypeStruct((h.shape[1] - 432, 128), jnp.bfloat16),
            half,
            half,
        ),
        in_specs=[WHOLE] * 4,
        out_specs=(WHOLE,) * 4,
        name="pack",
    )(h, kinds, pos, miller)


def phase_kernel(
    pos_ref,
    miller_ref,
    h_ref,
    dy_ref,
    cos_out,
    sin_out,
    part_ref,
    cos_ref,
    sin_ref,
    flip_ref,
    rhs_ref,
    t_ref,
    sems,
):
    f32, bf16 = jnp.float32, jnp.bfloat16
    width = 2 * h_ref.shape[0]
    flip_ref[...] = jnp.transpose(jnp.concatenate([h_ref[...], dy_ref[...]], axis=0))
    axes = ("gx", GY, GZ)
    turns = jnp.concatenate(
        [
            (pos_ref[d] + lax.axis_index(axes[d]).astype(f32)) / float(lax.axis_size(axes[d]))
            for d in range(3)
        ],
        axis=0,
    )
    t_hi = turns.astype(bf16)
    t_mid, t_lo = split_two(turns - t_hi.astype(f32))
    rhs_ref[...] = jnp.concatenate(
        [t_hi, t_mid, t_lo, jnp.zeros((7, turns.shape[1]), bf16)], axis=0
    )
    steps = miller_ref.shape[1] // CHUNK
    rows, lanes = 16, 256

    def copies(i):
        at = pl.ds(pl.multiple_of(i * CHUNK, CHUNK), CHUNK)
        return [
            pltpu.make_async_copy(src.at[at], dst.at[at], sems.at[n, i])
            for n, (src, dst) in enumerate(
                ((cos_ref, cos_out), (sin_ref, sin_out))
            )
        ]

    def one(i, carry):
        base = pl.multiple_of(i * CHUNK, CHUNK)
        t_ref[...] = lax.dot_general(
            miller_ref[:, pl.ds(base, CHUNK)],
            rhs_ref[...],
            (((0,), (0,)), ((), ())),
            preferred_element_type=f32,
        )
        for top in range(0, CHUNK, rows):
            for left in range(0, t_ref.shape[1], lanes):
                t = t_ref[top : top + rows, left : left + lanes]
                r = t - jnp.round(t)
                u = jnp.abs(r) - 0.25
                q = u * u
                s = SIN_TERMS[3]
                for term in SIN_TERMS[2::-1]:
                    s = s * q + term
                c = COS_TERMS[4]
                for term in COS_TERMS[3::-1]:
                    c = c * q + term
                at = (pl.ds(base + top, rows), pl.ds(left, lanes))
                cos_ref[at] = -(s * u).astype(bf16)
                sin_ref[at] = jnp.where(r < 0.0, -c, c).astype(bf16)
        here = pl.ds(base, CHUNK)
        part_ref[here, 0:width] = jnp.dot(
            cos_ref[here, :], flip_ref[...], preferred_element_type=f32
        )
        part_ref[here, width:] = jnp.dot(
            sin_ref[here, :], flip_ref[...], preferred_element_type=f32
        )
        for copy in copies(i):
            copy.start()
        return carry

    lax.fori_loop(0, steps, one, 0)
    for i in range(steps):
        for copy in copies(i):
            copy.wait()


def phase_sums(pos, miller, h, dy):
    points = miller.shape[1]
    channels, atoms = h.shape
    width = 2 * channels
    wave = jax.ShapeDtypeStruct((points, atoms), jnp.bfloat16)
    sums = jax.ShapeDtypeStruct((points, 2 * width), jnp.float32)
    return pl.pallas_call(
        phase_kernel,
        out_shape=(wave, wave, sums),
        in_specs=[WHOLE] * 4,
        out_specs=(pl.BlockSpec(memory_space=pl.ANY),) * 2 + (WHOLE,),
        scratch_shapes=[
            pltpu.VMEM(wave.shape, wave.dtype),
            pltpu.VMEM(wave.shape, wave.dtype),
            pltpu.VMEM((atoms, width), jnp.bfloat16),
            pltpu.VMEM((16, atoms), jnp.bfloat16),
            pltpu.VMEM((CHUNK, atoms), jnp.float32),
            pltpu.SemaphoreType.DMA((2, points // CHUNK)),
        ],
        cost_estimate=pl.CostEstimate(
            flops=6 * points * atoms * width, transcendentals=0, bytes_accessed=4 * points * atoms
        ),
        name="phase_sums",
    )(pos, miller, h, dy)


def ewald_kernel(last, coeff_in, cos_in, sin_in, miller_ref, h_ref, dy_ref, *rest):
    f32, bf16 = jnp.float32, jnp.bfloat16
    channels = h_ref.shape[0]
    width = 2 * channels
    coeff_ref, cos_ref, sin_ref, both_ref, sems = rest[-5:]
    steps = miller_ref.shape[1] // CHUNK
    run = coeff_ref.shape[1]
    few = CHUNK // run

    def copies(i):
        at = pl.ds(pl.multiple_of(i * CHUNK, CHUNK), CHUNK)
        return [
            pltpu.make_async_copy(
                coeff_in.at[pl.ds(i * few, few), pl.ds(0, run)],
                coeff_ref.at[pl.ds(i * few, few)],
                sems.at[0, i],
            ),
            pltpu.make_async_copy(cos_in.at[at], cos_ref.at[at], sems.at[1, i]),
            pltpu.make_async_copy(sin_in.at[at], sin_ref.at[at], sems.at[2, i]),
        ]

    for i in range(steps):
        for copy in copies(i):
            copy.start()
    both_ref[...] = jnp.concatenate([h_ref[...], dy_ref[...]], axis=0)
    if last:
        sums_ref, turn_ref = rest[-7:-5]
        first_ref, angle_ref, *planes, upper_ref, lower_ref = rest[0:7]
        core_ref, own_ref, all_ref, kind_ref, gain_ref, mix_ref = rest[7:13]
        cells = jnp.stack(
            [
                jnp.stack(
                    [
                        plane[:, 0, 1] + lower_ref[:, n, 0].astype(f32),
                        plane[:, 0, 2],
                        plane[:, 0, 3] + upper_ref[:, n, 0].astype(f32),
                    ],
                    axis=1,
                )
                for n, plane in enumerate(planes)
            ],
            axis=1,
        ).reshape(432, 128)
        flat = jnp.transpose(jnp.concatenate([cells, core_ref[...]], axis=0))
        gains = gains_of(gain_ref[...], kind_ref[...], (channels, flat.shape[1]))
        zscaled = (flat[0:channels] * gains).astype(bf16)
        halves = flat[channels : channels + 8]
        near = halves + pltpu.roll(halves, 4, 0) + own_ref[...]
        sums_ref[...] = first_ref[...] + jnp.dot(
            mix_ref[...], zscaled, preferred_element_type=f32
        )
        turn_ref[...] = angle_ref[...]
    else:
        sums_ref, turn_ref = rest[0:2]
        sums_ref[...] = jnp.zeros_like(sums_ref)
        turn_ref[...] = jnp.zeros_like(turn_ref)
    over_rows = (((0,), (0,)), ((), ()))

    def one(i, carry):
        for copy in copies(i):
            copy.wait()
        at = pl.ds(pl.multiple_of(i * CHUNK, CHUNK), CHUNK)
        coeffs = coeff_ref[pl.ds(i * few, few)].reshape(CHUNK, 2 * width)
        cos_part, sin_part = cos_ref[at, :], sin_ref[at, :]
        sums_ref[...] += lax.dot_general(
            coeffs[:, 0:channels], cos_part, over_rows, preferred_element_type=f32
        ) + lax.dot_general(
            coeffs[:, width : width + channels], sin_part, over_rows, preferred_element_type=f32
        )
        along_u = jnp.dot(coeffs[:, 0:width], both_ref[...], preferred_element_type=f32)
        along_v = jnp.dot(coeffs[:, width : 2 * width], both_ref[...], preferred_element_type=f32)
        angle = along_v * cos_part.astype(f32) - along_u * sin_part.astype(f32)
        a_hi, a_lo = split_two(angle)
        m = miller_ref[:, at]
        turn_ref[...] += jnp.dot(m, a_hi, preferred_element_type=f32) + jnp.dot(
            m, a_lo, preferred_element_type=f32
        )
        return carry

    lax.fori_loop(0, steps, one, 0)
    if last:
        atom_ref, pos_ref, weight_ref, radial_ref = rest[13:17]
        atom_ref[...] = (dy_ref[...].astype(f32) + sums_ref[...]).astype(bf16)
        axes = ("gx", GY, GZ)
        for d in range(3):
            pos_ref[d] = (
                turn_ref[d : d + 1, :] * (circle_angle / lax.axis_size(axes[d]))
                + near[d : d + 1, :]
            )
        full = jnp.sum(all_ref[...], axis=1).reshape(64, 128)
        cut = (channels + radial_ref.shape[0]) // 2
        tall = jnp.concatenate([full[0:cut, 0:channels], full[0:cut, channels:]], axis=0)
        weight_ref[...] = tall[0:channels]
        radial_ref[...] = tall[channels:]


def ewald(coeffs, cos_all, sin_all, miller, h, dy, more=(), basis=0):
    points, atoms = cos_all.shape
    channels = h.shape[0]
    last = len(more) > 0
    lines = coeffs.shape[0]
    sums = jax.ShapeDtypeStruct((channels, atoms), jnp.float32)
    turn = jax.ShapeDtypeStruct((16, atoms), jnp.float32)
    scratch = [
        pltpu.VMEM((lines, points // lines, 4 * channels), jnp.bfloat16),
        pltpu.VMEM(cos_all.shape, jnp.bfloat16),
        pltpu.VMEM(cos_all.shape, jnp.bfloat16),
        pltpu.VMEM((2 * channels, atoms), jnp.bfloat16),
        pltpu.SemaphoreType.DMA((3, points // CHUNK)),
    ]
    outs = (sums, turn)
    if last:
        scratch = [pltpu.VMEM(sums.shape, sums.dtype), pltpu.VMEM(turn.shape, turn.dtype)] + scratch
        outs = (
            jax.ShapeDtypeStruct(sums.shape, jnp.bfloat16),
            jax.ShapeDtypeStruct((3, 1, atoms), jnp.float32),
            jax.ShapeDtypeStruct((channels, channels), jnp.float32),
            jax.ShapeDtypeStruct((basis, channels), jnp.float32),
        )
    return pl.pallas_call(
        functools.partial(ewald_kernel, last),
        out_shape=outs,
        in_specs=[pl.BlockSpec(memory_space=pl.ANY)] * 3 + [WHOLE] * (3 + len(more)),
        out_specs=(WHOLE,) * len(outs),
        scratch_shapes=scratch,
        cost_estimate=pl.CostEstimate(
            flops=8 * points * atoms * channels,
            transcendentals=0,
            bytes_accessed=4 * points * atoms,
        ),
        name="ewald",
    )(coeffs, cos_all, sin_all, miller, h, dy, *more)


def coefficients(totals, filt_rows, norm_atoms, norm_k):
    channels = filt_rows.shape[1]
    cos_struct = totals[:, 0:channels] * norm_atoms
    cos_back = totals[:, channels : 2 * channels] * norm_k
    sin_struct = totals[:, 2 * channels : 3 * channels] * norm_atoms
    sin_back = totals[:, 3 * channels : 4 * channels] * norm_k
    coeffs = jnp.concatenate(
        [
            norm_atoms * filt_rows * cos_back,
            norm_k * filt_rows * cos_struct,
            norm_atoms * filt_rows * sin_back,
            norm_k * filt_rows * sin_struct,
        ],
        axis=1,
    )
    return (coeffs.astype(jnp.bfloat16), cos_struct * cos_back + sin_struct * sin_back)


def sent_out(x, axis, dim):
    length = x.shape[dim]
    before = from_behind(lax.slice_in_dim(x, length - 1, length, axis=dim), axis, 1)
    after = from_behind(lax.slice_in_dim(x, 0, 1, axis=dim), axis, -1)
    return before, after


def sent_back(x, axis, dim):
    length = x.shape[dim]
    first = lax.slice_in_dim(x, 0, 1, axis=dim).astype(jnp.bfloat16)
    last = lax.slice_in_dim(x, length - 1, length, axis=dim).astype(jnp.bfloat16)
    return from_behind(first, axis, -1), from_behind(last, axis, 1)


def whole(
    atom_embedding,
    output_adjoint,
    fractional_coords,
    element_labels,
    adjacent_ghost_entries,
    miller_triples,
    reciprocal_kernel,
    channel_mixing_matrix,
    element_channel_factor,
    distance_kernel,
):
    h = atom_embedding[0, 0, 0]
    dy = output_adjoint[0, 0, 0]
    pos = fractional_coords[0, 0, 0][:, None, :]
    kinds = element_labels[0, 0]
    channels, atoms = h.shape
    points = miller_triples.shape[1]
    devices = lax.axis_size(GX_GY_GZ)
    norm_atoms = (atoms * devices) ** (-0.5)
    norm_k = points ** (-0.5)
    share_rows = points // devices
    share_start = lax.axis_index(GX_GY_GZ) * share_rows
    half = points // 2

    cells, core, miller_mine, miller_next = pack(h, kinds, pos, miller_triples)
    cells = cells.reshape(3, 3, 3, 16, 128)
    below, above = sent_out(cells, GZ, 2)
    cos_next, sin_next, part_next = phase_sums(pos, miller_next, h, dy)
    received = from_behind(part_next, PAIR, 1)
    cells = jnp.concatenate([below, cells, above], axis=2)
    below, above = sent_out(cells, GY, 1)
    cos_mine, sin_mine, part_mine = phase_sums(pos, miller_mine, h, dy)
    cells = jnp.concatenate([below, cells, above], axis=1)
    below, above = sent_out(cells, "gx", 0)
    sheet, tower = lax.axis_size(SHEET), lax.axis_size(TOWER)
    width = 4 * channels
    paired = (part_mine + received).astype(jnp.bfloat16)
    pieces = lax.all_to_all(paired.reshape(sheet, half // sheet, width), SHEET, 0, 0)

    low, mid, high, core_grad, own_grad, sums = short_range(
        (below.reshape(400, 128), cells.reshape(1200, 128), above.reshape(400, 128), core),
        adjacent_ghost_entries[0, 0, 0],
        pos,
        dy,
        distance_kernel,
        channel_mixing_matrix,
        element_channel_factor,
    )
    sums_hi = lax.reduce_precision(sums, 8, 7)
    tiles = jnp.concatenate([sums_hi, sums - sums_hi], axis=1).astype(jnp.bfloat16)
    tiles = tiles.reshape(tower, 8, 256)

    partial = jnp.sum(pieces.astype(jnp.float32), axis=0).astype(jnp.bfloat16)
    pieces = lax.all_to_all(partial.reshape(tower, share_rows, width), TOWER, 0, 0)
    totals = jnp.sum(pieces.astype(jnp.float32), axis=0)
    filt_rows = lax.dynamic_slice_in_dim(reciprocal_kernel, share_start, share_rows, 0)
    own_coeffs, filter_share = coefficients(totals, filt_rows, norm_atoms, norm_k)
    spread = jnp.broadcast_to(own_coeffs[None], (tower, share_rows, width))
    got = lax.all_to_all(jnp.concatenate([spread, tiles], axis=2), TOWER, 0, 0)

    grid = mid.reshape(3, 5, 5, 16, 128)
    to_side = (
        from_behind(low.reshape(1, 5, 5, 16, 128), "gx", -1),
        from_behind(high.reshape(1, 5, 5, 16, 128), "gx", 1),
    )
    grid = jnp.concatenate(
        [
            grid[0:1] + to_side[1].astype(jnp.float32),
            grid[1:2],
            grid[2:3] + to_side[0].astype(jnp.float32),
        ],
        axis=0,
    )
    to_side = sent_back(grid, GY, 1)

    tile_part = jnp.sum(got[:, :, width:].astype(jnp.float32), axis=0)
    tile_part = tile_part[:, 0:128] + tile_part[:, 128:256]
    part_hi = lax.reduce_precision(tile_part, 8, 7)
    strip = jnp.concatenate(
        [
            got[:, :, 0:width].reshape(tower * share_rows, width),
            jnp.concatenate([part_hi, tile_part - part_hi], axis=1).astype(jnp.bfloat16),
        ],
        axis=0,
    )
    got = lax.all_to_all(jnp.broadcast_to(strip[None], (sheet,) + strip.shape), SHEET, 0, 0)
    planes = (
        grid[:, 1:2] + to_side[1].astype(jnp.float32),
        grid[:, 2:3],
        grid[:, 3:4] + to_side[0].astype(jnp.float32),
    )
    to_side = tuple(
        from_behind(
            jnp.concatenate([p[:, :, at : at + 1].astype(jnp.bfloat16) for p in planes], axis=1),
            GZ,
            by,
        )
        for at, by in ((0, -1), (4, 1))
    )
    tile_sum = jnp.sum(got[:, tower * share_rows :].astype(jnp.float32), axis=0)
    tile_sum = tile_sum[:, 0:128] + tile_sum[:, 128:256]
    got_next = from_behind(got, PAIR, 1)
    every = lax.all_to_all(
        jnp.broadcast_to(tile_sum[None], (2 * tower, 8, 128)), TOWER + (PAIR,), 0, 0
    )
    every = every.reshape(tower, 2, 8, 128)
    first = ewald(got, cos_mine, sin_mine, miller_mine, h, dy)
    atom_grad, position_grad, weight_grad, radial_grad = ewald(
        got_next,
        cos_next,
        sin_next,
        miller_next,
        h,
        dy,
        (
            *first,
            *planes,
            *to_side,
            core_grad,
            own_grad,
            every,
            kinds,
            element_channel_factor,
            channel_mixing_matrix,
        ),
        distance_kernel.shape[0],
    )
    position_grad = position_grad[:, 0, :]
    return (
        atom_grad[None, None, None],
        position_grad[None, None, None],
        weight_grad,
        radial_grad,
        filter_share,
    )


def solution(mesh):
    finer = Mesh(
        mesh.devices.reshape(mesh.shape["gx"], 4, 4, 2, 2), ("gx", "gy_0", "gy_1", "gz_0", "gz_1")
    )
    in_specs = (
        P("gx", GY, GZ, None, None),
        P("gx", GY, GZ, None, None),
        P("gx", GY, GZ, None, None),
        P("gx", GY, GZ, None),
        P("gx", GY, GZ, None, None),
        P(),
        P(),
        P(),
        P(),
        P(),
    )
    out_specs = (
        P("gx", GY, GZ, None, None),
        P("gx", GY, GZ, None, None),
        P(),
        P(),
        P(GX_GY_GZ, None),
    )
    return jax.shard_map(whole, mesh=finer, in_specs=in_specs, out_specs=out_specs, check_vma=False)
```

```python
import functools
import math

import jax
import jax.numpy as jnp
from jax import lax
from jax.experimental import pallas as pl
from jax.experimental.pallas import tpu as pltpu
from jax.sharding import Mesh
from jax.sharding import PartitionSpec as P


GY = ("gy_0", "gy_1")
GZ = ("gz_0", "gz_1")

SHEET = ("gx", "gy_1")
TOWER = ("gy_0", "gz_0")
PAIR = "gz_1"
GX_GY_GZ = ("gx", "gy_0", "gy_1", "gz_0", "gz_1")

circle_angle = 2.0 * math.pi
CHUNK = 256
SHARE = 8
SIN_TERMS = (6.28316404, -41.33714227, 81.34076528, -70.99339569)
COS_TERMS = (0.99999995, -19.73917143, 64.93459054, -85.24032775, 56.2423573)
WHOLE = pl.BlockSpec(memory_space=pltpu.VMEM)
LIMIT = pltpu.CompilerParams(vmem_limit_bytes=20 * 1024 * 1024)

reach_sq = 0.75
GROUPS = 9
ROWS = 72
BLOCKS = 135
HIGH = BLOCKS // GROUPS * 16


def split_two(x):
    high = x.astype(jnp.bfloat16)
    return high, (x - high.astype(jnp.float32)).astype(jnp.bfloat16)


def row_pick(first, second, third, shape):
    row = lax.broadcasted_iota(jnp.int32, shape, 0) % 4
    spread = lambda v: jnp.broadcast_to(v, shape)
    return jnp.where(
        row == 0,
        spread(first),
        jnp.where(row == 1, spread(second), jnp.where(row == 2, spread(third), 0.0)),
    )


def gains_of(gain_rows, labels, shape):
    columns = jnp.transpose(gain_rows)
    gains = jnp.zeros(shape, jnp.float32)
    for kind in range(gain_rows.shape[0]):
        gains = jnp.where(labels == kind, columns[:, kind : kind + 1], gains)
    return gains


def short_kernel(
    below_ref,
    cells_ref,
    above_ref,
    core_ref,
    ids_ref,
    pos_ref,
    dy_ref,
    radial_ref,
    mix_ref,
    gain_ref,
    low_out,
    mid_out,
    high_out,
    core_out,
    own_ref,
    sums_ref,
    lhs_ref,
    feat_ref,
    gains_ref,
    high_ref,
    low_ref,
    near_ref,
    rel_ref,
    basis_ref,
    filt_ref,
    acc_ref,
    table_ref,
    zgrad_ref,
):
    channels, atoms = dy_ref.shape
    side, inner, rest = below_ref.shape[0], cells_ref.shape[0], core_ref.shape[0]
    bounds = (0, side, side + inner, 2 * side + inner, 2 * side + inner + rest)
    for n, ref in enumerate((below_ref, cells_ref, above_ref, core_ref)):
        table_ref[bounds[n] : bounds[n + 1], :] = ref[...]
    table_ref[bounds[4] :, :] = jnp.zeros((GROUPS * HIGH - bounds[4], 128), jnp.bfloat16)
    listed = ids_ref.shape[0]
    count = radial_ref.shape[0]
    f32, bf16 = jnp.float32, jnp.bfloat16
    spacing = reach_sq / (count - 1)
    width = 2.0 * spacing
    share = listed ** (-0.5)
    for g in range(GROUPS):
        part = jnp.transpose(table_ref[g * HIGH : (g + 1) * HIGH, :].astype(f32))
        feat = part[0:channels].astype(bf16)
        gains = gains_of(gain_ref[...], part[ROWS : ROWS + 1], (channels, HIGH))
        feat_ref[g] = feat
        gains_ref[g] = gains
        z = lax.dot_general(
            mix_ref[...], feat, (((0,), (0,)), ((), ())), preferred_element_type=f32
        )
        lhs_ref[g * ROWS : (g + 1) * ROWS, :] = jnp.concatenate(
            [z * gains, part[channels:ROWS]], axis=0
        ).astype(bf16)
    ids = ids_ref[...]
    slot = lax.shift_right_logical(ids, 9)
    atom = jnp.bitwise_and(ids, 511)
    block = lax.shift_right_logical(atom, 4)
    ox = slot // 9
    oy = (slot // 3) % 3
    oz = slot % 3
    qx = block // 9
    qy = (block // 3) % 3
    qz = block % 3
    grid = ((3 * ox + qx - 2) * 5 + 3 * oy + qy - 2) * 5 + 3 * oz + qz - 2
    grid = jnp.where(block >= 27, block + (125 - 27), grid)
    low = grid // (BLOCKS // GROUPS)
    high = (grid - low * (BLOCKS // GROUPS)) * 16 + jnp.bitwise_and(atom, 15)
    high_ref[...] = high
    low_ref[...] = low
    offs = [(o - 1).astype(f32) for o in (ox, oy, oz)]
    own8 = row_pick(pos_ref[0], pos_ref[1], pos_ref[2], (8, atoms))
    w_hi, w_lo = split_two(radial_ref[...])
    w_stack = jnp.concatenate([w_hi, w_hi, w_lo], axis=0)
    centre = lax.broadcasted_iota(jnp.int32, (count, 1), 0).astype(f32) * spacing
    iota = lax.broadcasted_iota(jnp.int32, (HIGH, atoms), 0)

    def hot(j):
        return (high_ref[pl.ds(j, 1), :] == iota).astype(f32).astype(bf16)

    agg = jnp.zeros((channels, atoms), f32)
    for j in range(listed):
        found = jnp.dot(lhs_ref[...], hot(j), preferred_element_type=f32)
        low_j = low_ref[j : j + 1, :]
        near = found[0:ROWS]
        for g in range(1, GROUPS):
            near = jnp.where(low_j == g, found[g * ROWS : (g + 1) * ROWS], near)
        near_z = near[0:channels]
        near_ref[j] = near_z.astype(bf16)
        halves = near[channels : channels + 8]
        off8 = row_pick(offs[0][j : j + 1], offs[1][j : j + 1], offs[2][j : j + 1], (8, atoms))
        rel = halves + pltpu.roll(halves, 4, 0) + off8 - own8
        rel_ref[j] = rel
        dist = 0.5 * jnp.sum(rel * rel, axis=0, keepdims=True)
        scaled = (dist - centre) / width
        basis = jnp.exp(-(scaled * scaled))
        basis_ref[j] = basis
        b_hi, b_lo = split_two(basis)
        filt = lax.dot_general(
            w_stack,
            jnp.concatenate([b_hi, b_lo, b_hi], axis=0),
            (((0,), (0,)), ((), ())),
            preferred_element_type=f32,
        )
        filt_ref[j] = filt
        agg = agg + filt * near_z
    agg = agg * share
    gate = 1.0 / (1.0 + jnp.exp(-agg))
    g_all = dy_ref[...].astype(f32) * (gate * (1.0 + agg * (1.0 - gate))) * share
    acc_ref[...] = jnp.zeros_like(acc_ref)
    own_grad = jnp.zeros((8, atoms), f32)
    radial = jnp.zeros((2 * count, 2 * channels), f32)
    w_wide = jnp.concatenate([w_hi, w_hi, w_lo], axis=1)
    for j in range(listed):
        near_z = near_ref[j].astype(f32)
        dz = filt_ref[j] * g_all
        df = near_z * g_all
        f_hi, f_lo = split_two(df)
        basis = basis_ref[j]
        b_hi, b_lo = split_two(basis)
        radial = radial + lax.dot_general(
            jnp.concatenate([b_hi, b_lo], axis=0),
            jnp.concatenate([f_hi, f_lo], axis=0),
            (((1,), (1,)), ((), ())),
            preferred_element_type=f32,
        )
        dbasis = jnp.dot(
            w_wide, jnp.concatenate([f_hi, f_lo, f_hi], axis=0), preferred_element_type=f32
        )
        rel = rel_ref[j]
        dist = 0.5 * jnp.sum(rel * rel, axis=0, keepdims=True)
        slope = dbasis * basis * (dist - centre)
        ddist = jnp.sum(slope, axis=0, keepdims=True) * (-2.0 / (width * width))
        gpos = rel * (2.0 * ddist)
        own_grad = own_grad - gpos
        p_hi = gpos.astype(bf16).astype(f32)
        row8 = lax.broadcasted_iota(jnp.int32, (8, atoms), 0)
        tail = jnp.where(row8 < 4, p_hi, gpos - p_hi)
        full = jnp.concatenate([dz, tail], axis=0)
        low_j = low_ref[j : j + 1, :]
        spread = jnp.concatenate(
            [jnp.where(low_j == g, full, 0.0) for g in range(GROUPS)], axis=0
        ).astype(bf16)
        acc_ref[...] += lax.dot_general(
            spread, hot(j), (((1,), (1,)), ((), ())), preferred_element_type=f32
        )
    own_ref[...] = own_grad
    sums_ref[...] = jnp.zeros_like(sums_ref)
    radial = (
        radial[0:count, 0:channels]
        + radial[count:, 0:channels]
        + radial[0:count, channels:]
        + radial[count:, channels:]
    )
    weight = jnp.zeros((channels, channels), f32)
    for g in range(GROUPS):
        z_hi, z_lo = split_two(acc_ref[g * ROWS : g * ROWS + channels, :] * gains_ref[g])
        for piece in (z_hi, z_lo):
            weight = weight + lax.dot_general(
                feat_ref[g], piece, (((1,), (1,)), ((), ())), preferred_element_type=f32
            )
        part = jnp.transpose(acc_ref[g * ROWS : (g + 1) * ROWS, :])
        part = jnp.concatenate([part, jnp.zeros((HIGH, 128 - ROWS), f32)], axis=1)
        zgrad_ref[g * HIGH : (g + 1) * HIGH, :] = part
    for n, (ref, kind) in enumerate(
        ((low_out, bf16), (mid_out, f32), (high_out, bf16), (core_out, f32))
    ):
        ref[...] = zgrad_ref[bounds[n] : bounds[n + 1], :].astype(kind)
    tall = jnp.concatenate([weight, radial], axis=0)
    cut = (channels + count) // 2
    sums_ref[0:cut, :] = jnp.concatenate([tall[0:cut], tall[cut:]], axis=1)


def short_range(pieces, ids, pos, dy, radial, mix, gain, interpret=False):
    channels, atoms = dy.shape
    listed = ids.shape[0]
    count = radial.shape[0]
    vmem = lambda s, d: pltpu.VMEM(s, d)
    spec = pl.BlockSpec(memory_space=pltpu.VMEM)
    return pl.pallas_call(
        short_kernel,
        out_shape=(
            jax.ShapeDtypeStruct(pieces[0].shape, jnp.bfloat16),
            jax.ShapeDtypeStruct(pieces[1].shape, jnp.float32),
            jax.ShapeDtypeStruct(pieces[2].shape, jnp.bfloat16),
            jax.ShapeDtypeStruct(pieces[3].shape, jnp.float32),
            jax.ShapeDtypeStruct((8, atoms), jnp.float32),
            jax.ShapeDtypeStruct((128, 128), jnp.float32),
        ),
        in_specs=[spec] * 10,
        out_specs=(spec,) * 6,
        scratch_shapes=[
            vmem((GROUPS * ROWS, HIGH), jnp.bfloat16),
            vmem((GROUPS, channels, HIGH), jnp.bfloat16),
            vmem((GROUPS, channels, HIGH), jnp.float32),
            vmem((listed, atoms), jnp.int32),
            vmem((listed, atoms), jnp.int32),
            vmem((listed, channels, atoms), jnp.bfloat16),
            vmem((listed, 8, atoms), jnp.float32),
            vmem((listed, count, atoms), jnp.float32),
            vmem((listed, channels, atoms), jnp.float32),
            vmem((GROUPS * ROWS, HIGH), jnp.float32),
            vmem((GROUPS * HIGH, 128), jnp.bfloat16),
            vmem((GROUPS * HIGH, 128), jnp.float32),
        ],
        interpret=interpret,
        compiler_params=LIMIT,
        name="short_range",
    )(*pieces, ids, pos, dy, radial, mix, gain)


def from_behind(x, axis, by):
    devices = lax.axis_size(axis)
    return lax.ppermute(x, axis, [(i, (i + by) % devices) for i in range(devices)])


def chosen(parity):
    column = lax.broadcasted_iota(jnp.int32, (2 * CHUNK, CHUNK), 1)
    row = lax.broadcasted_iota(jnp.int32, (2 * CHUNK, CHUNK), 0)
    n = column // SHARE
    inner, least = [lax.axis_size(axis) for axis in ("gy_1", "gz_0")]
    level = n // inner
    group = (level // least * inner + n % inner) * least + level % least
    picked = group * (2 * SHARE) + column % SHARE + parity * SHARE
    return (row == picked).astype(jnp.float32).astype(jnp.bfloat16)


def pack_kernel(h_ref, kind_ref, pos_ref, miller_ref, cells_ref, core_ref, mine_ref, next_ref):
    f32, bf16 = jnp.float32, jnp.bfloat16
    _, atoms = h_ref.shape
    none = jnp.zeros((1, atoms), f32)
    halves = [split_two(pos_ref[d]) for d in range(3)]
    rows = jnp.concatenate(
        [h_ref[...].astype(f32)]
        + [half[0].astype(f32) for half in halves]
        + [none]
        + [half[1].astype(f32) for half in halves]
        + [none, kind_ref[...].astype(f32), jnp.zeros((127 - ROWS, atoms), f32)],
        axis=0,
    )
    flat = jnp.transpose(rows).astype(bf16)
    cells_ref[...] = flat[0 : cells_ref.shape[0]]
    core_ref[...] = flat[cells_ref.shape[0] :]
    m = miller_ref[...].astype(f32)
    tall = jnp.concatenate([m, m, m, jnp.zeros((7, m.shape[1]), f32)], axis=0).astype(bf16)
    runs = m.shape[1] // (2 * CHUNK)
    stack = jnp.concatenate(
        [tall[:, j * 2 * CHUNK : (j + 1) * 2 * CHUNK] for j in range(runs)], axis=0
    )
    core = lax.axis_index(PAIR)
    for parity, out_ref in ((core, mine_ref), (1 - core, next_ref)):
        got = jnp.dot(stack, chosen(parity), preferred_element_type=f32).astype(bf16)
        tower = lax.axis_size(TOWER)
        wide = CHUNK // tower
        out_ref[...] = jnp.concatenate(
            [
                got[j * 16 : (j + 1) * 16, w * wide : (w + 1) * wide]
                for w in range(tower)
                for j in range(runs)
            ],
            axis=1,
        )


def pack(h, kinds, pos, miller):
    half = jax.ShapeDtypeStruct((16, miller.shape[1] // 2), jnp.bfloat16)
    return pl.pallas_call(
        pack_kernel,
        out_shape=(
            jax.ShapeDtypeStruct((432, 128), jnp.bfloat16),
            jax.ShapeDtypeStruct((h.shape[1] - 432, 128), jnp.bfloat16),
            half,
            half,
        ),
        in_specs=[WHOLE] * 4,
        out_specs=(WHOLE,) * 4,
        compiler_params=LIMIT,
        name="pack",
    )(h, kinds, pos, miller)


def phase_kernel(
    pos_ref,
    miller_ref,
    h_ref,
    dy_ref,
    cos_out,
    sin_out,
    part_ref,
    cos_ref,
    sin_ref,
    flip_ref,
    rhs_ref,
    t_ref,
    sems,
):
    f32, bf16 = jnp.float32, jnp.bfloat16
    width = 2 * h_ref.shape[0]
    flip_ref[...] = jnp.transpose(jnp.concatenate([h_ref[...], dy_ref[...]], axis=0))
    axes = ("gx", GY, GZ)
    turns = jnp.concatenate(
        [
            (pos_ref[d] + lax.axis_index(axes[d]).astype(f32)) / float(lax.axis_size(axes[d]))
            for d in range(3)
        ],
        axis=0,
    )
    t_hi = turns.astype(bf16)
    t_mid, t_lo = split_two(turns - t_hi.astype(f32))
    rhs_ref[...] = jnp.concatenate(
        [t_hi, t_mid, t_lo, jnp.zeros((7, turns.shape[1]), bf16)], axis=0
    )
    steps = miller_ref.shape[1] // CHUNK
    rows, lanes = 16, 256

    def copies(i):
        at = pl.ds(pl.multiple_of(i * CHUNK, CHUNK), CHUNK)
        return [
            pltpu.make_async_copy(src.at[at], dst.at[at], sems.at[n, i])
            for n, (src, dst) in enumerate(
                ((cos_ref, cos_out), (sin_ref, sin_out))
            )
        ]

    def one(i, carry):
        base = pl.multiple_of(i * CHUNK, CHUNK)
        t_ref[...] = lax.dot_general(
            miller_ref[:, pl.ds(base, CHUNK)],
            rhs_ref[...],
            (((0,), (0,)), ((), ())),
            preferred_element_type=f32,
        )
        for top in range(0, CHUNK, rows):
            for left in range(0, t_ref.shape[1], lanes):
                t = t_ref[top : top + rows, left : left + lanes]
                r = t - jnp.round(t)
                u = jnp.abs(r) - 0.25
                q = u * u
                s = SIN_TERMS[3]
                for term in SIN_TERMS[2::-1]:
                    s = s * q + term
                c = COS_TERMS[4]
                for term in COS_TERMS[3::-1]:
                    c = c * q + term
                at = (pl.ds(base + top, rows), pl.ds(left, lanes))
                cos_ref[at] = -(s * u).astype(bf16)
                sin_ref[at] = jnp.where(r < 0.0, -c, c).astype(bf16)
        here = pl.ds(base, CHUNK)
        part_ref[here, 0:width] = jnp.dot(
            cos_ref[here, :], flip_ref[...], preferred_element_type=f32
        ).astype(part_ref.dtype)
        part_ref[here, width:] = jnp.dot(
            sin_ref[here, :], flip_ref[...], preferred_element_type=f32
        ).astype(part_ref.dtype)
        for copy in copies(i):
            copy.start()
        return carry

    lax.fori_loop(0, steps, one, 0)
    for i in range(steps):
        for copy in copies(i):
            copy.wait()


def phase_sums(pos, miller, h, dy):
    points = miller.shape[1]
    channels, atoms = h.shape
    width = 2 * channels
    wave = jax.ShapeDtypeStruct((points, atoms), jnp.bfloat16)
    sums = jax.ShapeDtypeStruct((points, 2 * width), jnp.bfloat16)
    return pl.pallas_call(
        phase_kernel,
        out_shape=(wave, wave, sums),
        in_specs=[WHOLE] * 4,
        out_specs=(pl.BlockSpec(memory_space=pl.ANY),) * 2 + (WHOLE,),
        scratch_shapes=[
            pltpu.VMEM(wave.shape, wave.dtype),
            pltpu.VMEM(wave.shape, wave.dtype),
            pltpu.VMEM((atoms, width), jnp.bfloat16),
            pltpu.VMEM((16, atoms), jnp.bfloat16),
            pltpu.VMEM((CHUNK, atoms), jnp.float32),
            pltpu.SemaphoreType.DMA((2, points // CHUNK)),
        ],
        cost_estimate=pl.CostEstimate(
            flops=6 * points * atoms * width, transcendentals=0, bytes_accessed=4 * points * atoms
        ),
        compiler_params=LIMIT,
        name="phase_sums",
    )(pos, miller, h, dy)


def ewald_kernel(last, coeff_in, cos_in, sin_in, miller_ref, h_ref, dy_ref, *rest):
    f32, bf16 = jnp.float32, jnp.bfloat16
    channels = h_ref.shape[0]
    width = 2 * channels
    coeff_ref, cos_ref, sin_ref, both_ref, sems = rest[-5:]
    steps = miller_ref.shape[1] // CHUNK
    run = coeff_ref.shape[1]
    few = CHUNK // run

    def copies(i):
        at = pl.ds(pl.multiple_of(i * CHUNK, CHUNK), CHUNK)
        return [
            pltpu.make_async_copy(
                coeff_in.at[pl.ds(i * few, few), pl.ds(0, run)],
                coeff_ref.at[pl.ds(i * few, few)],
                sems.at[0, i],
            ),
            pltpu.make_async_copy(cos_in.at[at], cos_ref.at[at], sems.at[1, i]),
            pltpu.make_async_copy(sin_in.at[at], sin_ref.at[at], sems.at[2, i]),
        ]

    for i in range(steps):
        for copy in copies(i):
            copy.start()
    both_ref[...] = jnp.concatenate([h_ref[...], dy_ref[...]], axis=0)
    if last:
        sums_ref, turn_ref = rest[-7:-5]
        first_ref, angle_ref, *planes, upper_ref, lower_ref = rest[0:7]
        core_ref, own_ref, all_ref, kind_ref, gain_ref, mix_ref = rest[7:13]
        cells = jnp.stack(
            [
                jnp.stack(
                    [
                        plane[:, 0, 1] + lower_ref[:, n, 0].astype(f32),
                        plane[:, 0, 2],
                        plane[:, 0, 3] + upper_ref[:, n, 0].astype(f32),
                    ],
                    axis=1,
                )
                for n, plane in enumerate(planes)
            ],
            axis=1,
        ).reshape(432, 128)
        flat = jnp.transpose(jnp.concatenate([cells, core_ref[...]], axis=0))
        gains = gains_of(gain_ref[...], kind_ref[...], (channels, flat.shape[1]))
        zscaled = (flat[0:channels] * gains).astype(bf16)
        halves = flat[channels : channels + 8]
        near = halves + pltpu.roll(halves, 4, 0) + own_ref[...]
        sums_ref[...] = first_ref[...] + jnp.dot(
            mix_ref[...], zscaled, preferred_element_type=f32
        )
        turn_ref[...] = angle_ref[...]
    else:
        sums_ref, turn_ref = rest[0:2]
        sums_ref[...] = jnp.zeros_like(sums_ref)
        turn_ref[...] = jnp.zeros_like(turn_ref)
    over_rows = (((0,), (0,)), ((), ()))

    def one(i, carry):
        for copy in copies(i):
            copy.wait()
        at = pl.ds(pl.multiple_of(i * CHUNK, CHUNK), CHUNK)
        coeffs = coeff_ref[pl.ds(i * few, few)].reshape(CHUNK, 2 * width)
        cos_part, sin_part = cos_ref[at, :], sin_ref[at, :]
        sums_ref[...] += lax.dot_general(
            coeffs[:, 0:channels], cos_part, over_rows, preferred_element_type=f32
        ) + lax.dot_general(
            coeffs[:, width : width + channels], sin_part, over_rows, preferred_element_type=f32
        )
        along_u = jnp.dot(coeffs[:, 0:width], both_ref[...], preferred_element_type=f32)
        along_v = jnp.dot(coeffs[:, width : 2 * width], both_ref[...], preferred_element_type=f32)
        angle = along_v * cos_part.astype(f32) - along_u * sin_part.astype(f32)
        a_hi, a_lo = split_two(angle)
        m = miller_ref[:, at]
        turn_ref[...] += jnp.dot(m, a_hi, preferred_element_type=f32) + jnp.dot(
            m, a_lo, preferred_element_type=f32
        )
        return carry

    lax.fori_loop(0, steps, one, 0)
    if last:
        atom_ref, pos_ref, weight_ref, radial_ref = rest[13:17]
        atom_ref[...] = (dy_ref[...].astype(f32) + sums_ref[...]).astype(bf16)
        axes = ("gx", GY, GZ)
        for d in range(3):
            pos_ref[d] = (
                turn_ref[d : d + 1, :] * (circle_angle / lax.axis_size(axes[d]))
                + near[d : d + 1, :]
            )
        full = jnp.sum(all_ref[...], axis=1).reshape(128, 128)
        cut = (channels + radial_ref.shape[0]) // 2
        tall = jnp.concatenate([full[0:cut, 0:channels], full[0:cut, channels:]], axis=0)
        weight_ref[...] = tall[0:channels]
        radial_ref[...] = tall[channels:]


def ewald(coeffs, cos_all, sin_all, miller, h, dy, more=(), basis=0):
    points, atoms = cos_all.shape
    channels = h.shape[0]
    last = len(more) > 0
    lines = coeffs.shape[0]
    sums = jax.ShapeDtypeStruct((channels, atoms), jnp.float32)
    turn = jax.ShapeDtypeStruct((16, atoms), jnp.float32)
    scratch = [
        pltpu.VMEM((lines, points // lines, 4 * channels), jnp.bfloat16),
        pltpu.VMEM(cos_all.shape, jnp.bfloat16),
        pltpu.VMEM(cos_all.shape, jnp.bfloat16),
        pltpu.VMEM((2 * channels, atoms), jnp.bfloat16),
        pltpu.SemaphoreType.DMA((3, points // CHUNK)),
    ]
    outs = (sums, turn)
    if last:
        scratch = [pltpu.VMEM(sums.shape, sums.dtype), pltpu.VMEM(turn.shape, turn.dtype)] + scratch
        outs = (
            jax.ShapeDtypeStruct(sums.shape, jnp.bfloat16),
            jax.ShapeDtypeStruct((3, 1, atoms), jnp.float32),
            jax.ShapeDtypeStruct((channels, channels), jnp.float32),
            jax.ShapeDtypeStruct((basis, channels), jnp.float32),
        )
    return pl.pallas_call(
        functools.partial(ewald_kernel, last),
        out_shape=outs,
        in_specs=[pl.BlockSpec(memory_space=pl.ANY)] * 3 + [WHOLE] * (3 + len(more)),
        out_specs=(WHOLE,) * len(outs),
        scratch_shapes=scratch,
        cost_estimate=pl.CostEstimate(
            flops=8 * points * atoms * channels,
            transcendentals=0,
            bytes_accessed=4 * points * atoms,
        ),
        compiler_params=LIMIT,
        name="ewald",
    )(coeffs, cos_all, sin_all, miller, h, dy, *more)


def coefficients(totals, filt_rows, norm_atoms, norm_k):
    channels = filt_rows.shape[1]
    cos_struct = totals[:, 0:channels] * norm_atoms
    cos_back = totals[:, channels : 2 * channels] * norm_k
    sin_struct = totals[:, 2 * channels : 3 * channels] * norm_atoms
    sin_back = totals[:, 3 * channels : 4 * channels] * norm_k
    coeffs = jnp.concatenate(
        [
            norm_atoms * filt_rows * cos_back,
            norm_k * filt_rows * cos_struct,
            norm_atoms * filt_rows * sin_back,
            norm_k * filt_rows * sin_struct,
        ],
        axis=1,
    )
    return (coeffs.astype(jnp.bfloat16), cos_struct * cos_back + sin_struct * sin_back)


def sent_out(x, axis, dim):
    length = x.shape[dim]
    before = from_behind(lax.slice_in_dim(x, length - 1, length, axis=dim), axis, 1)
    after = from_behind(lax.slice_in_dim(x, 0, 1, axis=dim), axis, -1)
    return before, after


def sent_back(x, axis, dim):
    length = x.shape[dim]
    first = lax.slice_in_dim(x, 0, 1, axis=dim).astype(jnp.bfloat16)
    last = lax.slice_in_dim(x, length - 1, length, axis=dim).astype(jnp.bfloat16)
    return from_behind(first, axis, -1), from_behind(last, axis, 1)


def whole(
    atom_embedding,
    output_adjoint,
    fractional_coords,
    element_labels,
    adjacent_ghost_entries,
    miller_triples,
    reciprocal_kernel,
    channel_mixing_matrix,
    element_channel_factor,
    distance_kernel,
):
    h = atom_embedding[0, 0, 0]
    dy = output_adjoint[0, 0, 0]
    pos = fractional_coords[0, 0, 0][:, None, :]
    kinds = element_labels[0, 0]
    channels, atoms = h.shape
    points = miller_triples.shape[1]
    devices = lax.axis_size(GX_GY_GZ)
    norm_atoms = (atoms * devices) ** (-0.5)
    norm_k = points ** (-0.5)
    share_rows = points // devices
    share_start = lax.axis_index(GX_GY_GZ) * share_rows
    half = points // 2

    cells, core, miller_mine, miller_next = pack(h, kinds, pos, miller_triples)
    cells = cells.reshape(3, 3, 3, 16, 128)
    below, above = sent_out(cells, GZ, 2)
    cos_next, sin_next, part_next = phase_sums(pos, miller_next, h, dy)
    received = from_behind(part_next, PAIR, 1)
    cells = jnp.concatenate([below, cells, above], axis=2)
    below, above = sent_out(cells, GY, 1)
    cos_mine, sin_mine, part_mine = phase_sums(pos, miller_mine, h, dy)
    cells = jnp.concatenate([below, cells, above], axis=1)
    below, above = sent_out(cells, "gx", 0)
    sheet, tower = lax.axis_size(SHEET), lax.axis_size(TOWER)
    width = 4 * channels
    paired = part_mine.astype(jnp.float32) + received.astype(jnp.float32)
    paired = paired.astype(jnp.bfloat16)
    pieces = lax.all_to_all(paired.reshape(tower, half // tower, width), TOWER, 0, 0)

    low, mid, high, core_grad, own_grad, sums = short_range(
        (below.reshape(400, 128), cells.reshape(1200, 128), above.reshape(400, 128), core),
        adjacent_ghost_entries[0, 0, 0],
        pos,
        dy,
        distance_kernel,
        channel_mixing_matrix,
        element_channel_factor,
    )
    sums_hi = lax.reduce_precision(sums, 8, 7)
    tiles = jnp.concatenate([sums_hi, sums - sums_hi], axis=1).astype(jnp.bfloat16)
    tiles = tiles.reshape(sheet, 8, 256)

    partial = jnp.sum(pieces.astype(jnp.float32), axis=0).astype(jnp.bfloat16)
    pieces = lax.all_to_all(partial.reshape(sheet, share_rows, width), SHEET, 0, 0)
    totals = jnp.sum(pieces.astype(jnp.float32), axis=0)
    filt_rows = lax.dynamic_slice_in_dim(reciprocal_kernel, share_start, share_rows, 0)
    own_coeffs, filter_share = coefficients(totals, filt_rows, norm_atoms, norm_k)
    spread = jnp.broadcast_to(own_coeffs[None], (sheet, share_rows, width))
    got = lax.all_to_all(jnp.concatenate([spread, tiles], axis=2), SHEET, 0, 0)

    grid = mid.reshape(3, 5, 5, 16, 128)
    to_side = (
        from_behind(low.reshape(1, 5, 5, 16, 128), "gx", -1),
        from_behind(high.reshape(1, 5, 5, 16, 128), "gx", 1),
    )
    grid = jnp.concatenate(
        [
            grid[0:1] + to_side[1].astype(jnp.float32),
            grid[1:2],
            grid[2:3] + to_side[0].astype(jnp.float32),
        ],
        axis=0,
    )
    to_side = sent_back(grid, GY, 1)

    tile_part = jnp.sum(got[:, :, width:].astype(jnp.float32), axis=0)
    tile_part = tile_part[:, 0:128] + tile_part[:, 128:256]
    part_hi = lax.reduce_precision(tile_part, 8, 7)
    strip = jnp.concatenate(
        [
            got[:, :, 0:width].reshape(sheet * share_rows, width),
            jnp.concatenate([part_hi, tile_part - part_hi], axis=1).astype(jnp.bfloat16),
        ],
        axis=0,
    )
    got = lax.all_to_all(jnp.broadcast_to(strip[None], (tower,) + strip.shape), TOWER, 0, 0)
    planes = (
        grid[:, 1:2] + to_side[1].astype(jnp.float32),
        grid[:, 2:3],
        grid[:, 3:4] + to_side[0].astype(jnp.float32),
    )
    to_side = tuple(
        from_behind(
            jnp.concatenate([p[:, :, at : at + 1].astype(jnp.bfloat16) for p in planes], axis=1),
            GZ,
            by,
        )
        for at, by in ((0, -1), (4, 1))
    )
    tile_sum = jnp.sum(got[:, sheet * share_rows :].astype(jnp.float32), axis=0)
    tile_sum = tile_sum[:, 0:128] + tile_sum[:, 128:256]
    got_next = from_behind(got, PAIR, 1)
    every = lax.all_to_all(
        jnp.broadcast_to(tile_sum[None], (2 * sheet, 8, 128)), SHEET + (PAIR,), 0, 0
    )
    every = every.reshape(sheet, 2, 8, 128)
    first = ewald(got, cos_mine, sin_mine, miller_mine, h, dy)
    atom_grad, position_grad, weight_grad, radial_grad = ewald(
        got_next,
        cos_next,
        sin_next,
        miller_next,
        h,
        dy,
        (
            *first,
            *planes,
            *to_side,
            core_grad,
            own_grad,
            every,
            kinds,
            element_channel_factor,
            channel_mixing_matrix,
        ),
        distance_kernel.shape[0],
    )
    position_grad = position_grad[:, 0, :]
    return (
        atom_grad[None, None, None],
        position_grad[None, None, None],
        weight_grad,
        radial_grad,
        filter_share,
    )


def solution(mesh):
    finer = Mesh(
        mesh.devices.reshape(mesh.shape["gx"], 4, 4, 2, 2), ("gx", "gy_0", "gy_1", "gz_0", "gz_1")
    )
    in_specs = (
        P("gx", GY, GZ, None, None),
        P("gx", GY, GZ, None, None),
        P("gx", GY, GZ, None, None),
        P("gx", GY, GZ, None),
        P("gx", GY, GZ, None, None),
        P(),
        P(),
        P(),
        P(),
        P(),
    )
    out_specs = (
        P("gx", GY, GZ, None, None),
        P("gx", GY, GZ, None, None),
        P(),
        P(),
        P(GX_GY_GZ, None),
    )
    return jax.shard_map(whole, mesh=finer, in_specs=in_specs, out_specs=out_specs, check_vma=False)
```

```python
import math

import jax
import jax.numpy as jnp
from jax import lax
from jax.experimental import pallas as pl
from jax.experimental.pallas import tpu as pltpu
from jax.sharding import Mesh
from jax.sharding import PartitionSpec as P


GY = ("gy_0", "gy_1")
GZ = ("gz_0", "gz_1")

SHEET = ("gx", "gy_1")
TOWER = ("gy_0", "gz_0")
PAIR = "gz_1"
GX_GY_GZ = ("gx", "gy_0", "gy_1", "gz_0", "gz_1")

circle_angle = 2.0 * math.pi
CHUNK = 256
SHARE = 8
SIN_TERMS = (6.28316404, -41.33714227, 81.34076528, -70.99339569)
COS_TERMS = (0.99999995, -19.73917143, 64.93459054, -85.24032775, 56.2423573)
WHOLE = pl.BlockSpec(memory_space=pltpu.VMEM)
FAR = pl.BlockSpec(memory_space=pltpu.HBM)
LIMIT = pltpu.CompilerParams(vmem_limit_bytes=20 * 1024 * 1024)

reach_sq = 0.75
GROUPS = 9
ROWS = 72
BLOCKS = 135
HIGH = BLOCKS // GROUPS * 16


def split_two(x):
    high = x.astype(jnp.bfloat16)
    return high, (x - high.astype(jnp.float32)).astype(jnp.bfloat16)


def row_pick(first, second, third, shape):
    row = lax.broadcasted_iota(jnp.int32, shape, 0) % 4
    spread = lambda v: jnp.broadcast_to(v, shape)
    return jnp.where(
        row == 0,
        spread(first),
        jnp.where(row == 1, spread(second), jnp.where(row == 2, spread(third), 0.0)),
    )


def gains_of(gain_rows, labels, shape):
    columns = jnp.transpose(gain_rows)
    gains = jnp.zeros(shape, jnp.float32)
    for kind in range(gain_rows.shape[0]):
        gains = jnp.where(labels == kind, columns[:, kind : kind + 1], gains)
    return gains


def short_kernel(
    ids_ref,
    pos_ref,
    dy_ref,
    radial_ref,
    mix_ref,
    gain_ref,
    below_ref,
    cells_ref,
    above_ref,
    core_ref,
    low_out,
    mid_out,
    high_out,
    core_out,
    own_ref,
    sums_ref,
    lhs_ref,
    feat_ref,
    gains_ref,
    high_ref,
    low_ref,
    near_ref,
    rel_ref,
    basis_ref,
    filt_ref,
    acc_ref,
    table_ref,
    zgrad_ref,
):
    channels, atoms = dy_ref.shape
    side, inner, rest = below_ref.shape[0], cells_ref.shape[0], core_ref.shape[0]
    bounds = (0, side, side + inner, 2 * side + inner, 2 * side + inner + rest)
    for n, ref in enumerate((below_ref, cells_ref, above_ref, core_ref)):
        table_ref[bounds[n] : bounds[n + 1], :] = ref[...]
    table_ref[bounds[4] :, :] = jnp.zeros((GROUPS * HIGH - bounds[4], 128), jnp.bfloat16)
    listed = ids_ref.shape[0]
    count = radial_ref.shape[0]
    f32, bf16 = jnp.float32, jnp.bfloat16
    spacing = reach_sq / (count - 1)
    width = 2.0 * spacing
    share = listed ** (-0.5)
    for g in range(GROUPS):
        part = jnp.transpose(table_ref[g * HIGH : (g + 1) * HIGH, :].astype(f32))
        feat = part[0:channels].astype(bf16)
        gains = gains_of(gain_ref[...], part[ROWS : ROWS + 1], (channels, HIGH))
        feat_ref[g] = feat
        gains_ref[g] = gains
        z = lax.dot_general(
            mix_ref[...], feat, (((0,), (0,)), ((), ())), preferred_element_type=f32
        )
        lhs_ref[g * ROWS : (g + 1) * ROWS, :] = jnp.concatenate(
            [z * gains, part[channels:ROWS]], axis=0
        ).astype(bf16)
    ids = ids_ref[...]
    slot = lax.shift_right_logical(ids, 9)
    atom = jnp.bitwise_and(ids, 511)
    block = lax.shift_right_logical(atom, 4)
    ox = slot // 9
    oy = (slot // 3) % 3
    oz = slot % 3
    qx = block // 9
    qy = (block // 3) % 3
    qz = block % 3
    grid = ((3 * ox + qx - 2) * 5 + 3 * oy + qy - 2) * 5 + 3 * oz + qz - 2
    grid = jnp.where(block >= 27, block + (125 - 27), grid)
    low = grid // (BLOCKS // GROUPS)
    high = (grid - low * (BLOCKS // GROUPS)) * 16 + jnp.bitwise_and(atom, 15)
    high_ref[...] = high
    low_ref[...] = low
    offs = [(o - 1).astype(f32) for o in (ox, oy, oz)]
    own8 = row_pick(pos_ref[0], pos_ref[1], pos_ref[2], (8, atoms))
    w_hi, w_lo = split_two(radial_ref[...])
    w_stack = jnp.concatenate([w_hi, w_hi, w_lo], axis=0)
    centre = lax.broadcasted_iota(jnp.int32, (count, 1), 0).astype(f32) * spacing
    iota = lax.broadcasted_iota(jnp.int32, (HIGH, atoms), 0)

    def hot(j):
        return (high_ref[pl.ds(j, 1), :] == iota).astype(f32).astype(bf16)

    agg = jnp.zeros((channels, atoms), f32)
    for j in range(listed):
        found = jnp.dot(lhs_ref[...], hot(j), preferred_element_type=f32)
        low_j = low_ref[j : j + 1, :]
        near = found[0:ROWS]
        for g in range(1, GROUPS):
            near = jnp.where(low_j == g, found[g * ROWS : (g + 1) * ROWS], near)
        near_z = near[0:channels]
        near_ref[j] = near_z.astype(bf16)
        halves = near[channels : channels + 8]
        off8 = row_pick(offs[0][j : j + 1], offs[1][j : j + 1], offs[2][j : j + 1], (8, atoms))
        rel = halves + pltpu.roll(halves, 4, 0) + off8 - own8
        rel_ref[j] = rel
        dist = 0.5 * jnp.sum(rel * rel, axis=0, keepdims=True)
        scaled = (dist - centre) / width
        basis = jnp.exp(-(scaled * scaled))
        basis_ref[j] = basis
        b_hi, b_lo = split_two(basis)
        filt = lax.dot_general(
            w_stack,
            jnp.concatenate([b_hi, b_lo, b_hi], axis=0),
            (((0,), (0,)), ((), ())),
            preferred_element_type=f32,
        )
        filt_ref[j] = filt
        agg = agg + filt * near_z
    agg = agg * share
    gate = 1.0 / (1.0 + jnp.exp(-agg))
    g_all = dy_ref[...].astype(f32) * (gate * (1.0 + agg * (1.0 - gate))) * share
    acc_ref[...] = jnp.zeros_like(acc_ref)
    own_grad = jnp.zeros((8, atoms), f32)
    radial = jnp.zeros((2 * count, 2 * channels), f32)
    w_wide = jnp.concatenate([w_hi, w_hi, w_lo], axis=1)
    for j in range(listed):
        near_z = near_ref[j].astype(f32)
        dz = filt_ref[j] * g_all
        df = near_z * g_all
        f_hi, f_lo = split_two(df)
        basis = basis_ref[j]
        b_hi, b_lo = split_two(basis)
        radial = radial + lax.dot_general(
            jnp.concatenate([b_hi, b_lo], axis=0),
            jnp.concatenate([f_hi, f_lo], axis=0),
            (((1,), (1,)), ((), ())),
            preferred_element_type=f32,
        )
        dbasis = jnp.dot(
            w_wide, jnp.concatenate([f_hi, f_lo, f_hi], axis=0), preferred_element_type=f32
        )
        rel = rel_ref[j]
        dist = 0.5 * jnp.sum(rel * rel, axis=0, keepdims=True)
        slope = dbasis * basis * (dist - centre)
        ddist = jnp.sum(slope, axis=0, keepdims=True) * (-2.0 / (width * width))
        gpos = rel * (2.0 * ddist)
        own_grad = own_grad - gpos
        p_hi = gpos.astype(bf16).astype(f32)
        row8 = lax.broadcasted_iota(jnp.int32, (8, atoms), 0)
        tail = jnp.where(row8 < 4, p_hi, gpos - p_hi)
        full = jnp.concatenate([dz, tail], axis=0)
        low_j = low_ref[j : j + 1, :]
        spread = jnp.concatenate(
            [jnp.where(low_j == g, full, 0.0) for g in range(GROUPS)], axis=0
        ).astype(bf16)
        acc_ref[...] += lax.dot_general(
            spread, hot(j), (((1,), (1,)), ((), ())), preferred_element_type=f32
        )
    own_ref[...] = own_grad
    sums_ref[...] = jnp.zeros_like(sums_ref)
    radial = (
        radial[0:count, 0:channels]
        + radial[count:, 0:channels]
        + radial[0:count, channels:]
        + radial[count:, channels:]
    )
    weight = jnp.zeros((channels, channels), f32)
    for g in range(GROUPS):
        z_hi, z_lo = split_two(acc_ref[g * ROWS : g * ROWS + channels, :] * gains_ref[g])
        for piece in (z_hi, z_lo):
            weight = weight + lax.dot_general(
                feat_ref[g], piece, (((1,), (1,)), ((), ())), preferred_element_type=f32
            )
        part = jnp.transpose(acc_ref[g * ROWS : (g + 1) * ROWS, :])
        part = jnp.concatenate([part, jnp.zeros((HIGH, 128 - ROWS), f32)], axis=1)
        zgrad_ref[g * HIGH : (g + 1) * HIGH, :] = part
    for n, (ref, kind) in enumerate(
        ((low_out, bf16), (mid_out, f32), (high_out, bf16), (core_out, f32))
    ):
        ref[...] = zgrad_ref[bounds[n] : bounds[n + 1], :].astype(kind)
    tall = jnp.concatenate([weight, radial], axis=0)
    cut = (channels + count) // 2
    sums_ref[0:cut, :] = jnp.concatenate([tall[0:cut], tall[cut:]], axis=1)


def short_range(pieces, ids, pos, dy, radial, mix, gain):
    channels, atoms = dy.shape
    listed = ids.shape[0]
    count = radial.shape[0]
    f32, bf16 = jnp.float32, jnp.bfloat16
    shaped = jax.ShapeDtypeStruct
    return fetching_call(
        short_kernel,
        (ids, pos, dy, radial, mix, gain),
        pieces,
        (
            shaped(pieces[0].shape, bf16),
            shaped(pieces[1].shape, f32),
            shaped(pieces[2].shape, bf16),
            shaped(pieces[3].shape, f32),
            shaped((8, atoms), f32),
            shaped((64, 128), f32),
        ),
        [
            pltpu.VMEM((GROUPS * ROWS, HIGH), bf16),
            pltpu.VMEM((GROUPS, channels, HIGH), bf16),
            pltpu.VMEM((GROUPS, channels, HIGH), f32),
            pltpu.VMEM((listed, atoms), jnp.int32),
            pltpu.VMEM((listed, atoms), jnp.int32),
            pltpu.VMEM((listed, channels, atoms), bf16),
            pltpu.VMEM((listed, 8, atoms), f32),
            pltpu.VMEM((listed, count, atoms), f32),
            pltpu.VMEM((listed, channels, atoms), f32),
            pltpu.VMEM((GROUPS * ROWS, HIGH), f32),
            pltpu.VMEM((GROUPS * HIGH, 128), bf16),
            pltpu.VMEM((GROUPS * HIGH, 128), f32),
        ],
    )


def fetching_call(
    kernel, fetched, resident, outs, scratch, early=None, in_specs=None, out_specs=None, flops=0
):
    n = len(fetched)

    def body(*refs):
        sources, rest = refs[:n], refs[n : -n - 1]
        buffers, sems = refs[-n - 1 : -1], refs[-1]
        copies = [
            pltpu.make_async_copy(sources[i], buffers[i], sems.at[i]) for i in range(n)
        ]
        if early is not None:
            early(*rest)
        for copy in copies:
            copy.start()
        for copy in copies:
            copy.wait()
        kernel(*buffers, *rest)

    cost = None
    if flops:
        cost = pl.CostEstimate(flops=flops, transcendentals=0, bytes_accessed=flops // 128)
    return pl.pallas_call(
        body,
        out_shape=outs,
        in_specs=[FAR] * n + list(in_specs or [WHOLE] * len(resident)),
        out_specs=tuple(out_specs or [WHOLE] * len(outs)),
        scratch_shapes=[
            *scratch,
            *[pltpu.VMEM(x.shape, x.dtype) for x in fetched],
            pltpu.SemaphoreType.DMA((n,)),
        ],
        compiler_params=LIMIT,
        cost_estimate=cost,
    )(*fetched, *resident)


def from_behind(x, axis, by):
    devices = lax.axis_size(axis)
    return lax.ppermute(x, axis, [(i, (i + by) % devices) for i in range(devices)])


def chosen(parity):
    column = lax.broadcasted_iota(jnp.int32, (2 * CHUNK, CHUNK), 1)
    row = lax.broadcasted_iota(jnp.int32, (2 * CHUNK, CHUNK), 0)
    n = column // SHARE
    outer, inner, least = [lax.axis_size(axis) for axis in ("gy_0", "gy_1", "gz_0")]
    group = ((n // least) % outer * inner + n // (least * outer)) * least + n % least
    picked = group * (2 * SHARE) + column % SHARE + parity * SHARE
    return (row == picked).astype(jnp.float32).astype(jnp.bfloat16)


def pack_kernel(h_ref, kind_ref, pos_ref, miller_ref, cells_ref, core_ref, mine_ref, next_ref):
    f32, bf16 = jnp.float32, jnp.bfloat16
    _, atoms = h_ref.shape
    none = jnp.zeros((1, atoms), f32)
    halves = [split_two(pos_ref[d]) for d in range(3)]
    rows = jnp.concatenate(
        [h_ref[...].astype(f32)]
        + [half[0].astype(f32) for half in halves]
        + [none]
        + [half[1].astype(f32) for half in halves]
        + [none, kind_ref[...].astype(f32), jnp.zeros((127 - ROWS, atoms), f32)],
        axis=0,
    )
    flat = jnp.transpose(rows).astype(bf16)
    cells_ref[...] = flat[0 : cells_ref.shape[0]]
    core_ref[...] = flat[cells_ref.shape[0] :]
    m = miller_ref[...].astype(f32)
    tall = jnp.concatenate([m, m, m, jnp.zeros((7, m.shape[1]), f32)], axis=0).astype(bf16)
    runs = m.shape[1] // (2 * CHUNK)
    stack = jnp.concatenate(
        [tall[:, j * 2 * CHUNK : (j + 1) * 2 * CHUNK] for j in range(runs)], axis=0
    )
    core = lax.axis_index(PAIR)
    for parity, out_ref in ((core, mine_ref), (1 - core, next_ref)):
        got = jnp.dot(stack, chosen(parity), preferred_element_type=f32).astype(bf16)
        for j in range(runs):
            out_ref[:, j * CHUNK : (j + 1) * CHUNK] = got[j * 16 : (j + 1) * 16]


def pack(h, kinds, pos, miller):
    half = jax.ShapeDtypeStruct((16, miller.shape[1] // 2), jnp.bfloat16)
    return fetching_call(
        pack_kernel,
        (h, kinds, pos, miller),
        (),
        (
            jax.ShapeDtypeStruct((432, 128), jnp.bfloat16),
            jax.ShapeDtypeStruct((h.shape[1] - 432, 128), jnp.bfloat16),
            half,
            half,
        ),
        [],
    )


def phase_kernel(
    pos_ref,
    h_ref,
    dy_ref,
    miller_ref,
    cos_out,
    sin_out,
    part_ref,
    cos_ref,
    sin_ref,
    flip_ref,
    rhs_ref,
    t_ref,
    sems,
):
    f32, bf16 = jnp.float32, jnp.bfloat16
    width = 2 * h_ref.shape[0]
    flip_ref[...] = jnp.transpose(jnp.concatenate([h_ref[...], dy_ref[...]], axis=0))
    axes = ("gx", GY, GZ)
    turns = jnp.concatenate(
        [
            (pos_ref[d] + lax.axis_index(axes[d]).astype(f32)) / float(lax.axis_size(axes[d]))
            for d in range(3)
        ],
        axis=0,
    )
    t_hi = turns.astype(bf16)
    t_mid, t_lo = split_two(turns - t_hi.astype(f32))
    rhs_ref[...] = jnp.concatenate(
        [t_hi, t_mid, t_lo, jnp.zeros((7, turns.shape[1]), bf16)], axis=0
    )
    steps = miller_ref.shape[1] // CHUNK
    rows, lanes = 16, 256

    def copies(i):
        at = pl.ds(pl.multiple_of(i * CHUNK, CHUNK), CHUNK)
        return [
            pltpu.make_async_copy(src.at[at], dst.at[at], sems.at[n, i])
            for n, (src, dst) in enumerate(
                ((cos_ref, cos_out), (sin_ref, sin_out))
            )
        ]

    def one(i, carry):
        base = pl.multiple_of(i * CHUNK, CHUNK)
        t_ref[...] = lax.dot_general(
            miller_ref[:, pl.ds(base, CHUNK)],
            rhs_ref[...],
            (((0,), (0,)), ((), ())),
            preferred_element_type=f32,
        )
        for top in range(0, CHUNK, rows):
            for left in range(0, t_ref.shape[1], lanes):
                t = t_ref[top : top + rows, left : left + lanes]
                r = t - jnp.round(t)
                u = jnp.abs(r) - 0.25
                q = u * u
                s = SIN_TERMS[3]
                for term in SIN_TERMS[2::-1]:
                    s = s * q + term
                c = COS_TERMS[4]
                for term in COS_TERMS[3::-1]:
                    c = c * q + term
                at = (pl.ds(base + top, rows), pl.ds(left, lanes))
                cos_ref[at] = -(s * u).astype(bf16)
                sin_ref[at] = jnp.where(r < 0.0, -c, c).astype(bf16)
        here = pl.ds(base, CHUNK)
        part_ref[here, 0:width] = jnp.dot(
            cos_ref[here, :], flip_ref[...], preferred_element_type=f32
        )
        part_ref[here, width:] = jnp.dot(
            sin_ref[here, :], flip_ref[...], preferred_element_type=f32
        )
        for copy in copies(i):
            copy.start()
        return carry

    lax.fori_loop(0, steps, one, 0)
    for i in range(steps):
        for copy in copies(i):
            copy.wait()


def phase_sums(pos, miller, h, dy):
    points = miller.shape[1]
    channels, atoms = h.shape
    width = 2 * channels
    wave = jax.ShapeDtypeStruct((points, atoms), jnp.bfloat16)
    sums = jax.ShapeDtypeStruct((points, 2 * width), jnp.float32)
    return fetching_call(
        phase_kernel,
        (pos, h, dy),
        (miller,),
        (wave, wave, sums),
        [
            pltpu.VMEM(wave.shape, wave.dtype),
            pltpu.VMEM(wave.shape, wave.dtype),
            pltpu.VMEM((atoms, width), jnp.bfloat16),
            pltpu.VMEM((16, atoms), jnp.bfloat16),
            pltpu.VMEM((CHUNK, atoms), jnp.float32),
            pltpu.SemaphoreType.DMA((2, points // CHUNK)),
        ],
        out_specs=(FAR, FAR, WHOLE),
        flops=6 * points * atoms * width,
    )


def wave_copies(cos_in, sin_in, cos_ref, sin_ref, sems, i):
    at = pl.ds(pl.multiple_of(i * CHUNK, CHUNK), CHUNK)
    return [
        pltpu.make_async_copy(cos_in.at[at], cos_ref.at[at], sems.at[0, i]),
        pltpu.make_async_copy(sin_in.at[at], sin_ref.at[at], sems.at[1, i]),
    ]


def ewald_early(cos_in, sin_in, *rest):
    for i in range(cos_in.shape[0] // CHUNK):
        for copy in wave_copies(cos_in, sin_in, *rest[-3:], i):
            copy.start()


def ewald_sums(coeff_ref, miller_ref, both, waves, sums_ref, turn_ref):
    f32 = jnp.float32
    width = both.shape[0]
    channels = width // 2
    run = CHUNK // (miller_ref.shape[1] // coeff_ref.shape[0])
    over_rows = (((0,), (0,)), ((), ()))

    def one(i, carry):
        for copy in wave_copies(*waves, i):
            copy.wait()
        at = pl.ds(pl.multiple_of(i * CHUNK, CHUNK), CHUNK)
        coeffs = coeff_ref[pl.ds(i * run, run), 0 : CHUNK // run].reshape(CHUNK, 2 * width)
        cos_part, sin_part = waves[2][at, :], waves[3][at, :]
        sums_ref[...] += lax.dot_general(
            coeffs[:, 0:channels], cos_part, over_rows, preferred_element_type=f32
        ) + lax.dot_general(
            coeffs[:, width : width + channels], sin_part, over_rows, preferred_element_type=f32
        )
        along_u = jnp.dot(coeffs[:, 0:width], both, preferred_element_type=f32)
        along_v = jnp.dot(coeffs[:, width:], both, preferred_element_type=f32)
        angle = along_v * cos_part.astype(f32) - along_u * sin_part.astype(f32)
        a_hi, a_lo = split_two(angle)
        m = miller_ref[:, at]
        turn_ref[...] += jnp.dot(m, a_hi, preferred_element_type=f32) + jnp.dot(
            m, a_lo, preferred_element_type=f32
        )
        return carry

    lax.fori_loop(0, miller_ref.shape[1] // CHUNK, one, 0)


def ewald_first(
    h_ref, dy_ref, cos_in, sin_in, coeff_ref, miller_ref, sums_ref, turn_ref, cos_ref, sin_ref, sems
):
    sums_ref[...] = jnp.zeros_like(sums_ref)
    turn_ref[...] = jnp.zeros_like(turn_ref)
    both = jnp.concatenate([h_ref[...], dy_ref[...]], axis=0)
    waves = (cos_in, sin_in, cos_ref, sin_ref, sems)
    ewald_sums(coeff_ref, miller_ref, both, waves, sums_ref, turn_ref)


def ewald_second(
    h_ref,
    dy_ref,
    kind_ref,
    gain_ref,
    mix_ref,
    cos_in,
    sin_in,
    coeff_ref,
    miller_ref,
    first_ref,
    angle_ref,
    low_ref,
    middle_ref,
    high_ref,
    upper_ref,
    lower_ref,
    core_ref,
    own_ref,
    mine_ref,
    atom_ref,
    pos_ref,
    weight_ref,
    radial_ref,
    sums_ref,
    turn_ref,
    cos_ref,
    sin_ref,
    sems,
):
    f32, bf16 = jnp.float32, jnp.bfloat16
    channels = h_ref.shape[0]
    cells = jnp.stack(
        [
            jnp.stack(
                [
                    plane[:, 0, 1] + lower_ref[:, n, 0].astype(f32),
                    plane[:, 0, 2],
                    plane[:, 0, 3] + upper_ref[:, n, 0].astype(f32),
                ],
                axis=1,
            )
            for n, plane in enumerate((low_ref, middle_ref, high_ref))
        ],
        axis=1,
    ).reshape(432, 128)
    flat = jnp.transpose(jnp.concatenate([cells, core_ref[...]], axis=0))
    gains = gains_of(gain_ref[...], kind_ref[...], (channels, flat.shape[1]))
    zscaled = (flat[0:channels] * gains).astype(bf16)
    halves = flat[channels : channels + 8]
    near = halves + pltpu.roll(halves, 4, 0) + own_ref[...]
    sums_ref[...] = first_ref[...] + jnp.dot(mix_ref[...], zscaled, preferred_element_type=f32)
    turn_ref[...] = angle_ref[...]
    both = jnp.concatenate([h_ref[...], dy_ref[...]], axis=0)
    waves = (cos_in, sin_in, cos_ref, sin_ref, sems)
    ewald_sums(coeff_ref, miller_ref, both, waves, sums_ref, turn_ref)
    atom_ref[...] = (dy_ref[...].astype(f32) + sums_ref[...]).astype(bf16)
    axes = ("gx", GY, GZ)
    for d in range(3):
        pos_ref[d] = (
            turn_ref[d : d + 1, :] * (circle_angle / lax.axis_size(axes[d])) + near[d : d + 1, :]
        )
    cut = (channels + radial_ref.shape[0]) // 2
    run = miller_ref.shape[1] // coeff_ref.shape[0]
    sides = []
    for ref in (mine_ref, coeff_ref):
        total = jnp.sum(ref[:, run : run + cut].astype(f32), axis=0)
        sides.append(total[:, 0:128] + total[:, 128:256])
    full = sides[0] + sides[1]
    tall = jnp.concatenate([full[:, 0:channels], full[:, channels:]], axis=0)
    weight_ref[...] = tall[0:channels]
    radial_ref[...] = tall[channels:]


def ewald(coeffs, cos_all, sin_all, miller, h, dy, more=(), params=(), basis=0):
    points, atoms = cos_all.shape
    channels = h.shape[0]
    last = len(more) > 0
    shaped = jax.ShapeDtypeStruct
    sums = shaped((channels, atoms), jnp.float32)
    turn = shaped((16, atoms), jnp.float32)
    scratch = [
        pltpu.VMEM(cos_all.shape, jnp.bfloat16),
        pltpu.VMEM(cos_all.shape, jnp.bfloat16),
        pltpu.SemaphoreType.DMA((2, points // CHUNK)),
    ]
    outs = (sums, turn)
    if last:
        scratch = [pltpu.VMEM(sums.shape, sums.dtype), pltpu.VMEM(turn.shape, turn.dtype)] + scratch
        outs = (
            shaped(sums.shape, jnp.bfloat16),
            shaped((3, 1, atoms), jnp.float32),
            shaped((channels, channels), jnp.float32),
            shaped((basis, channels), jnp.float32),
        )
    return fetching_call(
        ewald_second if last else ewald_first,
        (h, dy, *params),
        (cos_all, sin_all, coeffs, miller, *more),
        outs,
        scratch,
        early=ewald_early,
        in_specs=(FAR, FAR) + (WHOLE,) * (2 + len(more)),
        flops=8 * points * atoms * channels,
    )


def coefficients(totals, filt_rows, norm_atoms, norm_k):
    channels = filt_rows.shape[1]
    cos_struct = totals[:, 0:channels] * norm_atoms
    cos_back = totals[:, channels : 2 * channels] * norm_k
    sin_struct = totals[:, 2 * channels : 3 * channels] * norm_atoms
    sin_back = totals[:, 3 * channels : 4 * channels] * norm_k
    coeffs = jnp.concatenate(
        [
            norm_atoms * filt_rows * cos_back,
            norm_k * filt_rows * cos_struct,
            norm_atoms * filt_rows * sin_back,
            norm_k * filt_rows * sin_struct,
        ],
        axis=1,
    )
    return (coeffs.astype(jnp.bfloat16), cos_struct * cos_back + sin_struct * sin_back)


def sent_out(x, axis, dim):
    length = x.shape[dim]
    before = from_behind(lax.slice_in_dim(x, length - 1, length, axis=dim), axis, 1)
    after = from_behind(lax.slice_in_dim(x, 0, 1, axis=dim), axis, -1)
    return before, after


def sent_back(x, axis, dim):
    length = x.shape[dim]
    first = lax.slice_in_dim(x, 0, 1, axis=dim).astype(jnp.bfloat16)
    last = lax.slice_in_dim(x, length - 1, length, axis=dim).astype(jnp.bfloat16)
    return from_behind(first, axis, -1), from_behind(last, axis, 1)


def whole(
    atom_embedding,
    output_adjoint,
    fractional_coords,
    element_labels,
    adjacent_ghost_entries,
    miller_triples,
    reciprocal_kernel,
    channel_mixing_matrix,
    element_channel_factor,
    distance_kernel,
):
    h = atom_embedding[0, 0, 0]
    dy = output_adjoint[0, 0, 0]
    pos = fractional_coords[0, 0, 0][:, None, :]
    kinds = element_labels[0, 0]
    channels, atoms = h.shape
    points = miller_triples.shape[1]
    devices = lax.axis_size(GX_GY_GZ)
    norm_atoms = (atoms * devices) ** (-0.5)
    norm_k = points ** (-0.5)
    share_rows = points // devices
    share_start = lax.axis_index(GX_GY_GZ) * share_rows
    half = points // 2

    cells, core, miller_mine, miller_next = pack(h, kinds, pos, miller_triples)
    cells = cells.reshape(3, 3, 3, 16, 128)
    below, above = sent_out(cells, GZ, 2)
    cos_next, sin_next, part_next = phase_sums(pos, miller_next, h, dy)
    received = from_behind(part_next, PAIR, 1)
    cells = jnp.concatenate([below, cells, above], axis=2)
    below, above = sent_out(cells, GY, 1)
    cos_mine, sin_mine, part_mine = phase_sums(pos, miller_mine, h, dy)
    cells = jnp.concatenate([below, cells, above], axis=1)
    below, above = sent_out(cells, "gx", 0)
    sheet, tower = lax.axis_size(SHEET), lax.axis_size(TOWER)
    width = 4 * channels
    paired = (part_mine + received).astype(jnp.bfloat16)
    pieces = lax.all_to_all(paired.reshape(sheet, half // sheet, width), SHEET, 0, 0)

    low, mid, high, core_grad, own_grad, sums = short_range(
        (below.reshape(400, 128), cells.reshape(1200, 128), above.reshape(400, 128), core),
        adjacent_ghost_entries[0, 0, 0],
        pos,
        dy,
        distance_kernel,
        channel_mixing_matrix,
        element_channel_factor,
    )
    sums_hi = lax.reduce_precision(sums, 8, 7)
    tiles = jnp.concatenate([sums_hi, sums - sums_hi], axis=1).astype(jnp.bfloat16)
    tiles = tiles.reshape(tower, 8, 256)

    partial = jnp.sum(pieces.astype(jnp.float32), axis=0).astype(jnp.bfloat16)
    partial = partial.reshape(tower, share_rows, width)
    pieces = lax.all_to_all(jnp.concatenate([partial, tiles], axis=2), TOWER, 0, 0)
    pieces = jnp.sum(pieces.astype(jnp.float32), axis=0)
    totals, tile = pieces[:, 0:width], pieces[:, width:]
    filt_rows = lax.dynamic_slice_in_dim(reciprocal_kernel, share_start, share_rows, 0)
    own_coeffs, filter_share = coefficients(totals, filt_rows, norm_atoms, norm_k)
    tile = tile[:, 0:128] + tile[:, 128:256]
    tile_hi = lax.reduce_precision(tile, 8, 7)
    sent = jnp.concatenate(
        [own_coeffs, tile_hi.astype(jnp.bfloat16), (tile - tile_hi).astype(jnp.bfloat16)], axis=1
    )
    got = lax.all_to_all(jnp.broadcast_to(sent[None], (tower,) + sent.shape), TOWER, 0, 0)

    grid = mid.reshape(3, 5, 5, 16, 128)
    to_side = (
        from_behind(low.reshape(1, 5, 5, 16, 128), "gx", -1),
        from_behind(high.reshape(1, 5, 5, 16, 128), "gx", 1),
    )
    grid = jnp.concatenate(
        [
            grid[0:1] + to_side[1].astype(jnp.float32),
            grid[1:2],
            grid[2:3] + to_side[0].astype(jnp.float32),
        ],
        axis=0,
    )
    to_side = sent_back(grid, GY, 1)

    strip = jnp.concatenate(
        [
            got[:, :, 0:width].reshape(tower * share_rows, width),
            got[0:5, :, width:].reshape(5 * share_rows, width),
        ],
        axis=0,
    )
    got = lax.all_to_all(jnp.broadcast_to(strip[None], (sheet,) + strip.shape), SHEET, 0, 0)
    planes = (
        grid[:, 1:2] + to_side[1].astype(jnp.float32),
        grid[:, 2:3],
        grid[:, 3:4] + to_side[0].astype(jnp.float32),
    )
    to_side = tuple(
        from_behind(
            jnp.concatenate([p[:, :, at : at + 1].astype(jnp.bfloat16) for p in planes], axis=1),
            GZ,
            by,
        )
        for at, by in ((0, -1), (4, 1))
    )
    got_next = from_behind(got, PAIR, 1)
    first = ewald(got, cos_mine, sin_mine, miller_mine, h, dy)
    atom_grad, position_grad, weight_grad, radial_grad = ewald(
        got_next,
        cos_next,
        sin_next,
        miller_next,
        h,
        dy,
        (*first, *planes, *to_side, core_grad, own_grad, got),
        (kinds, element_channel_factor, channel_mixing_matrix),
        distance_kernel.shape[0],
    )
    position_grad = position_grad[:, 0, :]
    return (
        atom_grad[None, None, None],
        position_grad[None, None, None],
        weight_grad,
        radial_grad,
        filter_share,
    )


def solution(mesh):
    finer = Mesh(
        mesh.devices.reshape(mesh.shape["gx"], 4, 4, 2, 2), ("gx", "gy_0", "gy_1", "gz_0", "gz_1")
    )
    in_specs = (
        P("gx", GY, GZ, None, None),
        P("gx", GY, GZ, None, None),
        P("gx", GY, GZ, None, None),
        P("gx", GY, GZ, None),
        P("gx", GY, GZ, None, None),
        P(),
        P(),
        P(),
        P(),
        P(),
    )
    out_specs = (
        P("gx", GY, GZ, None, None),
        P("gx", GY, GZ, None, None),
        P(),
        P(),
        P(GX_GY_GZ, None),
    )
    return jax.shard_map(whole, mesh=finer, in_specs=in_specs, out_specs=out_specs, check_vma=False)
```

```python
import functools
import math

import jax
import jax.numpy as jnp
from jax import lax
from jax.experimental import pallas as pl
from jax.experimental.pallas import tpu as pltpu
from jax.sharding import Mesh
from jax.sharding import PartitionSpec as P


GY = ("gy_0", "gy_1")
GZ = ("gz_0", "gz_1")

SHEET = ("gx", "gy_1")
TOWER = ("gy_0", "gz_0")
PAIR = "gz_1"
GX_GY_GZ = ("gx", "gy_0", "gy_1", "gz_0", "gz_1")

circle_angle = 2.0 * math.pi
CHUNK = 256
SHARE = 8
SIN_TERMS = (6.28316404, -41.33714227, 81.34076528, -70.99339569)
COS_TERMS = (0.99999995, -19.73917143, 64.93459054, -85.24032775, 56.2423573)
WHOLE = pl.BlockSpec(memory_space=pltpu.VMEM)
FAR = pl.BlockSpec(memory_space=pltpu.HBM)
LIMIT = pltpu.CompilerParams(vmem_limit_bytes=20 * 1024 * 1024)

reach_sq = 0.75
GROUPS = 9
ROWS = 72
BLOCKS = 135
HIGH = BLOCKS // GROUPS * 16


def split_two(x):
    high = x.astype(jnp.bfloat16)
    return high, (x - high.astype(jnp.float32)).astype(jnp.bfloat16)


def row_pick(first, second, third, shape):
    row = lax.broadcasted_iota(jnp.int32, shape, 0) % 4
    spread = lambda v: jnp.broadcast_to(v, shape)
    return jnp.where(
        row == 0,
        spread(first),
        jnp.where(row == 1, spread(second), jnp.where(row == 2, spread(third), 0.0)),
    )


def gains_of(gain_rows, labels, shape):
    columns = jnp.transpose(gain_rows)
    gains = jnp.zeros(shape, jnp.float32)
    for kind in range(gain_rows.shape[0]):
        gains = jnp.where(labels == kind, columns[:, kind : kind + 1], gains)
    return gains


def short_kernel(
    ids_ref,
    pos_ref,
    dy_ref,
    radial_ref,
    mix_ref,
    gain_ref,
    below_ref,
    cells_ref,
    above_ref,
    core_ref,
    low_out,
    mid_out,
    high_out,
    core_out,
    own_ref,
    sums_ref,
    lhs_ref,
    feat_ref,
    gains_ref,
    high_ref,
    low_ref,
    near_ref,
    rel_ref,
    basis_ref,
    filt_ref,
    acc_ref,
    table_ref,
    zgrad_ref,
):
    channels, atoms = dy_ref.shape
    side, inner, rest = below_ref.shape[0], cells_ref.shape[0], core_ref.shape[0]
    bounds = (0, side, side + inner, 2 * side + inner, 2 * side + inner + rest)
    for n, ref in enumerate((below_ref, cells_ref, above_ref, core_ref)):
        table_ref[bounds[n] : bounds[n + 1], :] = ref[...]
    table_ref[bounds[4] :, :] = jnp.zeros((GROUPS * HIGH - bounds[4], 128), jnp.bfloat16)
    listed = ids_ref.shape[0]
    count = radial_ref.shape[0]
    f32, bf16 = jnp.float32, jnp.bfloat16
    spacing = reach_sq / (count - 1)
    width = 2.0 * spacing
    share = listed ** (-0.5)
    for g in range(GROUPS):
        part = jnp.transpose(table_ref[g * HIGH : (g + 1) * HIGH, :].astype(f32))
        feat = part[0:channels].astype(bf16)
        gains = gains_of(gain_ref[...], part[ROWS : ROWS + 1], (channels, HIGH))
        feat_ref[g] = feat
        gains_ref[g] = gains
        z = lax.dot_general(
            mix_ref[...], feat, (((0,), (0,)), ((), ())), preferred_element_type=f32
        )
        lhs_ref[g * ROWS : (g + 1) * ROWS, :] = jnp.concatenate(
            [z * gains, part[channels:ROWS]], axis=0
        ).astype(bf16)
    ids = ids_ref[...]
    slot = lax.shift_right_logical(ids, 9)
    atom = jnp.bitwise_and(ids, 511)
    block = lax.shift_right_logical(atom, 4)
    ox = slot // 9
    oy = (slot // 3) % 3
    oz = slot % 3
    qx = block // 9
    qy = (block // 3) % 3
    qz = block % 3
    grid = ((3 * ox + qx - 2) * 5 + 3 * oy + qy - 2) * 5 + 3 * oz + qz - 2
    grid = jnp.where(block >= 27, block + (125 - 27), grid)
    low = grid // (BLOCKS // GROUPS)
    high = (grid - low * (BLOCKS // GROUPS)) * 16 + jnp.bitwise_and(atom, 15)
    high_ref[...] = high
    low_ref[...] = low
    offs = [(o - 1).astype(f32) for o in (ox, oy, oz)]
    own8 = row_pick(pos_ref[0], pos_ref[1], pos_ref[2], (8, atoms))
    w_hi, w_lo = split_two(radial_ref[...])
    w_stack = jnp.concatenate([w_hi, w_hi, w_lo], axis=0)
    centre = lax.broadcasted_iota(jnp.int32, (count, 1), 0).astype(f32) * spacing
    iota = lax.broadcasted_iota(jnp.int32, (HIGH, atoms), 0)

    def hot(j):
        return (high_ref[pl.ds(j, 1), :] == iota).astype(f32).astype(bf16)

    agg = jnp.zeros((channels, atoms), f32)
    for j in range(listed):
        found = jnp.dot(lhs_ref[...], hot(j), preferred_element_type=f32)
        low_j = low_ref[j : j + 1, :]
        near = found[0:ROWS]
        for g in range(1, GROUPS):
            near = jnp.where(low_j == g, found[g * ROWS : (g + 1) * ROWS], near)
        near_z = near[0:channels]
        near_ref[j] = near_z.astype(bf16)
        halves = near[channels : channels + 8]
        off8 = row_pick(offs[0][j : j + 1], offs[1][j : j + 1], offs[2][j : j + 1], (8, atoms))
        rel = halves + pltpu.roll(halves, 4, 0) + off8 - own8
        rel_ref[j] = rel
        dist = 0.5 * jnp.sum(rel * rel, axis=0, keepdims=True)
        scaled = (dist - centre) / width
        basis = jnp.exp(-(scaled * scaled))
        basis_ref[j] = basis
        b_hi, b_lo = split_two(basis)
        filt = lax.dot_general(
            w_stack,
            jnp.concatenate([b_hi, b_lo, b_hi], axis=0),
            (((0,), (0,)), ((), ())),
            preferred_element_type=f32,
        )
        filt_ref[j] = filt
        agg = agg + filt * near_z
    agg = agg * share
    gate = 1.0 / (1.0 + jnp.exp(-agg))
    g_all = dy_ref[...].astype(f32) * (gate * (1.0 + agg * (1.0 - gate))) * share
    acc_ref[...] = jnp.zeros_like(acc_ref)
    own_grad = jnp.zeros((8, atoms), f32)
    radial = jnp.zeros((2 * count, 2 * channels), f32)
    w_wide = jnp.concatenate([w_hi, w_hi, w_lo], axis=1)
    for j in range(listed):
        near_z = near_ref[j].astype(f32)
        dz = filt_ref[j] * g_all
        df = near_z * g_all
        f_hi, f_lo = split_two(df)
        basis = basis_ref[j]
        b_hi, b_lo = split_two(basis)
        radial = radial + lax.dot_general(
            jnp.concatenate([b_hi, b_lo], axis=0),
            jnp.concatenate([f_hi, f_lo], axis=0),
            (((1,), (1,)), ((), ())),
            preferred_element_type=f32,
        )
        dbasis = jnp.dot(
            w_wide, jnp.concatenate([f_hi, f_lo, f_hi], axis=0), preferred_element_type=f32
        )
        rel = rel_ref[j]
        dist = 0.5 * jnp.sum(rel * rel, axis=0, keepdims=True)
        slope = dbasis * basis * (dist - centre)
        ddist = jnp.sum(slope, axis=0, keepdims=True) * (-2.0 / (width * width))
        gpos = rel * (2.0 * ddist)
        own_grad = own_grad - gpos
        p_hi = gpos.astype(bf16).astype(f32)
        row8 = lax.broadcasted_iota(jnp.int32, (8, atoms), 0)
        tail = jnp.where(row8 < 4, p_hi, gpos - p_hi)
        full = jnp.concatenate([dz, tail], axis=0)
        low_j = low_ref[j : j + 1, :]
        spread = jnp.concatenate(
            [jnp.where(low_j == g, full, 0.0) for g in range(GROUPS)], axis=0
        ).astype(bf16)
        acc_ref[...] += lax.dot_general(
            spread, hot(j), (((1,), (1,)), ((), ())), preferred_element_type=f32
        )
    own_ref[...] = own_grad
    sums_ref[...] = jnp.zeros_like(sums_ref)
    radial = (
        radial[0:count, 0:channels]
        + radial[count:, 0:channels]
        + radial[0:count, channels:]
        + radial[count:, channels:]
    )
    weight = jnp.zeros((channels, channels), f32)
    for g in range(GROUPS):
        z_hi, z_lo = split_two(acc_ref[g * ROWS : g * ROWS + channels, :] * gains_ref[g])
        for piece in (z_hi, z_lo):
            weight = weight + lax.dot_general(
                feat_ref[g], piece, (((1,), (1,)), ((), ())), preferred_element_type=f32
            )
        part = jnp.transpose(acc_ref[g * ROWS : (g + 1) * ROWS, :])
        part = jnp.concatenate([part, jnp.zeros((HIGH, 128 - ROWS), f32)], axis=1)
        zgrad_ref[g * HIGH : (g + 1) * HIGH, :] = part
    for n, (ref, kind) in enumerate(
        ((low_out, bf16), (mid_out, f32), (high_out, bf16), (core_out, f32))
    ):
        ref[...] = zgrad_ref[bounds[n] : bounds[n + 1], :].astype(kind)
    tall = jnp.concatenate([weight, radial], axis=0)
    cut = (channels + count) // 2
    sums_ref[0:cut, :] = jnp.concatenate([tall[0:cut], tall[cut:]], axis=1)


def short_range(pieces, ids, pos, dy, radial, mix, gain):
    channels, atoms = dy.shape
    listed = ids.shape[0]
    count = radial.shape[0]
    f32, bf16 = jnp.float32, jnp.bfloat16
    shaped = jax.ShapeDtypeStruct
    return fetching_call(
        short_kernel,
        (ids, pos, dy, radial, mix, gain),
        pieces,
        (
            shaped(pieces[0].shape, bf16),
            shaped(pieces[1].shape, f32),
            shaped(pieces[2].shape, bf16),
            shaped(pieces[3].shape, f32),
            shaped((8, atoms), f32),
            shaped((64, 128), f32),
        ),
        [
            pltpu.VMEM((GROUPS * ROWS, HIGH), bf16),
            pltpu.VMEM((GROUPS, channels, HIGH), bf16),
            pltpu.VMEM((GROUPS, channels, HIGH), f32),
            pltpu.VMEM((listed, atoms), jnp.int32),
            pltpu.VMEM((listed, atoms), jnp.int32),
            pltpu.VMEM((listed, channels, atoms), bf16),
            pltpu.VMEM((listed, 8, atoms), f32),
            pltpu.VMEM((listed, count, atoms), f32),
            pltpu.VMEM((listed, channels, atoms), f32),
            pltpu.VMEM((GROUPS * ROWS, HIGH), f32),
            pltpu.VMEM((GROUPS * HIGH, 128), bf16),
            pltpu.VMEM((GROUPS * HIGH, 128), f32),
        ],
    )


def fetching_call(
    kernel, fetched, resident, outs, scratch, early=None, in_specs=None, out_specs=None, flops=0,
    limit=True,
):
    n = len(fetched)

    def body(*refs):
        sources, rest = refs[:n], refs[n : -n - 1]
        buffers, sems = refs[-n - 1 : -1], refs[-1]
        copies = [
            pltpu.make_async_copy(sources[i], buffers[i], sems.at[i]) for i in range(n)
        ]
        if early is not None:
            early(*rest)
        for copy in copies:
            copy.start()
        for copy in copies:
            copy.wait()
        kernel(*buffers, *rest)

    cost = None
    if flops:
        cost = pl.CostEstimate(flops=flops, transcendentals=0, bytes_accessed=flops // 128)
    return pl.pallas_call(
        body,
        out_shape=outs,
        in_specs=[FAR] * n + list(in_specs or [WHOLE] * len(resident)),
        out_specs=tuple(out_specs or [WHOLE] * len(outs)),
        scratch_shapes=[
            *scratch,
            *[pltpu.VMEM(x.shape, x.dtype) for x in fetched],
            pltpu.SemaphoreType.DMA((n,)),
        ],
        compiler_params=LIMIT if limit else None,
        cost_estimate=cost,
    )(*fetched, *resident)


def from_behind(x, axis, by):
    devices = lax.axis_size(axis)
    return lax.ppermute(x, axis, [(i, (i + by) % devices) for i in range(devices)])


def chosen(parity):
    column = lax.broadcasted_iota(jnp.int32, (2 * CHUNK, CHUNK), 1)
    row = lax.broadcasted_iota(jnp.int32, (2 * CHUNK, CHUNK), 0)
    n = column // SHARE
    outer, inner, least = [lax.axis_size(axis) for axis in ("gy_0", "gy_1", "gz_0")]
    group = ((n // least) % outer * inner + n // (least * outer)) * least + n % least
    picked = group * (2 * SHARE) + column % SHARE + parity * SHARE
    return (row == picked).astype(jnp.float32).astype(jnp.bfloat16)


def pack_kernel(h_ref, kind_ref, pos_ref, miller_ref, cells_ref, core_ref, mine_ref, next_ref):
    f32, bf16 = jnp.float32, jnp.bfloat16
    _, atoms = h_ref.shape
    none = jnp.zeros((1, atoms), f32)
    halves = [split_two(pos_ref[d]) for d in range(3)]
    rows = jnp.concatenate(
        [h_ref[...].astype(f32)]
        + [half[0].astype(f32) for half in halves]
        + [none]
        + [half[1].astype(f32) for half in halves]
        + [none, kind_ref[...].astype(f32), jnp.zeros((127 - ROWS, atoms), f32)],
        axis=0,
    )
    flat = jnp.transpose(rows).astype(bf16)
    cells_ref[...] = flat[0 : cells_ref.shape[0]]
    core_ref[...] = flat[cells_ref.shape[0] :]
    m = miller_ref[...].astype(f32)
    tall = jnp.concatenate([m, m, m, jnp.zeros((7, m.shape[1]), f32)], axis=0).astype(bf16)
    runs = m.shape[1] // (2 * CHUNK)
    stack = jnp.concatenate(
        [tall[:, j * 2 * CHUNK : (j + 1) * 2 * CHUNK] for j in range(runs)], axis=0
    )
    core = lax.axis_index(PAIR)
    for parity, out_ref in ((core, mine_ref), (1 - core, next_ref)):
        got = jnp.dot(stack, chosen(parity), preferred_element_type=f32).astype(bf16)
        for j in range(runs):
            out_ref[:, j * CHUNK : (j + 1) * CHUNK] = got[j * 16 : (j + 1) * 16]


def pack(h, kinds, pos, miller):
    half = jax.ShapeDtypeStruct((16, miller.shape[1] // 2), jnp.bfloat16)
    return fetching_call(
        pack_kernel,
        (h, kinds, pos, miller),
        (),
        (
            jax.ShapeDtypeStruct((432, 128), jnp.bfloat16),
            jax.ShapeDtypeStruct((h.shape[1] - 432, 128), jnp.bfloat16),
            half,
            half,
        ),
        [],
        limit=False,
    )


def phase_kernel(
    pos_ref,
    h_ref,
    dy_ref,
    miller_ref,
    cos_out,
    sin_out,
    part_ref,
    cos_ref,
    sin_ref,
    flip_ref,
    rhs_ref,
    t_ref,
    sems,
):
    f32, bf16 = jnp.float32, jnp.bfloat16
    width = 2 * h_ref.shape[0]
    flip_ref[...] = jnp.transpose(jnp.concatenate([h_ref[...], dy_ref[...]], axis=0))
    axes = ("gx", GY, GZ)
    turns = jnp.concatenate(
        [
            (pos_ref[d] + lax.axis_index(axes[d]).astype(f32)) / float(lax.axis_size(axes[d]))
            for d in range(3)
        ],
        axis=0,
    )
    t_hi = turns.astype(bf16)
    t_mid, t_lo = split_two(turns - t_hi.astype(f32))
    rhs_ref[...] = jnp.concatenate(
        [t_hi, t_mid, t_lo, jnp.zeros((7, turns.shape[1]), bf16)], axis=0
    )
    steps = miller_ref.shape[1] // CHUNK
    rows, lanes = 16, 256

    def copies(i):
        at = pl.ds(pl.multiple_of(i * CHUNK, CHUNK), CHUNK)
        return [
            pltpu.make_async_copy(src.at[at], dst.at[at], sems.at[n, i])
            for n, (src, dst) in enumerate(
                ((cos_ref, cos_out), (sin_ref, sin_out))
            )
        ]

    def one(i, carry):
        base = pl.multiple_of(i * CHUNK, CHUNK)
        t_ref[...] = lax.dot_general(
            miller_ref[:, pl.ds(base, CHUNK)],
            rhs_ref[...],
            (((0,), (0,)), ((), ())),
            preferred_element_type=f32,
        )
        for top in range(0, CHUNK, rows):
            for left in range(0, t_ref.shape[1], lanes):
                t = t_ref[top : top + rows, left : left + lanes]
                r = t - jnp.round(t)
                u = jnp.abs(r) - 0.25
                q = u * u
                s = SIN_TERMS[3]
                for term in SIN_TERMS[2::-1]:
                    s = s * q + term
                c = COS_TERMS[4]
                for term in COS_TERMS[3::-1]:
                    c = c * q + term
                at = (pl.ds(base + top, rows), pl.ds(left, lanes))
                cos_ref[at] = -(s * u).astype(bf16)
                sin_ref[at] = jnp.where(r < 0.0, -c, c).astype(bf16)
        here = pl.ds(base, CHUNK)
        part_ref[here, 0:width] = jnp.dot(
            cos_ref[here, :], flip_ref[...], preferred_element_type=f32
        )
        part_ref[here, width:] = jnp.dot(
            sin_ref[here, :], flip_ref[...], preferred_element_type=f32
        )
        for copy in copies(i):
            copy.start()
        return carry

    lax.fori_loop(0, steps, one, 0)
    for i in range(steps):
        for copy in copies(i):
            copy.wait()


def phase_sums(pos, miller, h, dy):
    points = miller.shape[1]
    channels, atoms = h.shape
    width = 2 * channels
    wave = jax.ShapeDtypeStruct((points, atoms), jnp.bfloat16)
    sums = jax.ShapeDtypeStruct((points, 2 * width), jnp.float32)
    return fetching_call(
        phase_kernel,
        (pos, h, dy),
        (miller,),
        (wave, wave, sums),
        [
            pltpu.VMEM(wave.shape, wave.dtype),
            pltpu.VMEM(wave.shape, wave.dtype),
            pltpu.VMEM((atoms, width), jnp.bfloat16),
            pltpu.VMEM((16, atoms), jnp.bfloat16),
            pltpu.VMEM((CHUNK, atoms), jnp.float32),
            pltpu.SemaphoreType.DMA((2, points // CHUNK)),
        ],
        out_specs=(FAR, FAR, WHOLE),
        flops=6 * points * atoms * width,
    )


def wave_copies(cos_in, sin_in, cos_ref, sin_ref, sems, i):
    at = pl.ds(pl.multiple_of(i * CHUNK, CHUNK), CHUNK)
    return [
        pltpu.make_async_copy(cos_in.at[at], cos_ref.at[at], sems.at[0, i]),
        pltpu.make_async_copy(sin_in.at[at], sin_ref.at[at], sems.at[1, i]),
    ]


def ewald_early(cos_in, sin_in, *rest):
    for i in range(cos_in.shape[0] // CHUNK):
        for copy in wave_copies(cos_in, sin_in, *rest[-3:], i):
            copy.start()


def ewald_sums(coeff_ref, miller_ref, both, waves, sums_ref, turn_ref):
    f32 = jnp.float32
    width = both.shape[0]
    channels = width // 2
    run = CHUNK // (miller_ref.shape[1] // coeff_ref.shape[0])
    over_rows = (((0,), (0,)), ((), ()))

    def one(i, carry):
        for copy in wave_copies(*waves, i):
            copy.wait()
        at = pl.ds(pl.multiple_of(i * CHUNK, CHUNK), CHUNK)
        coeffs = coeff_ref[pl.ds(i * run, run), 0 : CHUNK // run].reshape(CHUNK, 2 * width)
        cos_part, sin_part = waves[2][at, :], waves[3][at, :]
        sums_ref[...] += lax.dot_general(
            coeffs[:, 0:channels], cos_part, over_rows, preferred_element_type=f32
        ) + lax.dot_general(
            coeffs[:, width : width + channels], sin_part, over_rows, preferred_element_type=f32
        )
        along_u = jnp.dot(coeffs[:, 0:width], both, preferred_element_type=f32)
        along_v = jnp.dot(coeffs[:, width:], both, preferred_element_type=f32)
        angle = along_v * cos_part.astype(f32) - along_u * sin_part.astype(f32)
        a_hi, a_lo = split_two(angle)
        m = miller_ref[:, at]
        turn_ref[...] += jnp.dot(m, a_hi, preferred_element_type=f32) + jnp.dot(
            m, a_lo, preferred_element_type=f32
        )
        return carry

    lax.fori_loop(0, miller_ref.shape[1] // CHUNK, one, 0)


def ewald_first(
    h_ref, dy_ref, cos_in, sin_in, coeff_ref, miller_ref, sums_ref, turn_ref, cos_ref, sin_ref, sems
):
    sums_ref[...] = jnp.zeros_like(sums_ref)
    turn_ref[...] = jnp.zeros_like(turn_ref)
    both = jnp.concatenate([h_ref[...], dy_ref[...]], axis=0)
    waves = (cos_in, sin_in, cos_ref, sin_ref, sems)
    ewald_sums(coeff_ref, miller_ref, both, waves, sums_ref, turn_ref)


def ewald_second(
    h_ref,
    dy_ref,
    kind_ref,
    gain_ref,
    mix_ref,
    cos_in,
    sin_in,
    coeff_ref,
    miller_ref,
    first_ref,
    angle_ref,
    inner_ref,
    upper_ref,
    lower_ref,
    core_ref,
    own_ref,
    mine_ref,
    atom_ref,
    pos_ref,
    weight_ref,
    radial_ref,
    sums_ref,
    turn_ref,
    cos_ref,
    sin_ref,
    sems,
):
    f32, bf16 = jnp.float32, jnp.bfloat16
    channels = h_ref.shape[0]
    cells = jnp.stack(
        [
            inner_ref[:, :, 0] + lower_ref[:, :, 0].astype(f32),
            inner_ref[:, :, 1],
            inner_ref[:, :, 2] + upper_ref[:, :, 0].astype(f32),
        ],
        axis=2,
    ).reshape(432, 128)
    flat = jnp.transpose(jnp.concatenate([cells, core_ref[...]], axis=0))
    gains = gains_of(gain_ref[...], kind_ref[...], (channels, flat.shape[1]))
    zscaled = (flat[0:channels] * gains).astype(bf16)
    halves = flat[channels : channels + 8]
    near = halves + pltpu.roll(halves, 4, 0) + own_ref[...]
    sums_ref[...] = first_ref[...] + jnp.dot(mix_ref[...], zscaled, preferred_element_type=f32)
    turn_ref[...] = angle_ref[...]
    both = jnp.concatenate([h_ref[...], dy_ref[...]], axis=0)
    waves = (cos_in, sin_in, cos_ref, sin_ref, sems)
    ewald_sums(coeff_ref, miller_ref, both, waves, sums_ref, turn_ref)
    atom_ref[...] = (dy_ref[...].astype(f32) + sums_ref[...]).astype(bf16)
    axes = ("gx", GY, GZ)
    for d in range(3):
        pos_ref[d] = (
            turn_ref[d : d + 1, :] * (circle_angle / lax.axis_size(axes[d])) + near[d : d + 1, :]
        )
    cut = (channels + radial_ref.shape[0]) // 2
    run = miller_ref.shape[1] // coeff_ref.shape[0]
    sides = []
    for ref in (mine_ref, coeff_ref):
        total = jnp.sum(ref[:, run : run + cut].astype(f32), axis=0)
        sides.append(total[:, 0:128] + total[:, 128:256])
    full = sides[0] + sides[1]
    tall = jnp.concatenate([full[:, 0:channels], full[:, channels:]], axis=0)
    weight_ref[...] = tall[0:channels]
    radial_ref[...] = tall[channels:]


def ewald(coeffs, cos_all, sin_all, miller, h, dy, more=(), params=(), basis=0):
    points, atoms = cos_all.shape
    channels = h.shape[0]
    last = len(more) > 0
    shaped = jax.ShapeDtypeStruct
    sums = shaped((channels, atoms), jnp.float32)
    turn = shaped((16, atoms), jnp.float32)
    scratch = [
        pltpu.VMEM(cos_all.shape, jnp.bfloat16),
        pltpu.VMEM(cos_all.shape, jnp.bfloat16),
        pltpu.SemaphoreType.DMA((2, points // CHUNK)),
    ]
    outs = (sums, turn)
    if last:
        scratch = [pltpu.VMEM(sums.shape, sums.dtype), pltpu.VMEM(turn.shape, turn.dtype)] + scratch
        outs = (
            shaped(sums.shape, jnp.bfloat16),
            shaped((3, 1, atoms), jnp.float32),
            shaped((channels, channels), jnp.float32),
            shaped((basis, channels), jnp.float32),
        )
    return fetching_call(
        ewald_second if last else ewald_first,
        (h, dy, *params),
        (cos_all, sin_all, coeffs, miller, *more),
        outs,
        scratch,
        early=ewald_early,
        in_specs=(FAR, FAR) + (WHOLE,) * (2 + len(more)),
        flops=8 * points * atoms * channels,
    )


def coefficients(totals, filt_rows, norm_atoms, norm_k):
    channels = filt_rows.shape[1]
    cos_struct = totals[:, 0:channels] * norm_atoms
    cos_back = totals[:, channels : 2 * channels] * norm_k
    sin_struct = totals[:, 2 * channels : 3 * channels] * norm_atoms
    sin_back = totals[:, 3 * channels : 4 * channels] * norm_k
    coeffs = jnp.concatenate(
        [
            norm_atoms * filt_rows * cos_back,
            norm_k * filt_rows * cos_struct,
            norm_atoms * filt_rows * sin_back,
            norm_k * filt_rows * sin_struct,
        ],
        axis=1,
    )
    return (coeffs, cos_struct * cos_back + sin_struct * sin_back)


def small_call(kernel, args, outs):
    return pl.pallas_call(
        kernel,
        out_shape=outs,
        in_specs=[WHOLE] * len(args),
        out_specs=(WHOLE,) * len(outs),
        compiler_params=LIMIT,
    )(*args)


def partial_kernel(pieces_ref, sums_ref, out_ref):
    f32, bf16 = jnp.float32, jnp.bfloat16
    tower, rows, _ = out_ref.shape
    width = pieces_ref.shape[2]
    total = jnp.sum(pieces_ref[...].astype(f32), axis=0)
    hi, lo = split_two(sums_ref[...])
    whole = jnp.concatenate([total, hi.astype(f32), lo.astype(f32)], axis=1)
    out_ref[...] = whole.reshape(tower, rows, width + 256).astype(bf16)


def partial_sums(pieces, sums, tower):
    shape = (tower, pieces.shape[1] // tower, pieces.shape[2] + 256)
    outs = (jax.ShapeDtypeStruct(shape, jnp.bfloat16),)
    return small_call(partial_kernel, (pieces, sums), outs)[0]


def coefficient_kernel(norm_atoms, norm_k, pieces_ref, filter_in, out_ref, filter_ref, tile, sem):
    f32 = jnp.float32
    _, share, _ = pieces_ref.shape
    channels = filter_ref.shape[1]
    width = 4 * channels
    start = lax.axis_index(GX_GY_GZ) * share
    lane = pl.multiple_of(start // 128 * 128, 128)
    copy = pltpu.make_async_copy(filter_in.at[:, pl.ds(lane, 128)], tile, sem)
    copy.start()
    both = jnp.sum(pieces_ref[...].astype(f32), axis=0)
    copy.wait()
    turned = jnp.transpose(tile[...])
    pick = lax.broadcasted_iota(jnp.int32, (128 // share, share, channels), 0)
    inside = (start - lane) // share
    filt = jnp.sum(
        jnp.where(pick == inside, turned.reshape(128 // share, share, channels), 0.0), axis=0
    )
    coeffs, filter_ref[...] = coefficients(both[:, 0:width], filt, norm_atoms, norm_k)
    hi, lo = split_two(both[:, width : width + 128] + both[:, width + 128 :])
    sent = jnp.concatenate([coeffs, hi.astype(f32), lo.astype(f32)], axis=1)
    out_ref[...] = jnp.broadcast_to(sent[None], out_ref.shape).astype(jnp.bfloat16)


def make_coefficients(pieces, filter_columns, norm_atoms, norm_k):
    share, channels = pieces.shape[1], filter_columns.shape[0]
    return pl.pallas_call(
        functools.partial(coefficient_kernel, norm_atoms, norm_k),
        out_shape=(
            jax.ShapeDtypeStruct(pieces.shape, jnp.bfloat16),
            jax.ShapeDtypeStruct((share, channels), jnp.float32),
        ),
        in_specs=[WHOLE, FAR],
        out_specs=(WHOLE, WHOLE),
        scratch_shapes=[pltpu.VMEM((channels, 128), jnp.float32), pltpu.SemaphoreType.DMA],
        compiler_params=LIMIT,
        name="coefficients",
    )(pieces, filter_columns)


def strip_kernel(got_ref, out_ref):
    f32 = jnp.float32
    tower, share, _ = got_ref.shape
    width = out_ref.shape[2]
    run, cut = tower * share, out_ref.shape[1] - tower * share
    got = got_ref[...].astype(f32).reshape(run, width + 256)
    strip = jnp.concatenate([got[:, 0:width], got[0:cut, width:]], axis=0)
    out_ref[...] = jnp.broadcast_to(strip[None], out_ref.shape).astype(jnp.bfloat16)


def make_strip(got, sheet, width, cut):
    shape = (sheet, got.shape[0] * got.shape[1] + cut, width)
    return small_call(strip_kernel, (got,), (jax.ShapeDtypeStruct(shape, got.dtype),))[0]


def fold_x_kernel(mid_ref, upper_ref, lower_ref, first_ref, last_ref, rest_ref):
    f32, bf16 = jnp.float32, jnp.bfloat16
    for n in range(3):
        plane = mid_ref[n]
        if n == 0:
            plane = plane + lower_ref[0].astype(f32)
        if n == 2:
            plane = plane + upper_ref[0].astype(f32)
        first_ref[n] = plane[0:1].astype(bf16)
        last_ref[n] = plane[4:5].astype(bf16)
        rest_ref[n] = plane[1:4]


def fold_x(mid, upper, lower):
    side = jax.ShapeDtypeStruct((3, 1, 5, 16, 128), jnp.bfloat16)
    rest = jax.ShapeDtypeStruct((3, 3, 5, 16, 128), jnp.float32)
    return small_call(fold_x_kernel, (mid, upper, lower), (side, side, rest))


def fold_y_kernel(rest_ref, upper_ref, lower_ref, first_ref, last_ref, inner_ref):
    f32, bf16 = jnp.float32, jnp.bfloat16
    for n in range(3):
        plane = rest_ref[:, n]
        if n == 0:
            plane = plane + lower_ref[:, 0].astype(f32)
        if n == 2:
            plane = plane + upper_ref[:, 0].astype(f32)
        first_ref[:, n] = plane[:, 0:1].astype(bf16)
        last_ref[:, n] = plane[:, 4:5].astype(bf16)
        inner_ref[:, n] = plane[:, 1:4]


def fold_y(rest, upper, lower):
    side = jax.ShapeDtypeStruct((3, 3, 1, 16, 128), jnp.bfloat16)
    inner = jax.ShapeDtypeStruct((3, 3, 3, 16, 128), jnp.float32)
    return small_call(fold_y_kernel, (rest, upper, lower), (side, side, inner))


def sent_out(x, axis, dim):
    length = x.shape[dim]
    before = from_behind(lax.slice_in_dim(x, length - 1, length, axis=dim), axis, 1)
    after = from_behind(lax.slice_in_dim(x, 0, 1, axis=dim), axis, -1)
    return before, after


def whole(
    atom_embedding,
    output_adjoint,
    fractional_coords,
    element_labels,
    adjacent_ghost_entries,
    miller_triples,
    reciprocal_kernel,
    channel_mixing_matrix,
    element_channel_factor,
    distance_kernel,
):
    h = atom_embedding[0, 0, 0]
    dy = output_adjoint[0, 0, 0]
    pos = fractional_coords[0, 0, 0][:, None, :]
    kinds = element_labels[0, 0]
    channels, atoms = h.shape
    points = miller_triples.shape[1]
    devices = lax.axis_size(GX_GY_GZ)
    norm_atoms = (atoms * devices) ** (-0.5)
    norm_k = points ** (-0.5)
    half = points // 2

    cells, core, miller_mine, miller_next = pack(h, kinds, pos, miller_triples)
    cells = cells.reshape(3, 3, 3, 16, 128)
    below, above = sent_out(cells, GZ, 2)
    cos_next, sin_next, part_next = phase_sums(pos, miller_next, h, dy)
    received = from_behind(part_next, PAIR, 1)
    cells = jnp.concatenate([below, cells, above], axis=2)
    below, above = sent_out(cells, GY, 1)
    cos_mine, sin_mine, part_mine = phase_sums(pos, miller_mine, h, dy)
    cells = jnp.concatenate([below, cells, above], axis=1)
    below, above = sent_out(cells, "gx", 0)
    sheet, tower = lax.axis_size(SHEET), lax.axis_size(TOWER)
    width = 4 * channels
    paired = (part_mine + received).astype(jnp.bfloat16)
    pieces = lax.all_to_all(paired.reshape(sheet, half // sheet, width), SHEET, 0, 0)

    low, mid, high, core_grad, own_grad, sums = short_range(
        (below.reshape(400, 128), cells.reshape(1200, 128), above.reshape(400, 128), core),
        adjacent_ghost_entries[0, 0, 0],
        pos,
        dy,
        distance_kernel,
        channel_mixing_matrix,
        element_channel_factor,
    )
    parts = partial_sums(pieces, sums, tower)
    pieces = lax.all_to_all(parts, TOWER, 0, 0)
    sent, filter_share = make_coefficients(pieces, reciprocal_kernel.T, norm_atoms, norm_k)
    got = lax.all_to_all(sent, TOWER, 0, 0)

    upper = from_behind(low.reshape(1, 5, 5, 16, 128), "gx", -1)
    lower = from_behind(high.reshape(1, 5, 5, 16, 128), "gx", 1)
    first, last, rest = fold_x(mid.reshape(3, 5, 5, 16, 128), upper, lower)
    upper, lower = from_behind(first, GY, -1), from_behind(last, GY, 1)
    strip = make_strip(got, sheet, width, (channels + distance_kernel.shape[0]) // 2)
    got = lax.all_to_all(strip, SHEET, 0, 0)
    first, last, inner = fold_y(rest, upper, lower)
    upper, lower = from_behind(first, GZ, -1), from_behind(last, GZ, 1)
    got_next = from_behind(got, PAIR, 1)
    early_sums = ewald(got, cos_mine, sin_mine, miller_mine, h, dy)
    atom_grad, position_grad, weight_grad, radial_grad = ewald(
        got_next,
        cos_next,
        sin_next,
        miller_next,
        h,
        dy,
        (*early_sums, inner, upper, lower, core_grad, own_grad, got),
        (kinds, element_channel_factor, channel_mixing_matrix),
        distance_kernel.shape[0],
    )
    position_grad = position_grad[:, 0, :]
    return (
        atom_grad[None, None, None],
        position_grad[None, None, None],
        weight_grad,
        radial_grad,
        filter_share,
    )


def solution(mesh):
    finer = Mesh(
        mesh.devices.reshape(mesh.shape["gx"], 4, 4, 2, 2), ("gx", "gy_0", "gy_1", "gz_0", "gz_1")
    )
    in_specs = (
        P("gx", GY, GZ, None, None),
        P("gx", GY, GZ, None, None),
        P("gx", GY, GZ, None, None),
        P("gx", GY, GZ, None),
        P("gx", GY, GZ, None, None),
        P(),
        P(),
        P(),
        P(),
        P(),
    )
    out_specs = (
        P("gx", GY, GZ, None, None),
        P("gx", GY, GZ, None, None),
        P(),
        P(),
        P(GX_GY_GZ, None),
    )
    return jax.shard_map(whole, mesh=finer, in_specs=in_specs, out_specs=out_specs, check_vma=False)
```

```python
import functools
import math

import jax
import jax.numpy as jnp
from jax import lax
from jax.experimental import pallas as pl
from jax.experimental.pallas import tpu as pltpu
from jax.sharding import Mesh
from jax.sharding import PartitionSpec as P


GY = ("gy_0", "gy_1")
GZ = ("gz_0", "gz_1")

SHEET = ("gx", "gy_1")
TOWER = ("gy_0", "gz_0")
PAIR = "gz_1"
GX_GY_GZ = ("gx", "gy_0", "gy_1", "gz_0", "gz_1")

circle_angle = 2.0 * math.pi
CHUNK = 256
SHARE = 8
SIN_TERMS = (6.28316404, -41.33714227, 81.34076528, -70.99339569)
COS_TERMS = (0.99999995, -19.73917143, 64.93459054, -85.24032775, 56.2423573)
WHOLE = pl.BlockSpec(memory_space=pltpu.VMEM)
FAR = pl.BlockSpec(memory_space=pltpu.HBM)
LIMIT = pltpu.CompilerParams(vmem_limit_bytes=20 * 1024 * 1024)

reach_sq = 0.75
GROUPS = 9
ROWS = 72
BLOCKS = 135
HIGH = BLOCKS // GROUPS * 16


def split_two(x):
    high = x.astype(jnp.bfloat16)
    return high, (x - high.astype(jnp.float32)).astype(jnp.bfloat16)


def row_pick(first, second, third, shape):
    row = lax.broadcasted_iota(jnp.int32, shape, 0) % 4
    spread = lambda v: jnp.broadcast_to(v, shape)
    return jnp.where(
        row == 0,
        spread(first),
        jnp.where(row == 1, spread(second), jnp.where(row == 2, spread(third), 0.0)),
    )


def gains_of(gain_rows, labels, shape):
    columns = jnp.transpose(gain_rows)
    gains = jnp.zeros(shape, jnp.float32)
    for kind in range(gain_rows.shape[0]):
        gains = jnp.where(labels == kind, columns[:, kind : kind + 1], gains)
    return gains


def short_kernel(
    ids_ref,
    pos_ref,
    dy_ref,
    radial_ref,
    mix_ref,
    gain_ref,
    below_ref,
    cells_ref,
    above_ref,
    core_ref,
    low_out,
    mid_out,
    high_out,
    core_out,
    own_ref,
    sums_ref,
    lhs_ref,
    feat_ref,
    gains_ref,
    high_ref,
    low_ref,
    near_ref,
    rel_ref,
    basis_ref,
    filt_ref,
    acc_ref,
    table_ref,
    zgrad_ref,
):
    channels, atoms = dy_ref.shape
    side, inner, rest = below_ref.shape[0], cells_ref.shape[0], core_ref.shape[0]
    bounds = (0, side, side + inner, 2 * side + inner, 2 * side + inner + rest)
    for n, ref in enumerate((below_ref, cells_ref, above_ref, core_ref)):
        table_ref[bounds[n] : bounds[n + 1], :] = ref[...]
    table_ref[bounds[4] :, :] = jnp.zeros((GROUPS * HIGH - bounds[4], 128), jnp.bfloat16)
    listed = ids_ref.shape[0]
    count = radial_ref.shape[0]
    f32, bf16 = jnp.float32, jnp.bfloat16
    spacing = reach_sq / (count - 1)
    width = 2.0 * spacing
    share = listed ** (-0.5)
    for g in range(GROUPS):
        part = jnp.transpose(table_ref[g * HIGH : (g + 1) * HIGH, :].astype(f32))
        feat = part[0:channels].astype(bf16)
        gains = gains_of(gain_ref[...], part[ROWS : ROWS + 1], (channels, HIGH))
        feat_ref[g] = feat
        gains_ref[g] = gains
        z = lax.dot_general(
            mix_ref[...], feat, (((0,), (0,)), ((), ())), preferred_element_type=f32
        )
        lhs_ref[g * ROWS : (g + 1) * ROWS, :] = jnp.concatenate(
            [z * gains, part[channels:ROWS]], axis=0
        ).astype(bf16)
    ids = ids_ref[...]
    slot = lax.shift_right_logical(ids, 9)
    atom = jnp.bitwise_and(ids, 511)
    block = lax.shift_right_logical(atom, 4)
    ox = slot // 9
    oy = (slot // 3) % 3
    oz = slot % 3
    qx = block // 9
    qy = (block // 3) % 3
    qz = block % 3
    grid = ((3 * ox + qx - 2) * 5 + 3 * oy + qy - 2) * 5 + 3 * oz + qz - 2
    grid = jnp.where(block >= 27, block + (125 - 27), grid)
    low = grid // (BLOCKS // GROUPS)
    high = (grid - low * (BLOCKS // GROUPS)) * 16 + jnp.bitwise_and(atom, 15)
    high_ref[...] = high
    low_ref[...] = low
    offs = [(o - 1).astype(f32) for o in (ox, oy, oz)]
    own8 = row_pick(pos_ref[0], pos_ref[1], pos_ref[2], (8, atoms))
    w_hi, w_lo = split_two(radial_ref[...])
    w_stack = jnp.concatenate([w_hi, w_hi, w_lo], axis=0)
    centre = lax.broadcasted_iota(jnp.int32, (count, 1), 0).astype(f32) * spacing
    iota = lax.broadcasted_iota(jnp.int32, (HIGH, atoms), 0)

    def hot(j):
        return (high_ref[pl.ds(j, 1), :] == iota).astype(f32).astype(bf16)

    agg = jnp.zeros((channels, atoms), f32)
    for j in range(listed):
        found = jnp.dot(lhs_ref[...], hot(j), preferred_element_type=f32)
        low_j = low_ref[j : j + 1, :]
        near = found[0:ROWS]
        for g in range(1, GROUPS):
            near = jnp.where(low_j == g, found[g * ROWS : (g + 1) * ROWS], near)
        near_z = near[0:channels]
        near_ref[j] = near_z.astype(bf16)
        halves = near[channels : channels + 8]
        off8 = row_pick(offs[0][j : j + 1], offs[1][j : j + 1], offs[2][j : j + 1], (8, atoms))
        rel = halves + pltpu.roll(halves, 4, 0) + off8 - own8
        rel_ref[j] = rel
        dist = 0.5 * jnp.sum(rel * rel, axis=0, keepdims=True)
        scaled = (dist - centre) / width
        basis = jnp.exp(-(scaled * scaled))
        basis_ref[j] = basis
        b_hi, b_lo = split_two(basis)
        filt = lax.dot_general(
            w_stack,
            jnp.concatenate([b_hi, b_lo, b_hi], axis=0),
            (((0,), (0,)), ((), ())),
            preferred_element_type=f32,
        )
        filt_ref[j] = filt
        agg = agg + filt * near_z
    agg = agg * share
    gate = 1.0 / (1.0 + jnp.exp(-agg))
    g_all = dy_ref[...].astype(f32) * (gate * (1.0 + agg * (1.0 - gate))) * share
    acc_ref[...] = jnp.zeros_like(acc_ref)
    own_grad = jnp.zeros((8, atoms), f32)
    radial = jnp.zeros((2 * count, 2 * channels), f32)
    w_wide = jnp.concatenate([w_hi, w_hi, w_lo], axis=1)
    for j in range(listed):
        near_z = near_ref[j].astype(f32)
        dz = filt_ref[j] * g_all
        df = near_z * g_all
        f_hi, f_lo = split_two(df)
        basis = basis_ref[j]
        b_hi, b_lo = split_two(basis)
        radial = radial + lax.dot_general(
            jnp.concatenate([b_hi, b_lo], axis=0),
            jnp.concatenate([f_hi, f_lo], axis=0),
            (((1,), (1,)), ((), ())),
            preferred_element_type=f32,
        )
        dbasis = jnp.dot(
            w_wide, jnp.concatenate([f_hi, f_lo, f_hi], axis=0), preferred_element_type=f32
        )
        rel = rel_ref[j]
        dist = 0.5 * jnp.sum(rel * rel, axis=0, keepdims=True)
        slope = dbasis * basis * (dist - centre)
        ddist = jnp.sum(slope, axis=0, keepdims=True) * (-2.0 / (width * width))
        gpos = rel * (2.0 * ddist)
        own_grad = own_grad - gpos
        p_hi = gpos.astype(bf16).astype(f32)
        row8 = lax.broadcasted_iota(jnp.int32, (8, atoms), 0)
        tail = jnp.where(row8 < 4, p_hi, gpos - p_hi)
        full = jnp.concatenate([dz, tail], axis=0)
        low_j = low_ref[j : j + 1, :]
        spread = jnp.concatenate(
            [jnp.where(low_j == g, full, 0.0) for g in range(GROUPS)], axis=0
        ).astype(bf16)
        acc_ref[...] += lax.dot_general(
            spread, hot(j), (((1,), (1,)), ((), ())), preferred_element_type=f32
        )
    own_ref[...] = own_grad
    sums_ref[...] = jnp.zeros_like(sums_ref)
    radial = (
        radial[0:count, 0:channels]
        + radial[count:, 0:channels]
        + radial[0:count, channels:]
        + radial[count:, channels:]
    )
    weight = jnp.zeros((channels, channels), f32)
    for g in range(GROUPS):
        z_hi, z_lo = split_two(acc_ref[g * ROWS : g * ROWS + channels, :] * gains_ref[g])
        for piece in (z_hi, z_lo):
            weight = weight + lax.dot_general(
                feat_ref[g], piece, (((1,), (1,)), ((), ())), preferred_element_type=f32
            )
        part = jnp.transpose(acc_ref[g * ROWS : (g + 1) * ROWS, :])
        part = jnp.concatenate([part, jnp.zeros((HIGH, 128 - ROWS), f32)], axis=1)
        zgrad_ref[g * HIGH : (g + 1) * HIGH, :] = part
    for n, (ref, kind) in enumerate(
        ((low_out, bf16), (mid_out, f32), (high_out, bf16), (core_out, f32))
    ):
        ref[...] = zgrad_ref[bounds[n] : bounds[n + 1], :].astype(kind)
    tall = jnp.concatenate([weight, radial], axis=0)
    cut = (channels + count) // 2
    sums_ref[0:cut, :] = jnp.concatenate([tall[0:cut], tall[cut:]], axis=1)


def short_range(pieces, ids, pos, dy, radial, mix, gain):
    channels, atoms = dy.shape
    listed = ids.shape[0]
    count = radial.shape[0]
    f32, bf16 = jnp.float32, jnp.bfloat16
    shaped = jax.ShapeDtypeStruct
    return fetching_call(
        short_kernel,
        (ids, pos, dy, radial, mix, gain),
        pieces,
        (
            shaped(pieces[0].shape, bf16),
            shaped(pieces[1].shape, f32),
            shaped(pieces[2].shape, bf16),
            shaped(pieces[3].shape, f32),
            shaped((8, atoms), f32),
            shaped((64, 128), f32),
        ),
        [
            pltpu.VMEM((GROUPS * ROWS, HIGH), bf16),
            pltpu.VMEM((GROUPS, channels, HIGH), bf16),
            pltpu.VMEM((GROUPS, channels, HIGH), f32),
            pltpu.VMEM((listed, atoms), jnp.int32),
            pltpu.VMEM((listed, atoms), jnp.int32),
            pltpu.VMEM((listed, channels, atoms), bf16),
            pltpu.VMEM((listed, 8, atoms), f32),
            pltpu.VMEM((listed, count, atoms), f32),
            pltpu.VMEM((listed, channels, atoms), f32),
            pltpu.VMEM((GROUPS * ROWS, HIGH), f32),
            pltpu.VMEM((GROUPS * HIGH, 128), bf16),
            pltpu.VMEM((GROUPS * HIGH, 128), f32),
        ],
        limit=False,
    )


def fetching_call(
    kernel, fetched, resident, outs, scratch, early=None, in_specs=None, out_specs=None, flops=0,
    limit=True,
):
    n = len(fetched)

    def body(*refs):
        sources, rest = refs[:n], refs[n : -n - 1]
        buffers, sems = refs[-n - 1 : -1], refs[-1]
        copies = [
            pltpu.make_async_copy(sources[i], buffers[i], sems.at[i]) for i in range(n)
        ]
        if early is not None:
            early(*rest)
        for copy in copies:
            copy.start()
        for copy in copies:
            copy.wait()
        kernel(*buffers, *rest)

    cost = None
    if flops:
        cost = pl.CostEstimate(flops=flops, transcendentals=0, bytes_accessed=flops // 128)
    return pl.pallas_call(
        body,
        out_shape=outs,
        in_specs=[FAR] * n + list(in_specs or [WHOLE] * len(resident)),
        out_specs=tuple(out_specs or [WHOLE] * len(outs)),
        scratch_shapes=[
            *scratch,
            *[pltpu.VMEM(x.shape, x.dtype) for x in fetched],
            pltpu.SemaphoreType.DMA((n,)),
        ],
        compiler_params=LIMIT if limit else None,
        cost_estimate=cost,
    )(*fetched, *resident)


def from_behind(x, axis, by):
    devices = lax.axis_size(axis)
    return lax.ppermute(x, axis, [(i, (i + by) % devices) for i in range(devices)])


def chosen(parity):
    column = lax.broadcasted_iota(jnp.int32, (2 * CHUNK, CHUNK), 1)
    row = lax.broadcasted_iota(jnp.int32, (2 * CHUNK, CHUNK), 0)
    n = column // SHARE
    outer, inner, least = [lax.axis_size(axis) for axis in ("gy_0", "gy_1", "gz_0")]
    group = ((n // least) % outer * inner + n // (least * outer)) * least + n % least
    picked = group * (2 * SHARE) + column % SHARE + parity * SHARE
    return (row == picked).astype(jnp.float32).astype(jnp.bfloat16)


def pack_kernel(
    h_ref,
    kind_ref,
    pos_ref,
    miller_ref,
    cells_ref,
    core_ref,
    first_ref,
    last_ref,
    mine_ref,
    next_ref,
):
    f32, bf16 = jnp.float32, jnp.bfloat16
    _, atoms = h_ref.shape
    none = jnp.zeros((1, atoms), f32)
    halves = [split_two(pos_ref[d]) for d in range(3)]
    rows = jnp.concatenate(
        [h_ref[...].astype(f32)]
        + [half[0].astype(f32) for half in halves]
        + [none]
        + [half[1].astype(f32) for half in halves]
        + [none, kind_ref[...].astype(f32), jnp.zeros((127 - ROWS, atoms), f32)],
        axis=0,
    )
    flat = jnp.transpose(rows).astype(bf16)
    cells_ref[...] = flat[0 : cells_ref.shape[0]]
    core_ref[...] = flat[cells_ref.shape[0] :]
    for n in range(9):
        first_ref[n // 3, n % 3, 0] = flat[48 * n : 48 * n + 16]
        last_ref[n // 3, n % 3, 0] = flat[48 * n + 32 : 48 * n + 48]
    m = miller_ref[...].astype(f32)
    tall = jnp.concatenate([m, m, m, jnp.zeros((7, m.shape[1]), f32)], axis=0).astype(bf16)
    runs = m.shape[1] // (2 * CHUNK)
    stack = jnp.concatenate(
        [tall[:, j * 2 * CHUNK : (j + 1) * 2 * CHUNK] for j in range(runs)], axis=0
    )
    core = lax.axis_index(PAIR)
    for parity, out_ref in ((core, mine_ref), (1 - core, next_ref)):
        got = jnp.dot(stack, chosen(parity), preferred_element_type=f32).astype(bf16)
        for j in range(runs):
            out_ref[:, j * CHUNK : (j + 1) * CHUNK] = got[j * 16 : (j + 1) * 16]


def pack(h, kinds, pos, miller):
    half = jax.ShapeDtypeStruct((16, miller.shape[1] // 2), jnp.bfloat16)
    side = jax.ShapeDtypeStruct((3, 3, 1, 16, 128), jnp.bfloat16)
    return fetching_call(
        pack_kernel,
        (h, kinds, pos, miller),
        (),
        (
            jax.ShapeDtypeStruct((432, 128), jnp.bfloat16),
            jax.ShapeDtypeStruct((h.shape[1] - 432, 128), jnp.bfloat16),
            side,
            side,
            half,
            half,
        ),
        [],
        limit=False,
    )


def phase_kernel(
    pos_ref,
    h_ref,
    dy_ref,
    miller_ref,
    cos_out,
    sin_out,
    part_ref,
    cos_ref,
    sin_ref,
    flip_ref,
    rhs_ref,
    t_ref,
    sems,
):
    f32, bf16 = jnp.float32, jnp.bfloat16
    width = 2 * h_ref.shape[0]
    flip_ref[...] = jnp.transpose(jnp.concatenate([h_ref[...], dy_ref[...]], axis=0))
    axes = ("gx", GY, GZ)
    turns = jnp.concatenate(
        [
            (pos_ref[d] + lax.axis_index(axes[d]).astype(f32)) / float(lax.axis_size(axes[d]))
            for d in range(3)
        ],
        axis=0,
    )
    t_hi = turns.astype(bf16)
    t_mid, t_lo = split_two(turns - t_hi.astype(f32))
    rhs_ref[...] = jnp.concatenate(
        [t_hi, t_mid, t_lo, jnp.zeros((7, turns.shape[1]), bf16)], axis=0
    )
    steps = miller_ref.shape[1] // CHUNK
    rows, lanes = 16, 256

    def copies(i):
        at = pl.ds(pl.multiple_of(i * CHUNK, CHUNK), CHUNK)
        return [
            pltpu.make_async_copy(src.at[at], dst.at[at], sems.at[n, i])
            for n, (src, dst) in enumerate(
                ((cos_ref, cos_out), (sin_ref, sin_out))
            )
        ]

    def one(i, carry):
        base = pl.multiple_of(i * CHUNK, CHUNK)
        t_ref[...] = lax.dot_general(
            miller_ref[:, pl.ds(base, CHUNK)],
            rhs_ref[...],
            (((0,), (0,)), ((), ())),
            preferred_element_type=f32,
        )
        for top in range(0, CHUNK, rows):
            for left in range(0, t_ref.shape[1], lanes):
                t = t_ref[top : top + rows, left : left + lanes]
                r = t - jnp.round(t)
                u = jnp.abs(r) - 0.25
                q = u * u
                s = SIN_TERMS[3]
                for term in SIN_TERMS[2::-1]:
                    s = s * q + term
                c = COS_TERMS[4]
                for term in COS_TERMS[3::-1]:
                    c = c * q + term
                at = (pl.ds(base + top, rows), pl.ds(left, lanes))
                cos_ref[at] = -(s * u).astype(bf16)
                sin_ref[at] = jnp.where(r < 0.0, -c, c).astype(bf16)
        here = pl.ds(base, CHUNK)
        part_ref[here, 0:width] = jnp.dot(
            cos_ref[here, :], flip_ref[...], preferred_element_type=f32
        )
        part_ref[here, width:] = jnp.dot(
            sin_ref[here, :], flip_ref[...], preferred_element_type=f32
        )
        for copy in copies(i):
            copy.start()
        return carry

    lax.fori_loop(0, steps, one, 0)
    for i in range(steps):
        for copy in copies(i):
            copy.wait()


def phase_sums(pos, miller, h, dy):
    points = miller.shape[1]
    channels, atoms = h.shape
    width = 2 * channels
    wave = jax.ShapeDtypeStruct((points, atoms), jnp.bfloat16)
    sums = jax.ShapeDtypeStruct((points, 2 * width), jnp.float32)
    return fetching_call(
        phase_kernel,
        (pos, h, dy),
        (miller,),
        (wave, wave, sums),
        [
            pltpu.VMEM(wave.shape, wave.dtype),
            pltpu.VMEM(wave.shape, wave.dtype),
            pltpu.VMEM((atoms, width), jnp.bfloat16),
            pltpu.VMEM((16, atoms), jnp.bfloat16),
            pltpu.VMEM((CHUNK, atoms), jnp.float32),
            pltpu.SemaphoreType.DMA((2, points // CHUNK)),
        ],
        out_specs=(FAR, FAR, WHOLE),
        flops=6 * points * atoms * width,
    )


def wave_copies(cos_in, sin_in, cos_ref, sin_ref, sems, i):
    at = pl.ds(pl.multiple_of(i * CHUNK, CHUNK), CHUNK)
    return [
        pltpu.make_async_copy(cos_in.at[at], cos_ref.at[at], sems.at[0, i]),
        pltpu.make_async_copy(sin_in.at[at], sin_ref.at[at], sems.at[1, i]),
    ]


def ewald_early(cos_in, sin_in, *rest):
    for i in range(cos_in.shape[0] // CHUNK):
        for copy in wave_copies(cos_in, sin_in, *rest[-3:], i):
            copy.start()


def ewald_sums(coeff_ref, miller_ref, both, waves, sums_ref, turn_ref):
    f32 = jnp.float32
    width = both.shape[0]
    channels = width // 2
    run = CHUNK // (miller_ref.shape[1] // coeff_ref.shape[0])
    over_rows = (((0,), (0,)), ((), ()))

    def one(i, carry):
        for copy in wave_copies(*waves, i):
            copy.wait()
        at = pl.ds(pl.multiple_of(i * CHUNK, CHUNK), CHUNK)
        coeffs = coeff_ref[pl.ds(i * run, run), 0 : CHUNK // run].reshape(CHUNK, 2 * width)
        cos_part, sin_part = waves[2][at, :], waves[3][at, :]
        sums_ref[...] += lax.dot_general(
            coeffs[:, 0:channels], cos_part, over_rows, preferred_element_type=f32
        ) + lax.dot_general(
            coeffs[:, width : width + channels], sin_part, over_rows, preferred_element_type=f32
        )
        along_u = jnp.dot(coeffs[:, 0:width], both, preferred_element_type=f32)
        along_v = jnp.dot(coeffs[:, width:], both, preferred_element_type=f32)
        angle = along_v * cos_part.astype(f32) - along_u * sin_part.astype(f32)
        a_hi, a_lo = split_two(angle)
        m = miller_ref[:, at]
        turn_ref[...] += jnp.dot(m, a_hi, preferred_element_type=f32) + jnp.dot(
            m, a_lo, preferred_element_type=f32
        )
        return carry

    lax.fori_loop(0, miller_ref.shape[1] // CHUNK, one, 0)


def ewald_first(
    h_ref, dy_ref, cos_in, sin_in, coeff_ref, miller_ref, sums_ref, turn_ref, cos_ref, sin_ref, sems
):
    sums_ref[...] = jnp.zeros_like(sums_ref)
    turn_ref[...] = jnp.zeros_like(turn_ref)
    both = jnp.concatenate([h_ref[...], dy_ref[...]], axis=0)
    waves = (cos_in, sin_in, cos_ref, sin_ref, sems)
    ewald_sums(coeff_ref, miller_ref, both, waves, sums_ref, turn_ref)


def ewald_second(
    h_ref,
    dy_ref,
    kind_ref,
    gain_ref,
    mix_ref,
    cos_in,
    sin_in,
    coeff_ref,
    miller_ref,
    first_ref,
    angle_ref,
    inner_ref,
    upper_ref,
    lower_ref,
    core_ref,
    own_ref,
    mine_ref,
    atom_ref,
    pos_ref,
    weight_ref,
    radial_ref,
    sums_ref,
    turn_ref,
    cos_ref,
    sin_ref,
    sems,
):
    f32, bf16 = jnp.float32, jnp.bfloat16
    channels = h_ref.shape[0]
    cells = jnp.stack(
        [
            inner_ref[:, :, 0] + lower_ref[:, :, 0].astype(f32),
            inner_ref[:, :, 1],
            inner_ref[:, :, 2] + upper_ref[:, :, 0].astype(f32),
        ],
        axis=2,
    ).reshape(432, 128)
    flat = jnp.transpose(jnp.concatenate([cells, core_ref[...]], axis=0))
    gains = gains_of(gain_ref[...], kind_ref[...], (channels, flat.shape[1]))
    zscaled = (flat[0:channels] * gains).astype(bf16)
    halves = flat[channels : channels + 8]
    near = halves + pltpu.roll(halves, 4, 0) + own_ref[...]
    sums_ref[...] = first_ref[...] + jnp.dot(mix_ref[...], zscaled, preferred_element_type=f32)
    turn_ref[...] = angle_ref[...]
    both = jnp.concatenate([h_ref[...], dy_ref[...]], axis=0)
    waves = (cos_in, sin_in, cos_ref, sin_ref, sems)
    ewald_sums(coeff_ref, miller_ref, both, waves, sums_ref, turn_ref)
    atom_ref[...] = (dy_ref[...].astype(f32) + sums_ref[...]).astype(bf16)
    axes = ("gx", GY, GZ)
    for d in range(3):
        pos_ref[d] = (
            turn_ref[d : d + 1, :] * (circle_angle / lax.axis_size(axes[d])) + near[d : d + 1, :]
        )
    cut = (channels + radial_ref.shape[0]) // 2
    run = miller_ref.shape[1] // coeff_ref.shape[0]
    sides = []
    for ref in (mine_ref, coeff_ref):
        total = jnp.sum(ref[:, run : run + cut].astype(f32), axis=0)
        sides.append(total[:, 0:128] + total[:, 128:256])
    full = sides[0] + sides[1]
    tall = jnp.concatenate([full[:, 0:channels], full[:, channels:]], axis=0)
    weight_ref[...] = tall[0:channels]
    radial_ref[...] = tall[channels:]


def ewald(coeffs, cos_all, sin_all, miller, h, dy, more=(), params=(), basis=0):
    points, atoms = cos_all.shape
    channels = h.shape[0]
    last = len(more) > 0
    shaped = jax.ShapeDtypeStruct
    sums = shaped((channels, atoms), jnp.float32)
    turn = shaped((16, atoms), jnp.float32)
    scratch = [
        pltpu.VMEM(cos_all.shape, jnp.bfloat16),
        pltpu.VMEM(cos_all.shape, jnp.bfloat16),
        pltpu.SemaphoreType.DMA((2, points // CHUNK)),
    ]
    outs = (sums, turn)
    if last:
        scratch = [pltpu.VMEM(sums.shape, sums.dtype), pltpu.VMEM(turn.shape, turn.dtype)] + scratch
        outs = (
            shaped(sums.shape, jnp.bfloat16),
            shaped((3, 1, atoms), jnp.float32),
            shaped((channels, channels), jnp.float32),
            shaped((basis, channels), jnp.float32),
        )
    return fetching_call(
        ewald_second if last else ewald_first,
        (h, dy, *params),
        (cos_all, sin_all, coeffs, miller, *more),
        outs,
        scratch,
        early=ewald_early,
        in_specs=(FAR, FAR) + (WHOLE,) * (2 + len(more)),
        flops=8 * points * atoms * channels,
    )


def coefficients(totals, filt_rows, norm_atoms, norm_k):
    channels = filt_rows.shape[1]
    cos_struct = totals[:, 0:channels] * norm_atoms
    cos_back = totals[:, channels : 2 * channels] * norm_k
    sin_struct = totals[:, 2 * channels : 3 * channels] * norm_atoms
    sin_back = totals[:, 3 * channels : 4 * channels] * norm_k
    coeffs = jnp.concatenate(
        [
            norm_atoms * filt_rows * cos_back,
            norm_k * filt_rows * cos_struct,
            norm_atoms * filt_rows * sin_back,
            norm_k * filt_rows * sin_struct,
        ],
        axis=1,
    )
    return (coeffs, cos_struct * cos_back + sin_struct * sin_back)


def small_call(kernel, args, outs):
    return pl.pallas_call(
        kernel,
        out_shape=outs,
        in_specs=[WHOLE] * len(args),
        out_specs=(WHOLE,) * len(outs),
        compiler_params=LIMIT,
    )(*args)


def partial_kernel(pieces_ref, sums_ref, out_ref):
    f32, bf16 = jnp.float32, jnp.bfloat16
    total = jnp.sum(pieces_ref[...].astype(f32), axis=0)
    extra = out_ref.shape[1] - total.shape[0]
    sums = sums_ref[...]
    wide = jnp.concatenate([sums[0:extra], sums[extra : 2 * extra]], axis=1)
    whole = jnp.concatenate([total, wide], axis=0).astype(bf16)
    out_ref[...] = jnp.broadcast_to(whole[None], out_ref.shape)


def partial_sums(pieces, sums, tower):
    shape = (tower, pieces.shape[1] + 24, pieces.shape[2])
    outs = (jax.ShapeDtypeStruct(shape, jnp.bfloat16),)
    return small_call(partial_kernel, (pieces, sums), outs)[0]


def coefficient_kernel(
    norm_atoms, norm_k, pieces_ref, filter_in, out_ref, filter_ref, tile, turned, all_filter, sem
):
    f32, bf16 = jnp.float32, jnp.bfloat16
    share, _ = filter_ref.shape
    tower = pieces_ref.shape[0]
    rows = tower * share
    span = tile.shape[1]
    lane = pl.multiple_of(lax.axis_index("gx") * span, span)
    copy = pltpu.make_async_copy(filter_in.at[:, pl.ds(lane, span)], tile, sem)
    copy.start()
    both = jnp.sum(pieces_ref[...].astype(f32), axis=0)
    copy.wait()
    turned[...] = jnp.transpose(tile[...])
    inner, least = [lax.axis_size(axis) for axis in ("gy_1", "gz_0")]
    filters = []
    for w in range(tower):
        group = (w // least * inner + lax.axis_index("gy_1")) * least + w % least
        at = pl.multiple_of((group * 2 + lax.axis_index(PAIR)) * share, share)
        filters.append(turned[pl.ds(at, share), :])
    filt = jnp.concatenate(filters, axis=0)
    coeffs, all_filter[...] = coefficients(both[0:rows], filt, norm_atoms, norm_k)
    mine = lax.axis_index(TOWER)
    filter_ref[...] = all_filter[pl.ds(pl.multiple_of(mine * share, share), share), :]
    tall = jnp.concatenate([both[rows:, 0:128], both[rows:, 128:256]], axis=0)
    hi, lo = split_two(tall[0 : out_ref.shape[1] - rows])
    strip = jnp.concatenate(
        [coeffs, jnp.concatenate([hi.astype(f32), lo.astype(f32)], axis=1)], axis=0
    ).astype(bf16)
    out_ref[...] = jnp.broadcast_to(strip[None], out_ref.shape)


def make_strip(pieces, filter_columns, sheet, cut, norm_atoms, norm_k):
    tower = pieces.shape[0]
    channels, points = filter_columns.shape
    share = points // (2 * tower * sheet)
    span = points // lax.axis_size("gx")
    return pl.pallas_call(
        functools.partial(coefficient_kernel, norm_atoms, norm_k),
        out_shape=(
            jax.ShapeDtypeStruct((sheet, tower * share + cut, pieces.shape[2]), jnp.bfloat16),
            jax.ShapeDtypeStruct((share, channels), jnp.float32),
        ),
        in_specs=[WHOLE, FAR],
        out_specs=(WHOLE, WHOLE),
        scratch_shapes=[
            pltpu.VMEM((channels, span), jnp.float32),
            pltpu.VMEM((span, channels), jnp.float32),
            pltpu.VMEM((tower * share, channels), jnp.float32),
            pltpu.SemaphoreType.DMA,
        ],
        compiler_params=LIMIT,
        name="coefficients",
    )(pieces, filter_columns)


def fold_x_kernel(mid_ref, upper_ref, lower_ref, first_ref, last_ref, rest_ref):
    f32, bf16 = jnp.float32, jnp.bfloat16
    for n in range(3):
        plane = mid_ref[n]
        if n == 0:
            plane = plane + lower_ref[0].astype(f32)
        if n == 2:
            plane = plane + upper_ref[0].astype(f32)
        first_ref[n] = plane[0:1].astype(bf16)
        last_ref[n] = plane[4:5].astype(bf16)
        rest_ref[n] = plane[1:4]


def fold_x(mid, upper, lower):
    side = jax.ShapeDtypeStruct((3, 1, 5, 16, 128), jnp.bfloat16)
    rest = jax.ShapeDtypeStruct((3, 3, 5, 16, 128), jnp.float32)
    return small_call(fold_x_kernel, (mid, upper, lower), (side, side, rest))


def fold_y_kernel(rest_ref, upper_ref, lower_ref, first_ref, last_ref, inner_ref):
    f32, bf16 = jnp.float32, jnp.bfloat16
    for n in range(3):
        plane = rest_ref[:, n]
        if n == 0:
            plane = plane + lower_ref[:, 0].astype(f32)
        if n == 2:
            plane = plane + upper_ref[:, 0].astype(f32)
        first_ref[:, n] = plane[:, 0:1].astype(bf16)
        last_ref[:, n] = plane[:, 4:5].astype(bf16)
        inner_ref[:, n] = plane[:, 1:4]


def fold_y(rest, upper, lower):
    side = jax.ShapeDtypeStruct((3, 3, 1, 16, 128), jnp.bfloat16)
    inner = jax.ShapeDtypeStruct((3, 3, 3, 16, 128), jnp.float32)
    return small_call(fold_y_kernel, (rest, upper, lower), (side, side, inner))


def sent_out(x, axis, dim):
    length = x.shape[dim]
    before = from_behind(lax.slice_in_dim(x, length - 1, length, axis=dim), axis, 1)
    after = from_behind(lax.slice_in_dim(x, 0, 1, axis=dim), axis, -1)
    return before, after


def whole(
    atom_embedding,
    output_adjoint,
    fractional_coords,
    element_labels,
    adjacent_ghost_entries,
    miller_triples,
    reciprocal_kernel,
    channel_mixing_matrix,
    element_channel_factor,
    distance_kernel,
):
    h = atom_embedding[0, 0, 0]
    dy = output_adjoint[0, 0, 0]
    pos = fractional_coords[0, 0, 0][:, None, :]
    kinds = element_labels[0, 0]
    channels, atoms = h.shape
    points = miller_triples.shape[1]
    devices = lax.axis_size(GX_GY_GZ)
    norm_atoms = (atoms * devices) ** (-0.5)
    norm_k = points ** (-0.5)
    half = points // 2

    cells, core, first, last, miller_mine, miller_next = pack(h, kinds, pos, miller_triples)
    cells = cells.reshape(3, 3, 3, 16, 128)
    below, above = from_behind(last, GZ, 1), from_behind(first, GZ, -1)
    cos_next, sin_next, part_next = phase_sums(pos, miller_next, h, dy)
    received = from_behind(part_next, PAIR, 1)
    cells = jnp.concatenate([below, cells, above], axis=2)
    below, above = sent_out(cells, GY, 1)
    cos_mine, sin_mine, part_mine = phase_sums(pos, miller_mine, h, dy)
    cells = jnp.concatenate([below, cells, above], axis=1)
    below, above = sent_out(cells, "gx", 0)
    sheet, tower = lax.axis_size(SHEET), lax.axis_size(TOWER)
    width = 4 * channels
    paired = (part_mine + received).astype(jnp.bfloat16)
    pieces = lax.all_to_all(paired.reshape(sheet, half // sheet, width), SHEET, 0, 0)

    low, mid, high, core_grad, own_grad, sums = short_range(
        (below.reshape(400, 128), cells.reshape(1200, 128), above.reshape(400, 128), core),
        adjacent_ghost_entries[0, 0, 0],
        pos,
        dy,
        distance_kernel,
        channel_mixing_matrix,
        element_channel_factor,
    )
    parts = partial_sums(pieces, sums, tower)
    pieces = lax.all_to_all(parts, TOWER, 0, 0)

    upper = from_behind(low.reshape(1, 5, 5, 16, 128), "gx", -1)
    lower = from_behind(high.reshape(1, 5, 5, 16, 128), "gx", 1)
    first, last, rest = fold_x(mid.reshape(3, 5, 5, 16, 128), upper, lower)
    upper, lower = from_behind(first, GY, -1), from_behind(last, GY, 1)
    cut = (channels + distance_kernel.shape[0]) // 2
    strip, filter_share = make_strip(
        pieces, reciprocal_kernel.T, sheet, cut, norm_atoms, norm_k
    )
    got = lax.all_to_all(strip, SHEET, 0, 0)
    first, last, inner = fold_y(rest, upper, lower)
    upper, lower = from_behind(first, GZ, -1), from_behind(last, GZ, 1)
    got_next = from_behind(got, PAIR, 1)
    early_sums = ewald(got, cos_mine, sin_mine, miller_mine, h, dy)
    atom_grad, position_grad, weight_grad, radial_grad = ewald(
        got_next,
        cos_next,
        sin_next,
        miller_next,
        h,
        dy,
        (*early_sums, inner, upper, lower, core_grad, own_grad, got),
        (kinds, element_channel_factor, channel_mixing_matrix),
        distance_kernel.shape[0],
    )
    position_grad = position_grad[:, 0, :]
    return (
        atom_grad[None, None, None],
        position_grad[None, None, None],
        weight_grad,
        radial_grad,
        filter_share,
    )


def solution(mesh):
    finer = Mesh(
        mesh.devices.reshape(mesh.shape["gx"], 4, 4, 2, 2), ("gx", "gy_0", "gy_1", "gz_0", "gz_1")
    )
    in_specs = (
        P("gx", GY, GZ, None, None),
        P("gx", GY, GZ, None, None),
        P("gx", GY, GZ, None, None),
        P("gx", GY, GZ, None),
        P("gx", GY, GZ, None, None),
        P(),
        P(),
        P(),
        P(),
        P(),
    )
    out_specs = (
        P("gx", GY, GZ, None, None),
        P("gx", GY, GZ, None, None),
        P(),
        P(),
        P(GX_GY_GZ, None),
    )
    return jax.shard_map(whole, mesh=finer, in_specs=in_specs, out_specs=out_specs, check_vma=False)
```

```python
import functools
import math

import jax
import jax.numpy as jnp
from jax import lax
from jax.experimental import pallas as pl
from jax.experimental.pallas import tpu as pltpu
from jax.sharding import Mesh
from jax.sharding import PartitionSpec as P


GY = ("gy_0", "gy_1")
GZ = ("gz_0", "gz_1")

SHEET = ("gx", "gy_1")
TOWER = ("gy_0", "gz_0")
PAIR = "gz_1"
GX_GY_GZ = ("gx", "gy_0", "gy_1", "gz_0", "gz_1")

circle_angle = 2.0 * math.pi
CHUNK = 256
SHARE = 8
SIN_TERMS = (6.28316404, -41.33714227, 81.34076528, -70.99339569)
COS_TERMS = (0.99999995, -19.73917143, 64.93459054, -85.24032775, 56.2423573)
WHOLE = pl.BlockSpec(memory_space=pltpu.VMEM)
FAR = pl.BlockSpec(memory_space=pltpu.HBM)
LIMIT = pltpu.CompilerParams(vmem_limit_bytes=20 * 1024 * 1024)

reach_sq = 0.75
GROUPS = 9
ROWS = 72
BLOCKS = 135
HIGH = BLOCKS // GROUPS * 16


def split_two(x):
    high = x.astype(jnp.bfloat16)
    return high, (x - high.astype(jnp.float32)).astype(jnp.bfloat16)


def row_pick(first, second, third, shape):
    row = lax.broadcasted_iota(jnp.int32, shape, 0) % 4
    spread = lambda v: jnp.broadcast_to(v, shape)
    return jnp.where(
        row == 0,
        spread(first),
        jnp.where(row == 1, spread(second), jnp.where(row == 2, spread(third), 0.0)),
    )


def gains_of(gain_rows, labels, shape):
    columns = jnp.transpose(gain_rows)
    gains = jnp.zeros(shape, jnp.float32)
    for kind in range(gain_rows.shape[0]):
        gains = jnp.where(labels == kind, columns[:, kind : kind + 1], gains)
    return gains


def filter_copy(filter_in, tile, sem):
    span = tile.shape[1]
    lane = pl.multiple_of(lax.axis_index("gx") * span, span)
    return pltpu.make_async_copy(filter_in.at[:, pl.ds(lane, span)], tile, sem)


def take_filter(tile, filter_ref, turned):
    inner, least = [lax.axis_size(axis) for axis in ("gy_1", "gz_0")]
    tower = lax.axis_size(TOWER)
    share = filter_ref.shape[0] // tower
    turned[...] = jnp.transpose(tile[...])
    for w in range(tower):
        group = (w // least * inner + lax.axis_index("gy_1")) * least + w % least
        at = pl.multiple_of((group * 2 + lax.axis_index(PAIR)) * share, share)
        filter_ref[w * share : (w + 1) * share, :] = turned[pl.ds(at, share), :]


def short_early(filter_in, *rest):
    filter_copy(filter_in, *rest[-2:]).start()


def short_kernel(
    ids_ref,
    pos_ref,
    dy_ref,
    radial_ref,
    mix_ref,
    gain_ref,
    filter_in,
    below_ref,
    cells_ref,
    above_ref,
    core_ref,
    low_out,
    mid_out,
    high_out,
    core_out,
    own_ref,
    sums_ref,
    filter_ref,
    lhs_ref,
    feat_ref,
    gains_ref,
    high_ref,
    low_ref,
    near_ref,
    rel_ref,
    basis_ref,
    filt_ref,
    acc_ref,
    table_ref,
    zgrad_ref,
    turned_ref,
    tile_ref,
    tile_sem,
):
    channels, atoms = dy_ref.shape
    filter_copy(filter_in, tile_ref, tile_sem).wait()
    take_filter(tile_ref, filter_ref, turned_ref)
    side, inner, rest = below_ref.shape[0], cells_ref.shape[0], core_ref.shape[0]
    bounds = (0, side, side + inner, 2 * side + inner, 2 * side + inner + rest)
    for n, ref in enumerate((below_ref, cells_ref, above_ref, core_ref)):
        table_ref[bounds[n] : bounds[n + 1], :] = ref[...]
    table_ref[bounds[4] :, :] = jnp.zeros((GROUPS * HIGH - bounds[4], 128), jnp.bfloat16)
    listed = ids_ref.shape[0]
    count = radial_ref.shape[0]
    f32, bf16 = jnp.float32, jnp.bfloat16
    spacing = reach_sq / (count - 1)
    width = 2.0 * spacing
    share = listed ** (-0.5)
    for g in range(GROUPS):
        part = jnp.transpose(table_ref[g * HIGH : (g + 1) * HIGH, :].astype(f32))
        feat = part[0:channels].astype(bf16)
        gains = gains_of(gain_ref[...], part[ROWS : ROWS + 1], (channels, HIGH))
        feat_ref[g] = feat
        gains_ref[g] = gains
        z = lax.dot_general(
            mix_ref[...], feat, (((0,), (0,)), ((), ())), preferred_element_type=f32
        )
        lhs_ref[g * ROWS : (g + 1) * ROWS, :] = jnp.concatenate(
            [z * gains, part[channels:ROWS]], axis=0
        ).astype(bf16)
    ids = ids_ref[...]
    slot = lax.shift_right_logical(ids, 9)
    atom = jnp.bitwise_and(ids, 511)
    block = lax.shift_right_logical(atom, 4)
    ox = slot // 9
    oy = (slot // 3) % 3
    oz = slot % 3
    qx = block // 9
    qy = (block // 3) % 3
    qz = block % 3
    grid = ((3 * ox + qx - 2) * 5 + 3 * oy + qy - 2) * 5 + 3 * oz + qz - 2
    grid = jnp.where(block >= 27, block + (125 - 27), grid)
    low = grid // (BLOCKS // GROUPS)
    high = (grid - low * (BLOCKS // GROUPS)) * 16 + jnp.bitwise_and(atom, 15)
    high_ref[...] = high
    low_ref[...] = low
    offs = [(o - 1).astype(f32) for o in (ox, oy, oz)]
    own8 = row_pick(pos_ref[0], pos_ref[1], pos_ref[2], (8, atoms))
    w_hi, w_lo = split_two(radial_ref[...])
    w_stack = jnp.concatenate([w_hi, w_hi, w_lo], axis=0)
    centre = lax.broadcasted_iota(jnp.int32, (count, 1), 0).astype(f32) * spacing
    iota = lax.broadcasted_iota(jnp.int32, (HIGH, atoms), 0)

    def hot(j):
        return (high_ref[pl.ds(j, 1), :] == iota).astype(f32).astype(bf16)

    agg = jnp.zeros((channels, atoms), f32)
    for j in range(listed):
        found = jnp.dot(lhs_ref[...], hot(j), preferred_element_type=f32)
        low_j = low_ref[j : j + 1, :]
        near = found[0:ROWS]
        for g in range(1, GROUPS):
            near = jnp.where(low_j == g, found[g * ROWS : (g + 1) * ROWS], near)
        near_z = near[0:channels]
        near_ref[j] = near_z.astype(bf16)
        halves = near[channels : channels + 8]
        off8 = row_pick(offs[0][j : j + 1], offs[1][j : j + 1], offs[2][j : j + 1], (8, atoms))
        rel = halves + pltpu.roll(halves, 4, 0) + off8 - own8
        rel_ref[j] = rel
        dist = 0.5 * jnp.sum(rel * rel, axis=0, keepdims=True)
        scaled = (dist - centre) / width
        basis = jnp.exp(-(scaled * scaled))
        basis_ref[j] = basis
        b_hi, b_lo = split_two(basis)
        filt = lax.dot_general(
            w_stack,
            jnp.concatenate([b_hi, b_lo, b_hi], axis=0),
            (((0,), (0,)), ((), ())),
            preferred_element_type=f32,
        )
        filt_ref[j] = filt
        agg = agg + filt * near_z
    agg = agg * share
    gate = 1.0 / (1.0 + jnp.exp(-agg))
    g_all = dy_ref[...].astype(f32) * (gate * (1.0 + agg * (1.0 - gate))) * share
    acc_ref[...] = jnp.zeros_like(acc_ref)
    own_grad = jnp.zeros((8, atoms), f32)
    radial = jnp.zeros((2 * count, 2 * channels), f32)
    w_wide = jnp.concatenate([w_hi, w_hi, w_lo], axis=1)
    for j in range(listed):
        near_z = near_ref[j].astype(f32)
        dz = filt_ref[j] * g_all
        df = near_z * g_all
        f_hi, f_lo = split_two(df)
        basis = basis_ref[j]
        b_hi, b_lo = split_two(basis)
        radial = radial + lax.dot_general(
            jnp.concatenate([b_hi, b_lo], axis=0),
            jnp.concatenate([f_hi, f_lo], axis=0),
            (((1,), (1,)), ((), ())),
            preferred_element_type=f32,
        )
        dbasis = jnp.dot(
            w_wide, jnp.concatenate([f_hi, f_lo, f_hi], axis=0), preferred_element_type=f32
        )
        rel = rel_ref[j]
        dist = 0.5 * jnp.sum(rel * rel, axis=0, keepdims=True)
        slope = dbasis * basis * (dist - centre)
        ddist = jnp.sum(slope, axis=0, keepdims=True) * (-2.0 / (width * width))
        gpos = rel * (2.0 * ddist)
        own_grad = own_grad - gpos
        p_hi = gpos.astype(bf16).astype(f32)
        row8 = lax.broadcasted_iota(jnp.int32, (8, atoms), 0)
        tail = jnp.where(row8 < 4, p_hi, gpos - p_hi)
        full = jnp.concatenate([dz, tail], axis=0)
        low_j = low_ref[j : j + 1, :]
        spread = jnp.concatenate(
            [jnp.where(low_j == g, full, 0.0) for g in range(GROUPS)], axis=0
        ).astype(bf16)
        acc_ref[...] += lax.dot_general(
            spread, hot(j), (((1,), (1,)), ((), ())), preferred_element_type=f32
        )
    own_ref[...] = own_grad
    sums_ref[...] = jnp.zeros_like(sums_ref)
    radial = (
        radial[0:count, 0:channels]
        + radial[count:, 0:channels]
        + radial[0:count, channels:]
        + radial[count:, channels:]
    )
    weight = jnp.zeros((channels, channels), f32)
    for g in range(GROUPS):
        z_hi, z_lo = split_two(acc_ref[g * ROWS : g * ROWS + channels, :] * gains_ref[g])
        for piece in (z_hi, z_lo):
            weight = weight + lax.dot_general(
                feat_ref[g], piece, (((1,), (1,)), ((), ())), preferred_element_type=f32
            )
        part = jnp.transpose(acc_ref[g * ROWS : (g + 1) * ROWS, :])
        part = jnp.concatenate([part, jnp.zeros((HIGH, 128 - ROWS), f32)], axis=1)
        zgrad_ref[g * HIGH : (g + 1) * HIGH, :] = part
    for n, (ref, kind) in enumerate(
        ((low_out, bf16), (mid_out, f32), (high_out, bf16), (core_out, f32))
    ):
        ref[...] = zgrad_ref[bounds[n] : bounds[n + 1], :].astype(kind)
    tall = jnp.concatenate([weight, radial], axis=0)
    cut = (channels + count) // 2
    sums_ref[0:cut, :] = jnp.concatenate([tall[0:cut], tall[cut:]], axis=1)


def short_range(pieces, ids, pos, dy, radial, mix, gain, filter_columns):
    channels, atoms = dy.shape
    listed = ids.shape[0]
    count = radial.shape[0]
    f32, bf16 = jnp.float32, jnp.bfloat16
    shaped = jax.ShapeDtypeStruct
    points, sheet = filter_columns.shape[1], lax.axis_size(SHEET)
    span = points // lax.axis_size("gx")
    return fetching_call(
        short_kernel,
        (ids, pos, dy, radial, mix, gain),
        (filter_columns, *pieces),
        (
            shaped(pieces[0].shape, bf16),
            shaped(pieces[1].shape, f32),
            shaped(pieces[2].shape, bf16),
            shaped(pieces[3].shape, f32),
            shaped((8, atoms), f32),
            shaped((64, 128), f32),
            shaped((points // (2 * sheet), channels), f32),
        ),
        [
            pltpu.VMEM((GROUPS * ROWS, HIGH), bf16),
            pltpu.VMEM((GROUPS, channels, HIGH), bf16),
            pltpu.VMEM((GROUPS, channels, HIGH), f32),
            pltpu.VMEM((listed, atoms), jnp.int32),
            pltpu.VMEM((listed, atoms), jnp.int32),
            pltpu.VMEM((listed, channels, atoms), bf16),
            pltpu.VMEM((listed, 8, atoms), f32),
            pltpu.VMEM((listed, count, atoms), f32),
            pltpu.VMEM((listed, channels, atoms), f32),
            pltpu.VMEM((GROUPS * ROWS, HIGH), f32),
            pltpu.VMEM((GROUPS * HIGH, 128), bf16),
            pltpu.VMEM((GROUPS * HIGH, 128), f32),
            pltpu.VMEM((span, channels), f32),
            pltpu.VMEM((channels, span), f32),
            pltpu.SemaphoreType.DMA,
        ],
        early=short_early,
        in_specs=(FAR,) + (WHOLE,) * len(pieces),
        limit=False,
    )


def fetching_call(
    kernel, fetched, resident, outs, scratch, early=None, in_specs=None, out_specs=None, flops=0,
    limit=20,
):
    n = len(fetched)

    def body(*refs):
        sources, rest = refs[:n], refs[n : -n - 1]
        buffers, sems = refs[-n - 1 : -1], refs[-1]
        copies = [
            pltpu.make_async_copy(sources[i], buffers[i], sems.at[i]) for i in range(n)
        ]
        if early is not None:
            early(*rest)
        for copy in copies:
            copy.start()
        for copy in copies:
            copy.wait()
        kernel(*buffers, *rest)

    cost = None
    if flops:
        cost = pl.CostEstimate(flops=flops, transcendentals=0, bytes_accessed=flops // 128)
    return pl.pallas_call(
        body,
        out_shape=outs,
        in_specs=[FAR] * n + list(in_specs or [WHOLE] * len(resident)),
        out_specs=tuple(out_specs or [WHOLE] * len(outs)),
        scratch_shapes=[
            *scratch,
            *[pltpu.VMEM(x.shape, x.dtype) for x in fetched],
            pltpu.SemaphoreType.DMA((n,)),
        ],
        compiler_params=(
            pltpu.CompilerParams(vmem_limit_bytes=limit * 1024 * 1024) if limit else None
        ),
        cost_estimate=cost,
    )(*fetched, *resident)


def from_behind(x, axis, by):
    devices = lax.axis_size(axis)
    return lax.ppermute(x, axis, [(i, (i + by) % devices) for i in range(devices)])


def chosen(parity):
    column = lax.broadcasted_iota(jnp.int32, (2 * CHUNK, CHUNK), 1)
    row = lax.broadcasted_iota(jnp.int32, (2 * CHUNK, CHUNK), 0)
    n = column // SHARE
    outer, inner, least = [lax.axis_size(axis) for axis in ("gy_0", "gy_1", "gz_0")]
    group = ((n // least) % outer * inner + n // (least * outer)) * least + n % least
    picked = group * (2 * SHARE) + column % SHARE + parity * SHARE
    return (row == picked).astype(jnp.float32).astype(jnp.bfloat16)


def pack_kernel(
    h_ref,
    kind_ref,
    pos_ref,
    miller_ref,
    cells_ref,
    core_ref,
    first_ref,
    last_ref,
    mine_ref,
    next_ref,
):
    f32, bf16 = jnp.float32, jnp.bfloat16
    _, atoms = h_ref.shape
    none = jnp.zeros((1, atoms), f32)
    halves = [split_two(pos_ref[d]) for d in range(3)]
    rows = jnp.concatenate(
        [h_ref[...].astype(f32)]
        + [half[0].astype(f32) for half in halves]
        + [none]
        + [half[1].astype(f32) for half in halves]
        + [none, kind_ref[...].astype(f32), jnp.zeros((127 - ROWS, atoms), f32)],
        axis=0,
    )
    flat = jnp.transpose(rows).astype(bf16)
    cells_ref[...] = flat[0 : cells_ref.shape[0]]
    core_ref[...] = flat[cells_ref.shape[0] :]
    for n in range(9):
        first_ref[n // 3, n % 3, 0] = flat[48 * n : 48 * n + 16]
        last_ref[n // 3, n % 3, 0] = flat[48 * n + 32 : 48 * n + 48]
    m = miller_ref[...].astype(f32)
    tall = jnp.concatenate([m, m, m, jnp.zeros((7, m.shape[1]), f32)], axis=0).astype(bf16)
    runs = m.shape[1] // (2 * CHUNK)
    stack = jnp.concatenate(
        [tall[:, j * 2 * CHUNK : (j + 1) * 2 * CHUNK] for j in range(runs)], axis=0
    )
    core = lax.axis_index(PAIR)
    for parity, out_ref in ((core, mine_ref), (1 - core, next_ref)):
        got = jnp.dot(stack, chosen(parity), preferred_element_type=f32).astype(bf16)
        for j in range(runs):
            out_ref[:, j * CHUNK : (j + 1) * CHUNK] = got[j * 16 : (j + 1) * 16]


def pack(h, kinds, pos, miller):
    half = jax.ShapeDtypeStruct((16, miller.shape[1] // 2), jnp.bfloat16)
    side = jax.ShapeDtypeStruct((3, 3, 1, 16, 128), jnp.bfloat16)
    return fetching_call(
        pack_kernel,
        (h, kinds, pos, miller),
        (),
        (
            jax.ShapeDtypeStruct((432, 128), jnp.bfloat16),
            jax.ShapeDtypeStruct((h.shape[1] - 432, 128), jnp.bfloat16),
            side,
            side,
            half,
            half,
        ),
        [],
        limit=False,
    )


def phase_kernel(
    pos_ref,
    h_ref,
    dy_ref,
    miller_ref,
    cos_out,
    sin_out,
    part_ref,
    cos_ref,
    sin_ref,
    flip_ref,
    rhs_ref,
    t_ref,
    sems,
):
    f32, bf16 = jnp.float32, jnp.bfloat16
    width = 2 * h_ref.shape[0]
    flip_ref[...] = jnp.transpose(jnp.concatenate([h_ref[...], dy_ref[...]], axis=0))
    axes = ("gx", GY, GZ)
    turns = jnp.concatenate(
        [
            (pos_ref[d] + lax.axis_index(axes[d]).astype(f32)) / float(lax.axis_size(axes[d]))
            for d in range(3)
        ],
        axis=0,
    )
    t_hi = turns.astype(bf16)
    t_mid, t_lo = split_two(turns - t_hi.astype(f32))
    rhs_ref[...] = jnp.concatenate(
        [t_hi, t_mid, t_lo, jnp.zeros((7, turns.shape[1]), bf16)], axis=0
    )
    steps = miller_ref.shape[1] // CHUNK
    rows, lanes = 16, 256

    def copies(i):
        at = pl.ds(pl.multiple_of(i * CHUNK, CHUNK), CHUNK)
        return [
            pltpu.make_async_copy(src.at[at], dst.at[at], sems.at[n, i])
            for n, (src, dst) in enumerate(
                ((cos_ref, cos_out), (sin_ref, sin_out))
            )
        ]

    def one(i, carry):
        base = pl.multiple_of(i * CHUNK, CHUNK)
        t_ref[...] = lax.dot_general(
            miller_ref[:, pl.ds(base, CHUNK)],
            rhs_ref[...],
            (((0,), (0,)), ((), ())),
            preferred_element_type=f32,
        )
        for top in range(0, CHUNK, rows):
            for left in range(0, t_ref.shape[1], lanes):
                t = t_ref[top : top + rows, left : left + lanes]
                r = t - jnp.round(t)
                u = jnp.abs(r) - 0.25
                q = u * u
                s = SIN_TERMS[3]
                for term in SIN_TERMS[2::-1]:
                    s = s * q + term
                c = COS_TERMS[4]
                for term in COS_TERMS[3::-1]:
                    c = c * q + term
                at = (pl.ds(base + top, rows), pl.ds(left, lanes))
                cos_ref[at] = -(s * u).astype(bf16)
                sin_ref[at] = jnp.where(r < 0.0, -c, c).astype(bf16)
        here = pl.ds(base, CHUNK)
        part_ref[here, 0:width] = jnp.dot(
            cos_ref[here, :], flip_ref[...], preferred_element_type=f32
        )
        part_ref[here, width:] = jnp.dot(
            sin_ref[here, :], flip_ref[...], preferred_element_type=f32
        )
        for copy in copies(i):
            copy.start()
        return carry

    lax.fori_loop(0, steps, one, 0)
    for i in range(steps):
        for copy in copies(i):
            copy.wait()


def phase_sums(pos, miller, h, dy):
    points = miller.shape[1]
    channels, atoms = h.shape
    width = 2 * channels
    wave = jax.ShapeDtypeStruct((points, atoms), jnp.bfloat16)
    sums = jax.ShapeDtypeStruct((points, 2 * width), jnp.float32)
    return fetching_call(
        phase_kernel,
        (pos, h, dy),
        (miller,),
        (wave, wave, sums),
        [
            pltpu.VMEM(wave.shape, wave.dtype),
            pltpu.VMEM(wave.shape, wave.dtype),
            pltpu.VMEM((atoms, width), jnp.bfloat16),
            pltpu.VMEM((16, atoms), jnp.bfloat16),
            pltpu.VMEM((CHUNK, atoms), jnp.float32),
            pltpu.SemaphoreType.DMA((2, points // CHUNK)),
        ],
        out_specs=(FAR, FAR, WHOLE),
        flops=6 * points * atoms * width,
    )


def wave_copies(cos_in, sin_in, cos_ref, sin_ref, sems, i):
    at = pl.ds(pl.multiple_of(i * CHUNK, CHUNK), CHUNK)
    return [
        pltpu.make_async_copy(cos_in.at[at], cos_ref.at[at], sems.at[0, i]),
        pltpu.make_async_copy(sin_in.at[at], sin_ref.at[at], sems.at[1, i]),
    ]


def ewald_early(cos_in, sin_in, *rest):
    for i in range(cos_in.shape[0] // CHUNK):
        for copy in wave_copies(cos_in, sin_in, *rest[-3:], i):
            copy.start()


def ewald_sums(coeff_ref, miller_ref, both, waves, sums_ref, turn_ref):
    f32 = jnp.float32
    width = both.shape[0]
    channels = width // 2
    run = CHUNK // (miller_ref.shape[1] // coeff_ref.shape[0])
    over_rows = (((0,), (0,)), ((), ()))

    def one(i, carry):
        for copy in wave_copies(*waves, i):
            copy.wait()
        at = pl.ds(pl.multiple_of(i * CHUNK, CHUNK), CHUNK)
        coeffs = coeff_ref[pl.ds(i * run, run), 0 : CHUNK // run].reshape(CHUNK, 2 * width)
        cos_part, sin_part = waves[2][at, :], waves[3][at, :]
        sums_ref[...] += lax.dot_general(
            coeffs[:, 0:channels], cos_part, over_rows, preferred_element_type=f32
        ) + lax.dot_general(
            coeffs[:, width : width + channels], sin_part, over_rows, preferred_element_type=f32
        )
        along_u = jnp.dot(coeffs[:, 0:width], both, preferred_element_type=f32)
        along_v = jnp.dot(coeffs[:, width:], both, preferred_element_type=f32)
        angle = along_v * cos_part.astype(f32) - along_u * sin_part.astype(f32)
        a_hi, a_lo = split_two(angle)
        m = miller_ref[:, at]
        turn_ref[...] += jnp.dot(m, a_hi, preferred_element_type=f32) + jnp.dot(
            m, a_lo, preferred_element_type=f32
        )
        return carry

    lax.fori_loop(0, miller_ref.shape[1] // CHUNK, one, 0)


def ewald_first(
    h_ref, dy_ref, cos_in, sin_in, coeff_ref, miller_ref, sums_ref, turn_ref, cos_ref, sin_ref, sems
):
    sums_ref[...] = jnp.zeros_like(sums_ref)
    turn_ref[...] = jnp.zeros_like(turn_ref)
    both = jnp.concatenate([h_ref[...], dy_ref[...]], axis=0)
    waves = (cos_in, sin_in, cos_ref, sin_ref, sems)
    ewald_sums(coeff_ref, miller_ref, both, waves, sums_ref, turn_ref)


def ewald_second(
    h_ref,
    dy_ref,
    kind_ref,
    gain_ref,
    mix_ref,
    cos_in,
    sin_in,
    coeff_ref,
    miller_ref,
    first_ref,
    angle_ref,
    inner_ref,
    upper_ref,
    lower_ref,
    core_ref,
    own_ref,
    mine_ref,
    atom_ref,
    pos_ref,
    weight_ref,
    radial_ref,
    sums_ref,
    turn_ref,
    cos_ref,
    sin_ref,
    sems,
):
    f32, bf16 = jnp.float32, jnp.bfloat16
    channels = h_ref.shape[0]
    cells = jnp.stack(
        [
            inner_ref[:, :, 0] + lower_ref[:, :, 0].astype(f32),
            inner_ref[:, :, 1],
            inner_ref[:, :, 2] + upper_ref[:, :, 0].astype(f32),
        ],
        axis=2,
    ).reshape(432, 128)
    flat = jnp.transpose(jnp.concatenate([cells, core_ref[...]], axis=0))
    gains = gains_of(gain_ref[...], kind_ref[...], (channels, flat.shape[1]))
    zscaled = (flat[0:channels] * gains).astype(bf16)
    halves = flat[channels : channels + 8]
    near = halves + pltpu.roll(halves, 4, 0) + own_ref[...]
    sums_ref[...] = first_ref[...] + jnp.dot(mix_ref[...], zscaled, preferred_element_type=f32)
    turn_ref[...] = angle_ref[...]
    both = jnp.concatenate([h_ref[...], dy_ref[...]], axis=0)
    waves = (cos_in, sin_in, cos_ref, sin_ref, sems)
    ewald_sums(coeff_ref, miller_ref, both, waves, sums_ref, turn_ref)
    atom_ref[...] = (dy_ref[...].astype(f32) + sums_ref[...]).astype(bf16)
    axes = ("gx", GY, GZ)
    for d in range(3):
        pos_ref[d] = (
            turn_ref[d : d + 1, :] * (circle_angle / lax.axis_size(axes[d])) + near[d : d + 1, :]
        )
    cut = (channels + radial_ref.shape[0]) // 2
    run = miller_ref.shape[1] // coeff_ref.shape[0]
    sides = []
    for ref in (mine_ref, coeff_ref):
        total = jnp.sum(ref[:, run:].astype(f32), axis=0)
        sides.append(jnp.concatenate([total[:, 0:128], total[:, 128:256]], axis=0))
    full = (sides[0] + sides[1])[0:cut]
    tall = jnp.concatenate([full[:, 0:channels], full[:, channels:]], axis=0)
    weight_ref[...] = tall[0:channels]
    radial_ref[...] = tall[channels:]


def ewald(coeffs, cos_all, sin_all, miller, h, dy, more=(), params=(), basis=0):
    points, atoms = cos_all.shape
    channels = h.shape[0]
    last = len(more) > 0
    shaped = jax.ShapeDtypeStruct
    sums = shaped((channels, atoms), jnp.float32)
    turn = shaped((16, atoms), jnp.float32)
    scratch = [
        pltpu.VMEM(cos_all.shape, jnp.bfloat16),
        pltpu.VMEM(cos_all.shape, jnp.bfloat16),
        pltpu.SemaphoreType.DMA((2, points // CHUNK)),
    ]
    outs = (sums, turn)
    if last:
        scratch = [pltpu.VMEM(sums.shape, sums.dtype), pltpu.VMEM(turn.shape, turn.dtype)] + scratch
        outs = (
            shaped(sums.shape, jnp.bfloat16),
            shaped((3, 1, atoms), jnp.float32),
            shaped((channels, channels), jnp.float32),
            shaped((basis, channels), jnp.float32),
        )
    return fetching_call(
        ewald_second if last else ewald_first,
        (h, dy, *params),
        (cos_all, sin_all, coeffs, miller, *more),
        outs,
        scratch,
        early=ewald_early,
        in_specs=(FAR, FAR) + (WHOLE,) * (2 + len(more)),
        flops=8 * points * atoms * channels,
        limit=20 if last else 52,
    )


def coefficients(totals, filt_rows, norm_atoms, norm_k):
    channels = filt_rows.shape[1]
    cos_struct = totals[:, 0:channels] * norm_atoms
    cos_back = totals[:, channels : 2 * channels] * norm_k
    sin_struct = totals[:, 2 * channels : 3 * channels] * norm_atoms
    sin_back = totals[:, 3 * channels : 4 * channels] * norm_k
    coeffs = jnp.concatenate(
        [
            norm_atoms * filt_rows * cos_back,
            norm_k * filt_rows * cos_struct,
            norm_atoms * filt_rows * sin_back,
            norm_k * filt_rows * sin_struct,
        ],
        axis=1,
    )
    return (coeffs, cos_struct * cos_back + sin_struct * sin_back)


def small_call(kernel, args, outs):
    return pl.pallas_call(
        kernel,
        out_shape=outs,
        in_specs=[WHOLE] * len(args),
        out_specs=(WHOLE,) * len(outs),
        compiler_params=LIMIT,
    )(*args)


def partial_kernel(pieces_ref, sums_ref, out_ref):
    f32, bf16 = jnp.float32, jnp.bfloat16
    total = jnp.sum(pieces_ref[...].astype(f32), axis=0)
    extra = out_ref.shape[1] - total.shape[0]
    sums = sums_ref[...]
    wide = jnp.concatenate([sums[0:extra], sums[extra : 2 * extra]], axis=1)
    whole = jnp.concatenate([total, wide], axis=0).astype(bf16)
    out_ref[...] = jnp.broadcast_to(whole[None], out_ref.shape)


def partial_sums(pieces, sums, tower):
    shape = (tower, pieces.shape[1] + 24, pieces.shape[2])
    outs = (jax.ShapeDtypeStruct(shape, jnp.bfloat16),)
    return small_call(partial_kernel, (pieces, sums), outs)[0]


def coefficient_kernel(norm_atoms, norm_k, pieces_ref, filt_ref, out_ref, filter_ref, all_filter):
    f32, bf16 = jnp.float32, jnp.bfloat16
    share = filter_ref.shape[0]
    rows = filt_ref.shape[0]
    both = jnp.sum(pieces_ref[...].astype(f32), axis=0)
    coeffs, all_filter[...] = coefficients(both[0:rows], filt_ref[...], norm_atoms, norm_k)
    mine = lax.axis_index(TOWER)
    filter_ref[...] = all_filter[pl.ds(pl.multiple_of(mine * share, share), share), :]
    strip = jnp.concatenate([coeffs, both[rows:]], axis=0).astype(bf16)
    out_ref[...] = jnp.broadcast_to(strip[None], out_ref.shape)


def make_strip(pieces, filt, sheet, norm_atoms, norm_k):
    tower, rows, width = pieces.shape
    share, channels = filt.shape[0] // tower, filt.shape[1]
    return pl.pallas_call(
        functools.partial(coefficient_kernel, norm_atoms, norm_k),
        out_shape=(
            jax.ShapeDtypeStruct((sheet, rows, width), jnp.bfloat16),
            jax.ShapeDtypeStruct((share, channels), jnp.float32),
        ),
        in_specs=[WHOLE, WHOLE],
        out_specs=(WHOLE, WHOLE),
        scratch_shapes=[pltpu.VMEM(filt.shape, jnp.float32)],
        compiler_params=LIMIT,
        name="coefficients",
    )(pieces, filt)


def fold_x_kernel(mid_ref, upper_ref, lower_ref, first_ref, last_ref, rest_ref):
    f32, bf16 = jnp.float32, jnp.bfloat16
    for n in range(3):
        plane = mid_ref[n]
        if n == 0:
            plane = plane + lower_ref[0].astype(f32)
        if n == 2:
            plane = plane + upper_ref[0].astype(f32)
        first_ref[n] = plane[0:1].astype(bf16)
        last_ref[n] = plane[4:5].astype(bf16)
        rest_ref[n] = plane[1:4]


def fold_x(mid, upper, lower):
    side = jax.ShapeDtypeStruct((3, 1, 5, 16, 128), jnp.bfloat16)
    rest = jax.ShapeDtypeStruct((3, 3, 5, 16, 128), jnp.float32)
    return small_call(fold_x_kernel, (mid, upper, lower), (side, side, rest))


def fold_y_kernel(rest_ref, upper_ref, lower_ref, first_ref, last_ref, inner_ref):
    f32, bf16 = jnp.float32, jnp.bfloat16
    for n in range(3):
        plane = rest_ref[:, n]
        if n == 0:
            plane = plane + lower_ref[:, 0].astype(f32)
        if n == 2:
            plane = plane + upper_ref[:, 0].astype(f32)
        first_ref[:, n] = plane[:, 0:1].astype(bf16)
        last_ref[:, n] = plane[:, 4:5].astype(bf16)
        inner_ref[:, n] = plane[:, 1:4]


def fold_y(rest, upper, lower):
    side = jax.ShapeDtypeStruct((3, 3, 1, 16, 128), jnp.bfloat16)
    inner = jax.ShapeDtypeStruct((3, 3, 3, 16, 128), jnp.float32)
    return small_call(fold_y_kernel, (rest, upper, lower), (side, side, inner))


def sent_out(x, axis, dim):
    length = x.shape[dim]
    before = from_behind(lax.slice_in_dim(x, length - 1, length, axis=dim), axis, 1)
    after = from_behind(lax.slice_in_dim(x, 0, 1, axis=dim), axis, -1)
    return before, after


def whole(
    atom_embedding,
    output_adjoint,
    fractional_coords,
    element_labels,
    adjacent_ghost_entries,
    miller_triples,
    reciprocal_kernel,
    channel_mixing_matrix,
    element_channel_factor,
    distance_kernel,
):
    h = atom_embedding[0, 0, 0]
    dy = output_adjoint[0, 0, 0]
    pos = fractional_coords[0, 0, 0][:, None, :]
    kinds = element_labels[0, 0]
    channels, atoms = h.shape
    points = miller_triples.shape[1]
    devices = lax.axis_size(GX_GY_GZ)
    norm_atoms = (atoms * devices) ** (-0.5)
    norm_k = points ** (-0.5)
    half = points // 2

    cells, core, first, last, miller_mine, miller_next = pack(h, kinds, pos, miller_triples)
    cells = cells.reshape(3, 3, 3, 16, 128)
    below, above = from_behind(last, GZ, 1), from_behind(first, GZ, -1)
    cos_next, sin_next, part_next = phase_sums(pos, miller_next, h, dy)
    received = from_behind(part_next, PAIR, 1)
    cells = jnp.concatenate([below, cells, above], axis=2)
    below, above = sent_out(cells, GY, 1)
    cos_mine, sin_mine, part_mine = phase_sums(pos, miller_mine, h, dy)
    cells = jnp.concatenate([below, cells, above], axis=1)
    below, above = sent_out(cells, "gx", 0)
    sheet, tower = lax.axis_size(SHEET), lax.axis_size(TOWER)
    width = 4 * channels
    paired = (part_mine + received).astype(jnp.bfloat16)
    pieces = lax.all_to_all(paired.reshape(sheet, half // sheet, width), SHEET, 0, 0)

    low, mid, high, core_grad, own_grad, sums, filt = short_range(
        (below.reshape(400, 128), cells.reshape(1200, 128), above.reshape(400, 128), core),
        adjacent_ghost_entries[0, 0, 0],
        pos,
        dy,
        distance_kernel,
        channel_mixing_matrix,
        element_channel_factor,
        reciprocal_kernel.T,
    )
    parts = partial_sums(pieces, sums, tower)
    pieces = lax.all_to_all(parts, TOWER, 0, 0)

    upper = from_behind(low.reshape(1, 5, 5, 16, 128), "gx", -1)
    lower = from_behind(high.reshape(1, 5, 5, 16, 128), "gx", 1)
    first, last, rest = fold_x(mid.reshape(3, 5, 5, 16, 128), upper, lower)
    upper, lower = from_behind(first, GY, -1), from_behind(last, GY, 1)
    strip, filter_share = make_strip(pieces, filt, sheet, norm_atoms, norm_k)
    got = lax.all_to_all(strip, SHEET, 0, 0)
    first, last, inner = fold_y(rest, upper, lower)
    upper, lower = from_behind(first, GZ, -1), from_behind(last, GZ, 1)
    got_next = from_behind(got, PAIR, 1)
    early_sums = ewald(got, cos_mine, sin_mine, miller_mine, h, dy)
    atom_grad, position_grad, weight_grad, radial_grad = ewald(
        got_next,
        cos_next,
        sin_next,
        miller_next,
        h,
        dy,
        (*early_sums, inner, upper, lower, core_grad, own_grad, got),
        (kinds, element_channel_factor, channel_mixing_matrix),
        distance_kernel.shape[0],
    )
    position_grad = position_grad[:, 0, :]
    return (
        atom_grad[None, None, None],
        position_grad[None, None, None],
        weight_grad,
        radial_grad,
        filter_share,
    )


def solution(mesh):
    finer = Mesh(
        mesh.devices.reshape(mesh.shape["gx"], 4, 4, 2, 2), ("gx", "gy_0", "gy_1", "gz_0", "gz_1")
    )
    in_specs = (
        P("gx", GY, GZ, None, None),
        P("gx", GY, GZ, None, None),
        P("gx", GY, GZ, None, None),
        P("gx", GY, GZ, None),
        P("gx", GY, GZ, None, None),
        P(),
        P(),
        P(),
        P(),
        P(),
    )
    out_specs = (
        P("gx", GY, GZ, None, None),
        P("gx", GY, GZ, None, None),
        P(),
        P(),
        P(GX_GY_GZ, None),
    )
    return jax.shard_map(whole, mesh=finer, in_specs=in_specs, out_specs=out_specs, check_vma=False)
```

```python
import functools
import math

import jax
import jax.numpy as jnp
from jax import lax
from jax.experimental import pallas as pl
from jax.experimental.pallas import tpu as pltpu
from jax.sharding import Mesh
from jax.sharding import PartitionSpec as P


GY = ("gy_0", "gy_1")
GZ = ("gz_0", "gz_1")

SHEET = ("gx", "gy_1")
TOWER = ("gy_0", "gz_0")
PAIR = "gz_1"
GX_GY_GZ = ("gx", "gy_0", "gy_1", "gz_0", "gz_1")

circle_angle = 2.0 * math.pi
CHUNK = 256
SHARE = 8
SIN_TERMS = (6.28316404, -41.33714227, 81.34076528, -70.99339569)
COS_TERMS = (0.99999995, -19.73917143, 64.93459054, -85.24032775, 56.2423573)
WHOLE = pl.BlockSpec(memory_space=pltpu.VMEM)
FAR = pl.BlockSpec(memory_space=pltpu.HBM)
LIMIT = pltpu.CompilerParams(vmem_limit_bytes=20 * 1024 * 1024)

reach_sq = 0.75
GROUPS = 9
ROWS = 72
BLOCKS = 135
HIGH = BLOCKS // GROUPS * 16


def split_two(x):
    high = x.astype(jnp.bfloat16)
    return high, (x - high.astype(jnp.float32)).astype(jnp.bfloat16)


def row_pick(first, second, third, shape):
    row = lax.broadcasted_iota(jnp.int32, shape, 0) % 4
    spread = lambda v: jnp.broadcast_to(v, shape)
    return jnp.where(
        row == 0,
        spread(first),
        jnp.where(row == 1, spread(second), jnp.where(row == 2, spread(third), 0.0)),
    )


def gains_of(gain_rows, labels, shape):
    columns = jnp.transpose(gain_rows)
    gains = jnp.zeros(shape, jnp.float32)
    for kind in range(gain_rows.shape[0]):
        gains = jnp.where(labels == kind, columns[:, kind : kind + 1], gains)
    return gains


def filter_copy(filter_in, tile, sem):
    span = tile.shape[1]
    lane = pl.multiple_of(lax.axis_index("gx") * span, span)
    return pltpu.make_async_copy(filter_in.at[:, pl.ds(lane, span)], tile, sem)


def take_filter(tile, filter_ref, turned):
    inner, least = [lax.axis_size(axis) for axis in ("gy_1", "gz_0")]
    tower = lax.axis_size(TOWER)
    share = filter_ref.shape[0] // tower
    turned[...] = jnp.transpose(tile[...])
    for w in range(tower):
        group = (w // least * inner + lax.axis_index("gy_1")) * least + w % least
        at = pl.multiple_of((group * 2 + lax.axis_index(PAIR)) * share, share)
        filter_ref[w * share : (w + 1) * share, :] = turned[pl.ds(at, share), :]


def short_early(filter_in, *rest):
    filter_copy(filter_in, *rest[-2:]).start()


def short_kernel(
    ids_ref,
    pos_ref,
    dy_ref,
    radial_ref,
    mix_ref,
    gain_ref,
    filter_in,
    below_ref,
    cells_ref,
    above_ref,
    core_ref,
    low_out,
    mid_out,
    high_out,
    core_out,
    own_ref,
    sums_ref,
    filter_ref,
    lhs_ref,
    feat_ref,
    gains_ref,
    high_ref,
    low_ref,
    near_ref,
    rel_ref,
    basis_ref,
    filt_ref,
    acc_ref,
    table_ref,
    zgrad_ref,
    turned_ref,
    tile_ref,
    tile_sem,
):
    channels, atoms = dy_ref.shape
    filter_copy(filter_in, tile_ref, tile_sem).wait()
    take_filter(tile_ref, filter_ref, turned_ref)
    side, inner, rest = below_ref.shape[0], cells_ref.shape[0], core_ref.shape[0]
    bounds = (0, side, side + inner, 2 * side + inner, 2 * side + inner + rest)
    for n, ref in enumerate((below_ref, cells_ref, above_ref, core_ref)):
        table_ref[bounds[n] : bounds[n + 1], :] = ref[...]
    table_ref[bounds[4] :, :] = jnp.zeros((GROUPS * HIGH - bounds[4], 128), jnp.bfloat16)
    listed = ids_ref.shape[0]
    count = radial_ref.shape[0]
    f32, bf16 = jnp.float32, jnp.bfloat16
    spacing = reach_sq / (count - 1)
    width = 2.0 * spacing
    share = listed ** (-0.5)
    for g in range(GROUPS):
        part = jnp.transpose(table_ref[g * HIGH : (g + 1) * HIGH, :].astype(f32))
        feat = part[0:channels].astype(bf16)
        gains = gains_of(gain_ref[...], part[ROWS : ROWS + 1], (channels, HIGH))
        feat_ref[g] = feat
        gains_ref[g] = gains
        z = lax.dot_general(
            mix_ref[...], feat, (((0,), (0,)), ((), ())), preferred_element_type=f32
        )
        lhs_ref[g * ROWS : (g + 1) * ROWS, :] = jnp.concatenate(
            [z * gains, part[channels:ROWS]], axis=0
        ).astype(bf16)
    ids = ids_ref[...]
    slot = lax.shift_right_logical(ids, 9)
    atom = jnp.bitwise_and(ids, 511)
    block = lax.shift_right_logical(atom, 4)
    ox = slot // 9
    oy = (slot // 3) % 3
    oz = slot % 3
    qx = block // 9
    qy = (block // 3) % 3
    qz = block % 3
    grid = ((3 * ox + qx - 2) * 5 + 3 * oy + qy - 2) * 5 + 3 * oz + qz - 2
    grid = jnp.where(block >= 27, block + (125 - 27), grid)
    low = grid // (BLOCKS // GROUPS)
    high = (grid - low * (BLOCKS // GROUPS)) * 16 + jnp.bitwise_and(atom, 15)
    high_ref[...] = high
    low_ref[...] = low
    offs = [(o - 1).astype(f32) for o in (ox, oy, oz)]
    own8 = row_pick(pos_ref[0], pos_ref[1], pos_ref[2], (8, atoms))
    w_hi, w_lo = split_two(radial_ref[...])
    w_stack = jnp.concatenate([w_hi, w_hi, w_lo], axis=0)
    centre = lax.broadcasted_iota(jnp.int32, (count, 1), 0).astype(f32) * spacing
    iota = lax.broadcasted_iota(jnp.int32, (HIGH, atoms), 0)

    def hot(j):
        return (high_ref[pl.ds(j, 1), :] == iota).astype(f32).astype(bf16)

    agg = jnp.zeros((channels, atoms), f32)
    for j in range(listed):
        found = jnp.dot(lhs_ref[...], hot(j), preferred_element_type=f32)
        low_j = low_ref[j : j + 1, :]
        near = found[0:ROWS]
        for g in range(1, GROUPS):
            near = jnp.where(low_j == g, found[g * ROWS : (g + 1) * ROWS], near)
        near_z = near[0:channels]
        near_ref[j] = near_z.astype(bf16)
        halves = near[channels : channels + 8]
        off8 = row_pick(offs[0][j : j + 1], offs[1][j : j + 1], offs[2][j : j + 1], (8, atoms))
        rel = halves + pltpu.roll(halves, 4, 0) + off8 - own8
        rel_ref[j] = rel
        dist = 0.5 * jnp.sum(rel * rel, axis=0, keepdims=True)
        scaled = (dist - centre) / width
        basis = jnp.exp(-(scaled * scaled))
        basis_ref[j] = basis
        b_hi, b_lo = split_two(basis)
        filt = lax.dot_general(
            w_stack,
            jnp.concatenate([b_hi, b_lo, b_hi], axis=0),
            (((0,), (0,)), ((), ())),
            preferred_element_type=f32,
        )
        filt_ref[j] = filt
        agg = agg + filt * near_z
    agg = agg * share
    gate = 1.0 / (1.0 + jnp.exp(-agg))
    g_all = dy_ref[...].astype(f32) * (gate * (1.0 + agg * (1.0 - gate))) * share
    acc_ref[...] = jnp.zeros_like(acc_ref)
    own_grad = jnp.zeros((8, atoms), f32)
    radial = jnp.zeros((2 * count, 2 * channels), f32)
    w_wide = jnp.concatenate([w_hi, w_hi, w_lo], axis=1)
    for j in range(listed):
        near_z = near_ref[j].astype(f32)
        dz = filt_ref[j] * g_all
        df = near_z * g_all
        f_hi, f_lo = split_two(df)
        basis = basis_ref[j]
        b_hi, b_lo = split_two(basis)
        radial = radial + lax.dot_general(
            jnp.concatenate([b_hi, b_lo], axis=0),
            jnp.concatenate([f_hi, f_lo], axis=0),
            (((1,), (1,)), ((), ())),
            preferred_element_type=f32,
        )
        dbasis = jnp.dot(
            w_wide, jnp.concatenate([f_hi, f_lo, f_hi], axis=0), preferred_element_type=f32
        )
        rel = rel_ref[j]
        dist = 0.5 * jnp.sum(rel * rel, axis=0, keepdims=True)
        slope = dbasis * basis * (dist - centre)
        ddist = jnp.sum(slope, axis=0, keepdims=True) * (-2.0 / (width * width))
        gpos = rel * (2.0 * ddist)
        own_grad = own_grad - gpos
        p_hi = gpos.astype(bf16).astype(f32)
        row8 = lax.broadcasted_iota(jnp.int32, (8, atoms), 0)
        tail = jnp.where(row8 < 4, p_hi, gpos - p_hi)
        full = jnp.concatenate([dz, tail], axis=0)
        low_j = low_ref[j : j + 1, :]
        spread = jnp.concatenate(
            [jnp.where(low_j == g, full, 0.0) for g in range(GROUPS)], axis=0
        ).astype(bf16)
        acc_ref[...] += lax.dot_general(
            spread, hot(j), (((1,), (1,)), ((), ())), preferred_element_type=f32
        )
    own_ref[...] = own_grad
    sums_ref[...] = jnp.zeros_like(sums_ref)
    radial = (
        radial[0:count, 0:channels]
        + radial[count:, 0:channels]
        + radial[0:count, channels:]
        + radial[count:, channels:]
    )
    weight = jnp.zeros((channels, channels), f32)
    for g in range(GROUPS):
        z_hi, z_lo = split_two(acc_ref[g * ROWS : g * ROWS + channels, :] * gains_ref[g])
        for piece in (z_hi, z_lo):
            weight = weight + lax.dot_general(
                feat_ref[g], piece, (((1,), (1,)), ((), ())), preferred_element_type=f32
            )
        part = jnp.transpose(acc_ref[g * ROWS : (g + 1) * ROWS, :])
        part = jnp.concatenate([part, jnp.zeros((HIGH, 128 - ROWS), f32)], axis=1)
        zgrad_ref[g * HIGH : (g + 1) * HIGH, :] = part
    for n, (ref, kind) in enumerate(
        ((low_out, bf16), (mid_out, f32), (high_out, bf16), (core_out, f32))
    ):
        ref[...] = zgrad_ref[bounds[n] : bounds[n + 1], :].astype(kind)
    tall = jnp.concatenate([weight, radial], axis=0)
    cut = (channels + count) // 2
    sums_ref[0:cut, :] = jnp.concatenate([tall[0:cut], tall[cut:]], axis=1)


def short_range(pieces, ids, pos, dy, radial, mix, gain, filter_columns):
    channels, atoms = dy.shape
    listed = ids.shape[0]
    count = radial.shape[0]
    f32, bf16 = jnp.float32, jnp.bfloat16
    shaped = jax.ShapeDtypeStruct
    points, sheet = filter_columns.shape[1], lax.axis_size(SHEET)
    span = points // lax.axis_size("gx")
    return fetching_call(
        short_kernel,
        (ids, pos, dy, radial, mix, gain),
        (filter_columns, *pieces),
        (
            shaped(pieces[0].shape, bf16),
            shaped(pieces[1].shape, f32),
            shaped(pieces[2].shape, bf16),
            shaped(pieces[3].shape, f32),
            shaped((8, atoms), f32),
            shaped((64, 128), f32),
            shaped((points // (2 * sheet), channels), f32),
        ),
        [
            pltpu.VMEM((GROUPS * ROWS, HIGH), bf16),
            pltpu.VMEM((GROUPS, channels, HIGH), bf16),
            pltpu.VMEM((GROUPS, channels, HIGH), f32),
            pltpu.VMEM((listed, atoms), jnp.int32),
            pltpu.VMEM((listed, atoms), jnp.int32),
            pltpu.VMEM((listed, channels, atoms), bf16),
            pltpu.VMEM((listed, 8, atoms), f32),
            pltpu.VMEM((listed, count, atoms), f32),
            pltpu.VMEM((listed, channels, atoms), f32),
            pltpu.VMEM((GROUPS * ROWS, HIGH), f32),
            pltpu.VMEM((GROUPS * HIGH, 128), bf16),
            pltpu.VMEM((GROUPS * HIGH, 128), f32),
            pltpu.VMEM((span, channels), f32),
            pltpu.VMEM((channels, span), f32),
            pltpu.SemaphoreType.DMA,
        ],
        early=short_early,
        in_specs=(FAR,) + (WHOLE,) * len(pieces),
        limit=False,
    )


def fetching_call(
    kernel, fetched, resident, outs, scratch, early=None, in_specs=None, out_specs=None, flops=0,
    limit=20,
):
    n = len(fetched)

    def body(*refs):
        sources, rest = refs[:n], refs[n : -n - 1]
        buffers, sems = refs[-n - 1 : -1], refs[-1]
        copies = [
            pltpu.make_async_copy(sources[i], buffers[i], sems.at[i]) for i in range(n)
        ]
        if early is not None:
            early(*rest)
        for copy in copies:
            copy.start()
        for copy in copies:
            copy.wait()
        kernel(*buffers, *rest)

    cost = None
    if flops:
        cost = pl.CostEstimate(flops=flops, transcendentals=0, bytes_accessed=flops // 128)
    return pl.pallas_call(
        body,
        out_shape=outs,
        in_specs=[FAR] * n + list(in_specs or [WHOLE] * len(resident)),
        out_specs=tuple(out_specs or [WHOLE] * len(outs)),
        scratch_shapes=[
            *scratch,
            *[pltpu.VMEM(x.shape, x.dtype) for x in fetched],
            pltpu.SemaphoreType.DMA((n,)),
        ],
        compiler_params=(
            pltpu.CompilerParams(vmem_limit_bytes=limit * 1024 * 1024) if limit else None
        ),
        cost_estimate=cost,
    )(*fetched, *resident)


def from_behind(x, axis, by):
    devices = lax.axis_size(axis)
    return lax.ppermute(x, axis, [(i, (i + by) % devices) for i in range(devices)])


def chosen(parity):
    column = lax.broadcasted_iota(jnp.int32, (2 * CHUNK, CHUNK), 1)
    row = lax.broadcasted_iota(jnp.int32, (2 * CHUNK, CHUNK), 0)
    n = column // SHARE
    outer, inner, least = [lax.axis_size(axis) for axis in ("gy_0", "gy_1", "gz_0")]
    group = ((n // least) % outer * inner + n // (least * outer)) * least + n % least
    picked = group * (2 * SHARE) + column % SHARE + parity * SHARE
    return (row == picked).astype(jnp.float32).astype(jnp.bfloat16)


def pack_kernel(
    h_ref,
    kind_ref,
    pos_ref,
    miller_ref,
    cells_ref,
    core_ref,
    first_ref,
    last_ref,
    mine_ref,
    next_ref,
):
    f32, bf16 = jnp.float32, jnp.bfloat16
    _, atoms = h_ref.shape
    none = jnp.zeros((1, atoms), f32)
    halves = [split_two(pos_ref[d]) for d in range(3)]
    rows = jnp.concatenate(
        [h_ref[...].astype(f32)]
        + [half[0].astype(f32) for half in halves]
        + [none]
        + [half[1].astype(f32) for half in halves]
        + [none, kind_ref[...].astype(f32), jnp.zeros((127 - ROWS, atoms), f32)],
        axis=0,
    )
    flat = jnp.transpose(rows).astype(bf16)
    cells_ref[...] = flat[0 : cells_ref.shape[0]]
    core_ref[...] = flat[cells_ref.shape[0] :]
    for n in range(9):
        first_ref[n // 3, n % 3, 0] = flat[48 * n : 48 * n + 16]
        last_ref[n // 3, n % 3, 0] = flat[48 * n + 32 : 48 * n + 48]
    m = miller_ref[...].astype(f32)
    tall = jnp.concatenate([m, m, m, jnp.zeros((7, m.shape[1]), f32)], axis=0).astype(bf16)
    runs = m.shape[1] // (2 * CHUNK)
    stack = jnp.concatenate(
        [tall[:, j * 2 * CHUNK : (j + 1) * 2 * CHUNK] for j in range(runs)], axis=0
    )
    core = lax.axis_index(PAIR)
    for parity, out_ref in ((core, mine_ref), (1 - core, next_ref)):
        got = jnp.dot(stack, chosen(parity), preferred_element_type=f32).astype(bf16)
        for j in range(runs):
            out_ref[:, j * CHUNK : (j + 1) * CHUNK] = got[j * 16 : (j + 1) * 16]


def pack(h, kinds, pos, miller):
    half = jax.ShapeDtypeStruct((16, miller.shape[1] // 2), jnp.bfloat16)
    side = jax.ShapeDtypeStruct((3, 3, 1, 16, 128), jnp.bfloat16)
    return fetching_call(
        pack_kernel,
        (h, kinds, pos, miller),
        (),
        (
            jax.ShapeDtypeStruct((432, 128), jnp.bfloat16),
            jax.ShapeDtypeStruct((h.shape[1] - 432, 128), jnp.bfloat16),
            side,
            side,
            half,
            half,
        ),
        [],
        limit=False,
    )


def phase_kernel(
    pos_ref,
    h_ref,
    dy_ref,
    miller_ref,
    cos_out,
    sin_out,
    part_ref,
    cos_ref,
    sin_ref,
    flip_ref,
    rhs_ref,
    t_ref,
    sems,
):
    f32, bf16 = jnp.float32, jnp.bfloat16
    width = 2 * h_ref.shape[0]
    flip_ref[...] = jnp.transpose(jnp.concatenate([h_ref[...], dy_ref[...]], axis=0))
    axes = ("gx", GY, GZ)
    turns = jnp.concatenate(
        [
            (pos_ref[d] + lax.axis_index(axes[d]).astype(f32)) / float(lax.axis_size(axes[d]))
            for d in range(3)
        ],
        axis=0,
    )
    t_hi = turns.astype(bf16)
    t_mid, t_lo = split_two(turns - t_hi.astype(f32))
    rhs_ref[...] = jnp.concatenate(
        [t_hi, t_mid, t_lo, jnp.zeros((7, turns.shape[1]), bf16)], axis=0
    )
    steps = miller_ref.shape[1] // CHUNK
    rows, lanes = 16, 256

    def copies(i):
        at = pl.ds(pl.multiple_of(i * CHUNK, CHUNK), CHUNK)
        return [
            pltpu.make_async_copy(src.at[at], dst.at[at], sems.at[n, i])
            for n, (src, dst) in enumerate(
                ((cos_ref, cos_out), (sin_ref, sin_out))
            )
        ]

    def one(i, carry):
        base = pl.multiple_of(i * CHUNK, CHUNK)
        t_ref[...] = lax.dot_general(
            miller_ref[:, pl.ds(base, CHUNK)],
            rhs_ref[...],
            (((0,), (0,)), ((), ())),
            preferred_element_type=f32,
        )
        for top in range(0, CHUNK, rows):
            for left in range(0, t_ref.shape[1], lanes):
                t = t_ref[top : top + rows, left : left + lanes]
                r = t - jnp.round(t)
                u = jnp.abs(r) - 0.25
                q = u * u
                s = SIN_TERMS[3]
                for term in SIN_TERMS[2::-1]:
                    s = s * q + term
                c = COS_TERMS[4]
                for term in COS_TERMS[3::-1]:
                    c = c * q + term
                at = (pl.ds(base + top, rows), pl.ds(left, lanes))
                cos_ref[at] = -(s * u).astype(bf16)
                sin_ref[at] = jnp.where(r < 0.0, -c, c).astype(bf16)
        here = pl.ds(base, CHUNK)
        part_ref[here, 0:width] = jnp.dot(
            cos_ref[here, :], flip_ref[...], preferred_element_type=f32
        )
        part_ref[here, width:] = jnp.dot(
            sin_ref[here, :], flip_ref[...], preferred_element_type=f32
        )
        for copy in copies(i):
            copy.start()
        return carry

    lax.fori_loop(0, steps, one, 0)
    for i in range(steps):
        for copy in copies(i):
            copy.wait()


def phase_sums(pos, miller, h, dy):
    points = miller.shape[1]
    channels, atoms = h.shape
    width = 2 * channels
    wave = jax.ShapeDtypeStruct((points, atoms), jnp.bfloat16)
    sums = jax.ShapeDtypeStruct((points, 2 * width), jnp.float32)
    return fetching_call(
        phase_kernel,
        (pos, h, dy),
        (miller,),
        (wave, wave, sums),
        [
            pltpu.VMEM(wave.shape, wave.dtype),
            pltpu.VMEM(wave.shape, wave.dtype),
            pltpu.VMEM((atoms, width), jnp.bfloat16),
            pltpu.VMEM((16, atoms), jnp.bfloat16),
            pltpu.VMEM((CHUNK, atoms), jnp.float32),
            pltpu.SemaphoreType.DMA((2, points // CHUNK)),
        ],
        out_specs=(FAR, FAR, WHOLE),
        flops=6 * points * atoms * width,
    )


def wave_copies(cos_in, sin_in, cos_ref, sin_ref, sems, i):
    at = pl.ds(pl.multiple_of(i * CHUNK, CHUNK), CHUNK)
    return [
        pltpu.make_async_copy(cos_in.at[at], cos_ref.at[at], sems.at[0, i]),
        pltpu.make_async_copy(sin_in.at[at], sin_ref.at[at], sems.at[1, i]),
    ]


def ewald_early(cos_in, sin_in, *rest):
    for i in range(cos_in.shape[0] // CHUNK):
        for copy in wave_copies(cos_in, sin_in, *rest[-3:], i):
            copy.start()


def ewald_sums(coeff_ref, miller_ref, both, waves, sums_ref, turn_ref):
    f32 = jnp.float32
    width = both.shape[0]
    channels = width // 2
    run = CHUNK // (miller_ref.shape[1] // coeff_ref.shape[0])
    over_rows = (((0,), (0,)), ((), ()))

    def one(i, carry):
        for copy in wave_copies(*waves, i):
            copy.wait()
        at = pl.ds(pl.multiple_of(i * CHUNK, CHUNK), CHUNK)
        coeffs = coeff_ref[pl.ds(i * run, run), 0 : CHUNK // run].reshape(CHUNK, 2 * width)
        cos_part, sin_part = waves[2][at, :], waves[3][at, :]
        sums_ref[...] += lax.dot_general(
            coeffs[:, 0:channels], cos_part, over_rows, preferred_element_type=f32
        ) + lax.dot_general(
            coeffs[:, width : width + channels], sin_part, over_rows, preferred_element_type=f32
        )
        along_u = jnp.dot(coeffs[:, 0:width], both, preferred_element_type=f32)
        along_v = jnp.dot(coeffs[:, width:], both, preferred_element_type=f32)
        angle = along_v * cos_part.astype(f32) - along_u * sin_part.astype(f32)
        a_hi, a_lo = split_two(angle)
        m = miller_ref[:, at]
        turn_ref[...] += jnp.dot(m, a_hi, preferred_element_type=f32) + jnp.dot(
            m, a_lo, preferred_element_type=f32
        )
        return carry

    lax.fori_loop(0, miller_ref.shape[1] // CHUNK, one, 0)


def ewald_first(
    h_ref, dy_ref, cos_in, sin_in, coeff_ref, miller_ref, sums_ref, turn_ref, cos_ref, sin_ref, sems
):
    sums_ref[...] = jnp.zeros_like(sums_ref)
    turn_ref[...] = jnp.zeros_like(turn_ref)
    both = jnp.concatenate([h_ref[...], dy_ref[...]], axis=0)
    waves = (cos_in, sin_in, cos_ref, sin_ref, sems)
    ewald_sums(coeff_ref, miller_ref, both, waves, sums_ref, turn_ref)


def ewald_second(
    h_ref,
    dy_ref,
    kind_ref,
    gain_ref,
    mix_ref,
    cos_in,
    sin_in,
    coeff_ref,
    miller_ref,
    first_ref,
    angle_ref,
    inner_ref,
    upper_ref,
    lower_ref,
    core_ref,
    own_ref,
    mine_ref,
    atom_ref,
    pos_ref,
    weight_ref,
    radial_ref,
    sums_ref,
    turn_ref,
    cos_ref,
    sin_ref,
    sems,
):
    f32, bf16 = jnp.float32, jnp.bfloat16
    channels = h_ref.shape[0]
    cells = jnp.stack(
        [
            inner_ref[:, :, 0] + lower_ref[:, :, 0].astype(f32),
            inner_ref[:, :, 1],
            inner_ref[:, :, 2] + upper_ref[:, :, 0].astype(f32),
        ],
        axis=2,
    ).reshape(432, 128)
    flat = jnp.transpose(jnp.concatenate([cells, core_ref[...]], axis=0))
    gains = gains_of(gain_ref[...], kind_ref[...], (channels, flat.shape[1]))
    zscaled = (flat[0:channels] * gains).astype(bf16)
    halves = flat[channels : channels + 8]
    near = halves + pltpu.roll(halves, 4, 0) + own_ref[...]
    sums_ref[...] = first_ref[...] + jnp.dot(mix_ref[...], zscaled, preferred_element_type=f32)
    turn_ref[...] = angle_ref[...]
    both = jnp.concatenate([h_ref[...], dy_ref[...]], axis=0)
    waves = (cos_in, sin_in, cos_ref, sin_ref, sems)
    ewald_sums(coeff_ref, miller_ref, both, waves, sums_ref, turn_ref)
    atom_ref[...] = (dy_ref[...].astype(f32) + sums_ref[...]).astype(bf16)
    axes = ("gx", GY, GZ)
    for d in range(3):
        pos_ref[d] = (
            turn_ref[d : d + 1, :] * (circle_angle / lax.axis_size(axes[d])) + near[d : d + 1, :]
        )
    cut = (channels + radial_ref.shape[0]) // 2
    run = miller_ref.shape[1] // coeff_ref.shape[0]
    sides = []
    for ref in (mine_ref, coeff_ref):
        total = jnp.sum(ref[:, run:].astype(f32), axis=0)
        sides.append(jnp.concatenate([total[:, 0:128], total[:, 128:256]], axis=0))
    full = (sides[0] + sides[1])[0:cut]
    tall = jnp.concatenate([full[:, 0:channels], full[:, channels:]], axis=0)
    weight_ref[...] = tall[0:channels]
    radial_ref[...] = tall[channels:]


def ewald(coeffs, cos_all, sin_all, miller, h, dy, more=(), params=(), basis=0):
    points, atoms = cos_all.shape
    channels = h.shape[0]
    last = len(more) > 0
    shaped = jax.ShapeDtypeStruct
    sums = shaped((channels, atoms), jnp.float32)
    turn = shaped((16, atoms), jnp.float32)
    scratch = [
        pltpu.VMEM(cos_all.shape, jnp.bfloat16),
        pltpu.VMEM(cos_all.shape, jnp.bfloat16),
        pltpu.SemaphoreType.DMA((2, points // CHUNK)),
    ]
    outs = (sums, turn)
    if last:
        scratch = [pltpu.VMEM(sums.shape, sums.dtype), pltpu.VMEM(turn.shape, turn.dtype)] + scratch
        outs = (
            shaped(sums.shape, jnp.bfloat16),
            shaped((3, 1, atoms), jnp.float32),
            shaped((channels, channels), jnp.float32),
            shaped((basis, channels), jnp.float32),
        )
    return fetching_call(
        ewald_second if last else ewald_first,
        (h, dy, *params),
        (cos_all, sin_all, coeffs, miller, *more),
        outs,
        scratch,
        early=ewald_early,
        in_specs=(FAR, FAR) + (WHOLE,) * (2 + len(more)),
        flops=8 * points * atoms * channels,
        limit=20 if last else 52,
    )


def coefficients(totals, filt_rows, norm_atoms, norm_k):
    channels = filt_rows.shape[1]
    cos_struct = totals[:, 0:channels] * norm_atoms
    cos_back = totals[:, channels : 2 * channels] * norm_k
    sin_struct = totals[:, 2 * channels : 3 * channels] * norm_atoms
    sin_back = totals[:, 3 * channels : 4 * channels] * norm_k
    coeffs = jnp.concatenate(
        [
            norm_atoms * filt_rows * cos_back,
            norm_k * filt_rows * cos_struct,
            norm_atoms * filt_rows * sin_back,
            norm_k * filt_rows * sin_struct,
        ],
        axis=1,
    )
    return (coeffs, cos_struct * cos_back + sin_struct * sin_back)


def small_call(kernel, args, outs, params=LIMIT):
    return pl.pallas_call(
        kernel,
        out_shape=outs,
        in_specs=[WHOLE] * len(args),
        out_specs=(WHOLE,) * len(outs),
        compiler_params=params,
    )(*args)


def partial_kernel(pieces_ref, sums_ref, out_ref):
    f32, bf16 = jnp.float32, jnp.bfloat16
    total = jnp.sum(pieces_ref[...].astype(f32), axis=0)
    extra = out_ref.shape[1] - total.shape[0]
    sums = sums_ref[...]
    wide = jnp.concatenate([sums[0:extra], sums[extra : 2 * extra]], axis=1)
    whole = jnp.concatenate([total, wide], axis=0).astype(bf16)
    out_ref[...] = jnp.broadcast_to(whole[None], out_ref.shape)


def partial_sums(pieces, sums, tower):
    shape = (tower, pieces.shape[1] + 24, pieces.shape[2])
    outs = (jax.ShapeDtypeStruct(shape, jnp.bfloat16),)
    return small_call(partial_kernel, (pieces, sums), outs)[0]


def coefficient_kernel(norm_atoms, norm_k, pieces_ref, filt_ref, out_ref, filter_ref, all_filter):
    f32, bf16 = jnp.float32, jnp.bfloat16
    share = filter_ref.shape[0]
    rows = filt_ref.shape[0]
    both = jnp.sum(pieces_ref[...].astype(f32), axis=0)
    coeffs, all_filter[...] = coefficients(both[0:rows], filt_ref[...], norm_atoms, norm_k)
    mine = lax.axis_index(TOWER)
    filter_ref[...] = all_filter[pl.ds(pl.multiple_of(mine * share, share), share), :]
    strip = jnp.concatenate([coeffs, both[rows:]], axis=0).astype(bf16)
    out_ref[...] = jnp.broadcast_to(strip[None], out_ref.shape)


def make_strip(pieces, filt, sheet, norm_atoms, norm_k):
    tower, rows, width = pieces.shape
    share, channels = filt.shape[0] // tower, filt.shape[1]
    return pl.pallas_call(
        functools.partial(coefficient_kernel, norm_atoms, norm_k),
        out_shape=(
            jax.ShapeDtypeStruct((sheet, rows, width), jnp.bfloat16),
            jax.ShapeDtypeStruct((share, channels), jnp.float32),
        ),
        in_specs=[WHOLE, WHOLE],
        out_specs=(WHOLE, WHOLE),
        scratch_shapes=[pltpu.VMEM(filt.shape, jnp.float32)],
        compiler_params=LIMIT,
        name="coefficients",
    )(pieces, filt)


def fold_x_kernel(mid_ref, upper_ref, lower_ref, first_ref, last_ref, rest_ref):
    f32, bf16 = jnp.float32, jnp.bfloat16
    for n in range(3):
        plane = mid_ref[n]
        if n == 0:
            plane = plane + lower_ref[0].astype(f32)
        if n == 2:
            plane = plane + upper_ref[0].astype(f32)
        first_ref[n] = plane[0:1].astype(bf16)
        last_ref[n] = plane[4:5].astype(bf16)
        rest_ref[n] = plane[1:4]


def fold_x(mid, upper, lower):
    side = jax.ShapeDtypeStruct((3, 1, 5, 16, 128), jnp.bfloat16)
    rest = jax.ShapeDtypeStruct((3, 3, 5, 16, 128), jnp.float32)
    return small_call(fold_x_kernel, (mid, upper, lower), (side, side, rest), pltpu.CompilerParams(vmem_limit_bytes=20 * 1024 * 1024))


def fold_y_kernel(rest_ref, upper_ref, lower_ref, first_ref, last_ref, inner_ref):
    f32, bf16 = jnp.float32, jnp.bfloat16
    for n in range(3):
        plane = rest_ref[:, n]
        if n == 0:
            plane = plane + lower_ref[:, 0].astype(f32)
        if n == 2:
            plane = plane + upper_ref[:, 0].astype(f32)
        first_ref[:, n] = plane[:, 0:1].astype(bf16)
        last_ref[:, n] = plane[:, 4:5].astype(bf16)
        inner_ref[:, n] = plane[:, 1:4]


def fold_y(rest, upper, lower):
    side = jax.ShapeDtypeStruct((3, 3, 1, 16, 128), jnp.bfloat16)
    inner = jax.ShapeDtypeStruct((3, 3, 3, 16, 128), jnp.float32)
    return small_call(fold_y_kernel, (rest, upper, lower), (side, side, inner), None)


def sent_out(x, axis, dim):
    length = x.shape[dim]
    before = from_behind(lax.slice_in_dim(x, length - 1, length, axis=dim), axis, 1)
    after = from_behind(lax.slice_in_dim(x, 0, 1, axis=dim), axis, -1)
    return before, after


def whole(
    atom_embedding,
    output_adjoint,
    fractional_coords,
    element_labels,
    adjacent_ghost_entries,
    miller_triples,
    reciprocal_kernel,
    channel_mixing_matrix,
    element_channel_factor,
    distance_kernel,
):
    h = atom_embedding[0, 0, 0]
    dy = output_adjoint[0, 0, 0]
    pos = fractional_coords[0, 0, 0][:, None, :]
    kinds = element_labels[0, 0]
    channels, atoms = h.shape
    points = miller_triples.shape[1]
    devices = lax.axis_size(GX_GY_GZ)
    norm_atoms = (atoms * devices) ** (-0.5)
    norm_k = points ** (-0.5)
    half = points // 2

    cells, core, first, last, miller_mine, miller_next = pack(h, kinds, pos, miller_triples)
    cells = cells.reshape(3, 3, 3, 16, 128)
    below, above = from_behind(last, GZ, 1), from_behind(first, GZ, -1)
    cos_next, sin_next, part_next = phase_sums(pos, miller_next, h, dy)
    received = from_behind(part_next, PAIR, 1)
    cells = jnp.concatenate([below, cells, above], axis=2)
    below, above = sent_out(cells, GY, 1)
    cos_mine, sin_mine, part_mine = phase_sums(pos, miller_mine, h, dy)
    cells = jnp.concatenate([below, cells, above], axis=1)
    below, above = sent_out(cells, "gx", 0)
    sheet, tower = lax.axis_size(SHEET), lax.axis_size(TOWER)
    width = 4 * channels
    paired = (part_mine + received).astype(jnp.bfloat16)
    pieces = lax.all_to_all(paired.reshape(sheet, half // sheet, width), SHEET, 0, 0)

    low, mid, high, core_grad, own_grad, sums, filt = short_range(
        (below.reshape(400, 128), cells.reshape(1200, 128), above.reshape(400, 128), core),
        adjacent_ghost_entries[0, 0, 0],
        pos,
        dy,
        distance_kernel,
        channel_mixing_matrix,
        element_channel_factor,
        reciprocal_kernel.T,
    )
    parts = partial_sums(pieces, sums, tower)
    pieces = lax.all_to_all(parts, TOWER, 0, 0)

    upper = from_behind(low.reshape(1, 5, 5, 16, 128), "gx", -1)
    lower = from_behind(high.reshape(1, 5, 5, 16, 128), "gx", 1)
    first, last, rest = fold_x(mid.reshape(3, 5, 5, 16, 128), upper, lower)
    upper, lower = from_behind(first, GY, -1), from_behind(last, GY, 1)
    strip, filter_share = make_strip(pieces, filt, sheet, norm_atoms, norm_k)
    got = lax.all_to_all(strip, SHEET, 0, 0)
    first, last, inner = fold_y(rest, upper, lower)
    upper, lower = from_behind(first, GZ, -1), from_behind(last, GZ, 1)
    got_next = from_behind(got, PAIR, 1)
    early_sums = ewald(got, cos_mine, sin_mine, miller_mine, h, dy)
    atom_grad, position_grad, weight_grad, radial_grad = ewald(
        got_next,
        cos_next,
        sin_next,
        miller_next,
        h,
        dy,
        (*early_sums, inner, upper, lower, core_grad, own_grad, got),
        (kinds, element_channel_factor, channel_mixing_matrix),
        distance_kernel.shape[0],
    )
    position_grad = position_grad[:, 0, :]
    return (
        atom_grad[None, None, None],
        position_grad[None, None, None],
        weight_grad,
        radial_grad,
        filter_share,
    )


def solution(mesh):
    finer = Mesh(
        mesh.devices.reshape(mesh.shape["gx"], 4, 4, 2, 2), ("gx", "gy_0", "gy_1", "gz_0", "gz_1")
    )
    in_specs = (
        P("gx", GY, GZ, None, None),
        P("gx", GY, GZ, None, None),
        P("gx", GY, GZ, None, None),
        P("gx", GY, GZ, None),
        P("gx", GY, GZ, None, None),
        P(),
        P(),
        P(),
        P(),
        P(),
    )
    out_specs = (
        P("gx", GY, GZ, None, None),
        P("gx", GY, GZ, None, None),
        P(),
        P(),
        P(GX_GY_GZ, None),
    )
    return jax.shard_map(whole, mesh=finer, in_specs=in_specs, out_specs=out_specs, check_vma=False)
```
